8 devices in a mesh: dp: 1 (over z), hid: 2 (over y), tp: 4 (over x, core).
Axes of the slice: x: 2, y: 2, z: 1, core: 2. Of those that a mesh axis runs over, the one named last changes fastest.
Arguments:
- hidden: bfloat16 [1024, 2048], P('dp', 'hid')
- rms_attn: float32 [2048], P('hid')
- rms_mlp: float32 [2048], P('hid')
- w_q: bfloat16 [2048, 2048], P('hid', 'tp')
- w_k: bfloat16 [2048, 512], P('hid', 'tp')
- w_v: bfloat16 [2048, 512], P('hid', 'tp')
- w_o: bfloat16 [2048, 2048], P('tp', 'hid')
- w_gate: bfloat16 [2048, 8192], P('hid', 'tp')
- w_up: bfloat16 [2048, 8192], P('hid', 'tp')
- w_down: bfloat16 [8192, 2048], P('tp', 'hid')
- k_cache: bfloat16 [2048, 8, 64], P('dp', 'tp')
- v_cache: bfloat16 [2048, 8, 64], P('dp', 'tp')
- past_len: int32 [1], P('dp')
Outputs:
- output 1: bfloat16 [1024, 2048], P('dp', 'hid')
- output 2: bfloat16 [2048, 8, 64], P('dp', 'tp')
- output 3: bfloat16 [2048, 8, 64], P('dp', 'tp')
All inputs are finite; a program needn't handle non-finite values.
Results may differ from the reference program's by a relative error of at most 0.0148705.
Values are sent between devices in bfloat16 or wider.
A program may use at most 1 GiB of HBM per device.

```python
import math
import jax
import jax.numpy as jnp
from jax import lax

D = 2048
HEADS = 32
KV_HEADS = 8
HEAD = 64
FF = 8192
TOKENS = 1024
PAST = 1024
ROPE_BASE = 10000
TMAX = PAST + TOKENS


def setup_inputs(seed: int = 0, part: int = 0) -> dict:
    shared = jax.random.split(jax.random.key(seed), 9)
    own_keys = jax.random.split(jax.random.fold_in(jax.random.key(seed + 1), part), 5)

    def draw_weight(rng_key, n_rows, n_cols, gain_val):
        normal_draw = jax.random.normal(rng_key, (n_rows, n_cols), jnp.float32)
        return (normal_draw * (gain_val / math.sqrt(n_rows))).astype(jnp.bfloat16)

    col_scale = 0.5 * jnp.exp2(2.0 * jnp.arange(D, dtype=jnp.float32) / D)
    tok_scale = jnp.exp(jax.random.uniform(own_keys[0], (TOKENS, 1), jnp.float32, -0.7, 0.7))
    hidden = (jax.random.normal(own_keys[1], (TOKENS, D), jnp.float32) * tok_scale * col_scale).astype(jnp.bfloat16)
    k_cache = (1.5 * jax.random.normal(own_keys[2], (TMAX, KV_HEADS, HEAD), jnp.float32)).astype(jnp.bfloat16)
    v_cache = jax.random.normal(own_keys[3], (TMAX, KV_HEADS, HEAD), jnp.float32).astype(jnp.bfloat16)
    past_len = jax.random.randint(own_keys[4], (1,), PAST // 4, PAST + 1, jnp.int32)
    return {
        'hidden': hidden,
        'rms_attn': 1.0 + 0.2 * jax.random.normal(shared[0], (D,), jnp.float32),
        'rms_mlp': 1.0 + 0.2 * jax.random.normal(shared[1], (D,), jnp.float32),
        'w_q': draw_weight(shared[2], D, HEADS * HEAD, 1.5),
        'w_k': draw_weight(shared[3], D, KV_HEADS * HEAD, 1.5),
        'w_v': draw_weight(shared[4], D, KV_HEADS * HEAD, 1.0),
        'w_o': draw_weight(shared[5], HEADS * HEAD, D, 2.0),
        'w_gate': draw_weight(shared[6], D, FF, 1.0),
        'w_up': draw_weight(shared[7], D, FF, 1.0),
        'w_down': draw_weight(shared[8], FF, D, 1.0),
        'k_cache': k_cache,
        'v_cache': v_cache,
        'past_len': past_len,
    }


def rms_norm(x_in, gain_vec):
    x_f32 = x_in.astype(jnp.float32)
    inv_rms = lax.rsqrt(jnp.mean(x_f32 * x_f32, axis=-1, keepdims=True) + 1e-5)
    return (x_f32 * inv_rms * gain_vec).astype(jnp.bfloat16)


def rope_tables(pos_start):
    positions = (pos_start + jnp.arange(TOKENS)).astype(jnp.float32)
    inv_freq = jnp.exp(jnp.arange(HEAD // 2, dtype=jnp.float32) * (-2.0 * math.log(ROPE_BASE) / HEAD))
    angles = positions[:, None] * inv_freq[None, :]
    return jnp.cos(angles)[:, None, :], jnp.sin(angles)[:, None, :]


def apply_rope(x_in, cos_t, sin_t):
    x_f32 = x_in.astype(jnp.float32)
    half_dim = x_f32.shape[-1] // 2
    x_first = x_f32[..., :half_dim]
    x_second = x_f32[..., half_dim:]
    rotated = jnp.concatenate([x_first * cos_t - x_second * sin_t, x_second * cos_t + x_first * sin_t], axis=-1)
    return rotated.astype(jnp.bfloat16)


def reference(hidden, rms_attn, rms_mlp, w_q, w_k, w_v, w_o, w_gate, w_up, w_down, k_cache, v_cache, past_len):
    pos_start = past_len[0]
    u_attn = rms_norm(hidden, rms_attn)
    cos_t, sin_t = rope_tables(pos_start)
    q_proj = jnp.dot(u_attn, w_q, preferred_element_type=jnp.float32).astype(jnp.bfloat16)
    k_proj = jnp.dot(u_attn, w_k, preferred_element_type=jnp.float32).astype(jnp.bfloat16)
    q_rot = apply_rope(q_proj.reshape(TOKENS, HEADS, HEAD), cos_t, sin_t)
    k_rot = apply_rope(k_proj.reshape(TOKENS, KV_HEADS, HEAD), cos_t, sin_t)
    v_new = jnp.dot(u_attn, w_v, preferred_element_type=jnp.float32).astype(jnp.bfloat16).reshape(TOKENS, KV_HEADS, HEAD)
    k_full = lax.dynamic_update_slice_in_dim(k_cache, k_rot, pos_start, axis=0)
    v_full = lax.dynamic_update_slice_in_dim(v_cache, v_new, pos_start, axis=0)
    group_size = HEADS // KV_HEADS
    q_grp = q_rot.reshape(TOKENS, KV_HEADS, group_size, HEAD).transpose(1, 2, 0, 3)
    causal = jnp.arange(TMAX)[None, :] <= (pos_start + jnp.arange(TOKENS))[:, None]

    def one_kv_head(operands):
        q_head, k_head, v_head = operands
        scores = jnp.einsum('rcd,td->rct', q_head.astype(jnp.float32), k_head.astype(jnp.float32)) * (HEAD ** -0.5)
        attn_probs = jax.nn.softmax(jnp.where(causal, scores, -1e30), axis=-1).astype(jnp.bfloat16)
        return jnp.einsum('rct,td->rcd', attn_probs.astype(jnp.float32), v_head.astype(jnp.float32)).astype(jnp.bfloat16)

    head_mix = lax.map(one_kv_head, (q_grp, k_full.transpose(1, 0, 2), v_full.transpose(1, 0, 2)))
    head_mix = head_mix.transpose(2, 0, 1, 3).reshape(TOKENS, HEADS * HEAD)
    attn_out = jnp.dot(head_mix, w_o, preferred_element_type=jnp.float32).astype(jnp.bfloat16)
    h_mid = (hidden.astype(jnp.float32) + attn_out.astype(jnp.float32)).astype(jnp.bfloat16)
    u_mlp = rms_norm(h_mid, rms_mlp)
    gate_sum = jnp.dot(u_mlp, w_gate, preferred_element_type=jnp.float32).astype(jnp.bfloat16)
    up_sum = jnp.dot(u_mlp, w_up, preferred_element_type=jnp.float32).astype(jnp.bfloat16)
    activated = (jax.nn.silu(gate_sum.astype(jnp.float32)) * up_sum.astype(jnp.float32)).astype(jnp.bfloat16)
    down_sum = jnp.dot(activated, w_down, preferred_element_type=jnp.float32).astype(jnp.bfloat16)
    layer_out = (h_mid.astype(jnp.float32) + down_sum.astype(jnp.float32)).astype(jnp.bfloat16)
    return layer_out, k_full, v_full
```

```python
import functools
import math
import jax
import jax.numpy as jnp
from jax import lax
from jax.experimental import pallas as pl
from jax.experimental.pallas import tpu as pltpu
from jax.sharding import PartitionSpec as P

ROPE_BASE = 10000.0
F32, BF16 = jnp.float32, jnp.bfloat16
NEG = -1e30
BLK = 256
HALF = BLK // 2
PAST_MAX = 1024


def call(body, out_shape, grid=(), in_specs=None, out_specs=None, nscalar=0, scratch=(), flops=0, name=None, vmem=None):
    return pl.pallas_call(
        body,
        out_shape=out_shape,
        grid_spec=pltpu.PrefetchScalarGridSpec(
            num_scalar_prefetch=nscalar, grid=grid, in_specs=in_specs, out_specs=out_specs, scratch_shapes=list(scratch)),
        cost_estimate=pl.CostEstimate(flops=int(flops), bytes_accessed=1 << 20, transcendentals=0),
        compiler_params=pltpu.CompilerParams(vmem_limit_bytes=vmem or (32 << 20)),
        name=name)


def sds(*shape, dtype=BF16):
    return jax.ShapeDtypeStruct(shape, dtype)


def whole(*shape):
    return pl.BlockSpec(shape, lambda *_: (0,) * len(shape))


def qkv_body(h_ref, x_ref, g_ref, wq_ref, wk_ref, wv_ref, send_ref, keep_ref):
    own = h_ref[0] == 0
    xg = (x_ref[...].astype(F32) * g_ref[...]).astype(BF16)
    q = jnp.dot(xg, wq_ref[...], preferred_element_type=F32).astype(BF16)
    n = q.shape[1] // 2
    send_ref[:, :n] = jnp.where(own, q[:, n:], q[:, :n])
    keep_ref[...] = jnp.where(own, q[:, :n], q[:, n:])
    m = wk_ref.shape[1]
    send_ref[:, n:n + m] = jnp.dot(xg, wk_ref[...], preferred_element_type=F32).astype(BF16)
    send_ref[:, n + m:] = jnp.dot(xg, wv_ref[...], preferred_element_type=F32).astype(BF16)


def rope(t, cos_t, sin_t):
    width = t.shape[1]
    reps = width // 128
    lane = lax.broadcasted_iota(jnp.int32, t.shape, 1)
    swapped = jnp.where((lane & 63) < 32, pltpu.roll(t, width - 32, 1), pltpu.roll(t, 32, 1))
    cos_w = jnp.concatenate([cos_t] * reps, axis=1)
    sin_w = jnp.concatenate([sin_t] * reps, axis=1)
    return (t * cos_w + swapped * sin_w).astype(BF16)


def att_body(i, h_ref, p_ref, send_ref, keep_ref, recv_ref, r_ref, cos_ref, sin_ref, kc_ref, vc_ref, *rest):
    prev, (o_ref, kv_ref, kh_ref, vh_ref, kk, vv) = rest[:2 * i], rest[2 * i:]
    own = h_ref[0] == 0
    r = r_ref[...][:, :1]
    cos_t, sin_t = cos_ref[...], sin_ref[...]
    q = ((keep_ref[...].astype(F32) + recv_ref[:, :256].astype(F32)) * r).astype(BF16)
    kv = ((send_ref[:, 256:].astype(F32) + recv_ref[:, 256:].astype(F32)) * r).astype(BF16)
    q = (rope(q.astype(F32), cos_t, sin_t).astype(F32) * 0.125).astype(BF16)
    k = rope(kv[:, :128].astype(F32), cos_t, sin_t)
    v = kv[:, 128:]
    kv_ref[:, :128] = k
    kv_ref[:, 128:] = v
    kh = jnp.where(own, k[:, :64], k[:, 64:])
    vh = jnp.where(own, v[:, :64], v[:, 64:])
    kh_ref[...] = kh
    vh_ref[...] = vh
    kk[:PAST_MAX] = kc_ref[...]
    vv[:PAST_MAX] = vc_ref[...]
    for j in range(i):
        kk[PAST_MAX + j * BLK:PAST_MAX + (j + 1) * BLK] = prev[2 * j][...]
        vv[PAST_MAX + j * BLK:PAST_MAX + (j + 1) * BLK] = prev[2 * j + 1][...]
    main = PAST_MAX + i * BLK
    col = lax.broadcasted_iota(jnp.int32, (1, main), 1)
    bias = jnp.where((col >= p_ref[0]) & (col < PAST_MAX), NEG, 0.0)
    causal = lax.broadcasted_iota(jnp.int32, (BLK, BLK), 1) <= lax.broadcasted_iota(jnp.int32, (BLK, BLK), 0)
    nt = (((1,), (1,)), ((), ()))
    for n in range(4):
        qn = q[:, n * 64:(n + 1) * 64]
        s_main = lax.dot_general(qn, kk[...], nt, preferred_element_type=F32) + bias
        s_diag = jnp.where(causal, lax.dot_general(qn, kh, nt, preferred_element_type=F32), NEG)
        top = jnp.maximum(jnp.max(s_main, axis=1, keepdims=True), jnp.max(s_diag, axis=1, keepdims=True))
        e_main = jnp.exp(s_main - top)
        e_diag = jnp.exp(s_diag - top)
        inv = 1.0 / (jnp.sum(e_main, axis=1, keepdims=True) + jnp.sum(e_diag, axis=1, keepdims=True))
        o = jnp.dot((e_main * inv).astype(BF16), vv[...], preferred_element_type=F32)
        o += jnp.dot((e_diag * inv).astype(BF16), vh, preferred_element_type=F32)
        o_ref[:, n * 64:(n + 1) * 64] = o.astype(BF16)


def wo_body(h_ref, c_ref, own_ref, recv_ref, w_ref, send_ref, keep_ref, acc):
    n = own_ref.shape[1]
    h, c = h_ref[0], c_ref[0]
    acc[...] = jnp.dot(own_ref[...], w_ref[pl.ds(pl.multiple_of(h * n, n), n), :], preferred_element_type=F32)
    acc[...] += jnp.dot(recv_ref[...], w_ref[pl.ds(pl.multiple_of((1 - h) * n, n), n), :], preferred_element_type=F32)
    keep_ref[...] = acc[pl.ds(pl.multiple_of(c * HALF, HALF), HALF), :].astype(BF16)
    send_ref[...] = acc[pl.ds(pl.multiple_of((1 - c) * HALF, HALF), HALF), :].astype(BF16)


def gu_body(h_ref, own_ref, recv_ref, g_ref, wg_ref, wu_ref, out_ref):
    g = g_ref[...]
    hg = jnp.concatenate([(own_ref[...].astype(F32) * g).astype(BF16), (recv_ref[...].astype(F32) * g).astype(BF16)], axis=0)
    n = wg_ref.shape[1]
    out_ref[:, :n] = jnp.dot(hg, wg_ref[...], preferred_element_type=F32).astype(BF16)
    out_ref[:, n:] = jnp.dot(hg, wu_ref[...], preferred_element_type=F32).astype(BF16)


def act_body(keep_ref, recv_ref, r_ref, a_ref):
    n = a_ref.shape[1]
    both = ((keep_ref[...].astype(F32) + recv_ref[...].astype(F32)) * r_ref[...][:, :1]).astype(BF16).astype(F32)
    g, e = both[:, :n], both[:, n:]
    a_ref[...] = (g * jax.nn.sigmoid(g) * e).astype(BF16)


def down_body(h_ref, own_ref, recv_ref, w_ref, send_ref, keep_ref):
    n = own_ref.shape[1]
    h = h_ref[0]
    y = jnp.dot(own_ref[...], w_ref[pl.ds(pl.multiple_of(h * n, n), n), :], preferred_element_type=F32)
    y += jnp.dot(recv_ref[...], w_ref[pl.ds(pl.multiple_of((1 - h) * n, n), n), :], preferred_element_type=F32)
    keep_ref[...] = y[:HALF].astype(BF16)
    send_ref[...] = y[HALF:].astype(BF16)


def solution(mesh):
    def over_hid(t):
        return lax.ppermute(t, 'hid', [(0, 1), (1, 0)])

    def over_x(t):
        return lax.ppermute(t, 'tp', [(0, 2), (2, 0), (1, 3), (3, 1)])

    def over_core(t):
        return lax.ppermute(t, 'tp', [(0, 1), (1, 0), (2, 3), (3, 2)])

    def add(a, b):
        return (a.astype(F32) + b.astype(F32)).astype(BF16)

    def local_layer(hidden, rms_attn, rms_mlp, w_q, w_k, w_v, w_o, w_gate, w_up, w_down, k_cache, v_cache, past_len):
        new_len, width = hidden.shape
        d_model = width * 2
        blocks = new_len // BLK
        h = lax.axis_index('hid').reshape(1)
        c = (lax.axis_index('tp') % 2).reshape(1)
        pos_start = past_len[0]
        g1 = rms_attn.reshape(1, width)
        g2 = rms_mlp.reshape(1, width)

        sends, keeps, recvs = [], [], []
        for i in range(blocks):
            send, keep = call(
                qkv_body, (sds(BLK, 512), sds(BLK, 256)), grid=(1,), nscalar=1,
                in_specs=[pl.BlockSpec((BLK, width), lambda *_, i=i: (i, 0)), whole(1, width), whole(*w_q.shape),
                          whole(*w_k.shape), whole(*w_v.shape)],
                out_specs=(whole(BLK, 512), whole(BLK, 256)), flops=2 * BLK * width * 768, name=f"qkv{i}",
            )(h, hidden, g1, w_q, w_k, w_v)
            sends.append(send)
            keeps.append(keep)
            recvs.append(over_hid(send))

        x_f32 = hidden.astype(F32)
        sq = jnp.sum(x_f32 * x_f32, axis=1)
        r1 = lax.rsqrt((sq + over_hid(sq)) / d_model + 1e-5)
        r1 = jnp.broadcast_to(r1[:, None], (new_len, 128))
        positions = (pos_start + jnp.arange(new_len)).astype(F32)
        inv_freq = jnp.exp(jnp.arange(32, dtype=F32) * (-2.0 * math.log(ROPE_BASE) / 64))
        angles = positions[:, None] * inv_freq[None, :]
        cos_t, sin_t = jnp.cos(angles), jnp.sin(angles)
        cos_t = jnp.concatenate([cos_t] * 4, axis=1)
        sin_t = jnp.concatenate([-sin_t, sin_t] * 2, axis=1)
        kc = lax.dynamic_slice(k_cache, (0, h[0], 0), (PAST_MAX, 1, 64)).reshape(PAST_MAX, 64)
        vc = lax.dynamic_slice(v_cache, (0, h[0], 0), (PAST_MAX, 1, 64)).reshape(PAST_MAX, 64)

        def reduce_tp(send, keep, residual):
            part = add(keep, over_core(send))
            own = add(residual, add(part, over_x(part)))
            return own, over_core(own)

        row = lambda i: pl.BlockSpec((BLK, 128), lambda *_: (i, 0))
        prev, kvs, mids = [], [], []
        for i in range(blocks):
            main = PAST_MAX + i * BLK
            o, kv, kh, vh = call(
                functools.partial(att_body, i), (sds(BLK, 256), sds(BLK, 256), sds(BLK, 64), sds(BLK, 64)), grid=(1,), nscalar=2,
                in_specs=[whole(BLK, 512), whole(BLK, 256), whole(BLK, 512), row(i), row(i), row(i),
                          whole(PAST_MAX, 64), whole(PAST_MAX, 64)] + [whole(BLK, 64)] * (2 * i),
                out_specs=(whole(BLK, 256), whole(BLK, 256), whole(BLK, 64), whole(BLK, 64)),
                scratch=[pltpu.VMEM((main, 64), BF16)] * 2, flops=4 * 4 * BLK * (main + BLK) * 64 * 4, name=f"att{i}",
            )(h, past_len, sends[i], keeps[i], recvs[i], r1, cos_t, sin_t, kc, vc, *prev)
            prev += [kh, vh]
            kvs.append(kv)
            o_recv = over_hid(o)
            send, keep = call(
                wo_body, (sds(HALF, width), sds(HALF, width)), grid=(1,), nscalar=2,
                in_specs=[whole(BLK, 256), whole(BLK, 256), whole(*w_o.shape)],
                out_specs=(whole(HALF, width), whole(HALF, width)), scratch=[pltpu.VMEM((BLK, width), F32)],
                flops=2 * BLK * 512 * width, name=f"wo{i}",
            )(h, c, o, o_recv, w_o)
            x_own = lax.dynamic_slice(hidden, (i * BLK + c[0] * HALF, 0), (HALF, width))
            mids.append(reduce_tp(send, keep, x_own))

        kv_new = jnp.concatenate(kvs, axis=0)
        k_full = lax.dynamic_update_slice(k_cache, kv_new[:, :128].reshape(new_len, 2, 64), (pos_start, 0, 0))
        v_full = lax.dynamic_update_slice(v_cache, kv_new[:, 128:].reshape(new_len, 2, 64), (pos_start, 0, 0))

        tile = 512
        cols = w_gate.shape[1] // 2
        steps = cols // tile
        outs = []
        for i in range(blocks):
            own, other = mids[i]

            def gate_up(flip, tag):
                def col(j, h_ref):
                    return (0, (h_ref[0] + flip - 2 * flip * h_ref[0]) * steps + j)
                return call(
                    gu_body, sds(BLK, 2 * cols), grid=(steps,), nscalar=1,
                    in_specs=[whole(HALF, width), whole(HALF, width), whole(1, width),
                              pl.BlockSpec((width, tile), col), pl.BlockSpec((width, tile), col)],
                    out_specs=pl.BlockSpec((BLK, 2 * tile), lambda j, *_: (0, j)),
                    flops=2 * BLK * width * 2 * cols, name=f"{tag}{i}",
                )(h, own, other, g2, w_gate, w_up)

            gu_recv = over_hid(gate_up(1, "gs"))
            sq2 = jnp.concatenate([jnp.sum(jnp.square(t.astype(F32)), axis=1) for t in (own, other)])
            r2 = lax.rsqrt((sq2 + over_hid(sq2)) / d_model + 1e-5)
            r2 = jnp.broadcast_to(r2[:, None], (BLK, 128))
            gu_keep = gate_up(0, "gk")
            a = call(
                act_body, sds(BLK, cols), grid=(steps,),
                in_specs=[pl.BlockSpec((BLK, 2 * tile), lambda j: (0, j)), pl.BlockSpec((BLK, 2 * tile), lambda j: (0, j)),
                          whole(BLK, 128)],
                out_specs=pl.BlockSpec((BLK, tile), lambda j: (0, j)), flops=BLK * cols * 2000, name=f"act{i}",
            )(gu_keep, gu_recv, r2)
            a_recv = over_hid(a)
            wide = w_down.shape[1] // 4
            send, keep = call(
                down_body, (sds(HALF, width), sds(HALF, width)), grid=(4,), nscalar=1,
                in_specs=[whole(BLK, cols), whole(BLK, cols), pl.BlockSpec((2 * cols, wide), lambda j, *_: (0, j))],
                out_specs=(pl.BlockSpec((HALF, wide), lambda j, *_: (0, j)), pl.BlockSpec((HALF, wide), lambda j, *_: (0, j))),
                flops=2 * BLK * 2 * cols * width, name=f"down{i}",
            )(h, a, a_recv, w_down)
            fin, fin_other = reduce_tp(send, keep, own)
            first = c[0] == 0
            outs += [jnp.where(first, fin, fin_other), jnp.where(first, fin_other, fin)]
        return jnp.concatenate(outs, axis=0), k_full, v_full

    row_split = P('hid', 'tp')
    col_split = P('tp', 'hid')
    cache_spec = P('dp', 'tp', None)
    in_specs = (P('dp', 'hid'), P('hid'), P('hid'), row_split, row_split, row_split, col_split,
                row_split, row_split, col_split, cache_spec, cache_spec, P('dp'))
    out_specs = (P('dp', 'hid'), cache_spec, cache_spec)
    return jax.shard_map(local_layer, mesh=mesh, in_specs=in_specs, out_specs=out_specs, check_vma=False)
```

```python
import functools
import math
import jax
import jax.numpy as jnp
from jax import lax
from jax.experimental import pallas as pl
from jax.experimental.pallas import tpu as pltpu
from jax.sharding import PartitionSpec as P

ROPE_BASE = 10000.0
F32, BF16 = jnp.float32, jnp.bfloat16
NEG = -1e30
BLK = 256
HALF = BLK // 2
PAST_MAX = 1024


def call(body, out_shape, grid=(), in_specs=None, out_specs=None, nscalar=0, scratch=(), flops=0, vmem=None, alias=None):
    return pl.pallas_call(
        body,
        out_shape=out_shape,
        grid_spec=pltpu.PrefetchScalarGridSpec(
            num_scalar_prefetch=nscalar, grid=grid, in_specs=in_specs, out_specs=out_specs, scratch_shapes=list(scratch)),
        cost_estimate=pl.CostEstimate(flops=int(flops), bytes_accessed=1 << 20, transcendentals=0),
        compiler_params=pltpu.CompilerParams(vmem_limit_bytes=vmem or (32 << 20)),
        input_output_aliases=alias or {})


def sds(*shape, dtype=BF16):
    return jax.ShapeDtypeStruct(shape, dtype)


def whole(*shape):
    return pl.BlockSpec(shape, lambda *_: (0,) * len(shape))


def qkv_body(h_ref, x_ref, g_ref, wq_ref, wk_ref, wv_ref, send_ref, keep_ref):
    own = h_ref[0] == 0
    xg = (x_ref[...].astype(F32) * g_ref[...]).astype(BF16)
    q = jnp.dot(xg, wq_ref[...], preferred_element_type=F32).astype(BF16)
    n = q.shape[1] // 2
    send_ref[:, :n] = jnp.where(own, q[:, n:], q[:, :n])
    keep_ref[...] = jnp.where(own, q[:, :n], q[:, n:])
    m = wk_ref.shape[1]
    send_ref[:, n:n + m] = jnp.dot(xg, wk_ref[...], preferred_element_type=F32).astype(BF16)
    send_ref[:, n + m:] = jnp.dot(xg, wv_ref[...], preferred_element_type=F32).astype(BF16)


def rope(t, cos_t, sin_t):
    width = t.shape[1]
    reps = width // 128
    lane = lax.broadcasted_iota(jnp.int32, t.shape, 1)
    swapped = jnp.where((lane & 63) < 32, pltpu.roll(t, width - 32, 1), pltpu.roll(t, 32, 1))
    cos_w = jnp.concatenate([cos_t] * reps, axis=1)
    sin_w = jnp.concatenate([sin_t] * reps, axis=1)
    return (t * cos_w + swapped * sin_w).astype(BF16)


def att_body(i, h_ref, p_ref, send_ref, keep_ref, recv_ref, r_ref, cos_ref, sin_ref, kc_ref, vc_ref, *rest):
    prev, (o_ref, kv_ref, kh_ref, vh_ref, kk, vv) = rest[:2 * i], rest[2 * i:]
    own = h_ref[0] == 0
    r = r_ref[...][:, :1]
    cos_t, sin_t = cos_ref[...], sin_ref[...]
    q = ((keep_ref[...].astype(F32) + recv_ref[:, :256].astype(F32)) * r).astype(BF16)
    kv = ((send_ref[:, 256:].astype(F32) + recv_ref[:, 256:].astype(F32)) * r).astype(BF16)
    q = (rope(q.astype(F32), cos_t, sin_t).astype(F32) * 0.125).astype(BF16)
    k = rope(kv[:, :128].astype(F32), cos_t, sin_t)
    v = kv[:, 128:]
    kv_ref[:, :128] = k
    kv_ref[:, 128:] = v
    kh = jnp.where(own, k[:, :64], k[:, 64:])
    vh = jnp.where(own, v[:, :64], v[:, 64:])
    kh_ref[...] = kh
    vh_ref[...] = vh
    kk[:PAST_MAX] = jnp.where(own, kc_ref[:, :64], kc_ref[:, 64:])
    vv[:PAST_MAX] = jnp.where(own, vc_ref[:, :64], vc_ref[:, 64:])
    for j in range(i):
        kk[PAST_MAX + j * BLK:PAST_MAX + (j + 1) * BLK] = prev[2 * j][...]
        vv[PAST_MAX + j * BLK:PAST_MAX + (j + 1) * BLK] = prev[2 * j + 1][...]
    main = PAST_MAX + i * BLK
    col = lax.broadcasted_iota(jnp.int32, (1, main), 1)
    bias = jnp.where((col >= p_ref[0]) & (col < PAST_MAX), NEG, 0.0)
    causal = lax.broadcasted_iota(jnp.int32, (BLK, BLK), 1) <= lax.broadcasted_iota(jnp.int32, (BLK, BLK), 0)
    nt = (((1,), (1,)), ((), ()))
    for n in range(4):
        qn = q[:, n * 64:(n + 1) * 64]
        s_main = lax.dot_general(qn, kk[...], nt, preferred_element_type=F32) + bias
        s_diag = jnp.where(causal, lax.dot_general(qn, kh, nt, preferred_element_type=F32), NEG)
        top = jnp.maximum(jnp.max(s_main, axis=1, keepdims=True), jnp.max(s_diag, axis=1, keepdims=True))
        e_main = jnp.exp(s_main - top)
        e_diag = jnp.exp(s_diag - top)
        inv = 1.0 / (jnp.sum(e_main, axis=1, keepdims=True) + jnp.sum(e_diag, axis=1, keepdims=True))
        o = jnp.dot((e_main * inv).astype(BF16), vv[...], preferred_element_type=F32)
        o += jnp.dot((e_diag * inv).astype(BF16), vh, preferred_element_type=F32)
        o_ref[:, n * 64:(n + 1) * 64] = o.astype(BF16)


def wo_body(h_ref, c_ref, own_ref, recv_ref, w_ref, send_ref, keep_ref, acc):
    n = own_ref.shape[1]
    h, c = h_ref[0], c_ref[0]
    acc[...] = jnp.dot(own_ref[...], w_ref[pl.ds(pl.multiple_of(h * n, n), n), :], preferred_element_type=F32)
    acc[...] += jnp.dot(recv_ref[...], w_ref[pl.ds(pl.multiple_of((1 - h) * n, n), n), :], preferred_element_type=F32)
    keep_ref[...] = acc[pl.ds(pl.multiple_of(c * HALF, HALF), HALF), :].astype(BF16)
    send_ref[...] = acc[pl.ds(pl.multiple_of((1 - c) * HALF, HALF), HALF), :].astype(BF16)


def add2_body(a_ref, b_ref, o_ref):
    o_ref[...] = (a_ref[...].astype(F32) + b_ref[...].astype(F32)).astype(BF16)


def add3_body(c_ref, res_ref, a_ref, b_ref, o_ref):
    part = (a_ref[...].astype(F32) + b_ref[...].astype(F32)).astype(BF16)
    o_ref[...] = (res_ref[...].astype(F32) + part.astype(F32)).astype(BF16)


def write_body(c_ref, own_ref, other_ref, *rest):
    rest[-1][...] = jnp.where(pl.program_id(0) == 0, own_ref[...], other_ref[...])


def gu_body(h_ref, own_ref, recv_ref, g_ref, wg_ref, wu_ref, out_ref, *sq_ref):
    if sq_ref:
        @pl.when(pl.program_id(0) == 0)
        def _():
            for k, ref in enumerate((own_ref, recv_ref)):
                t = ref[...].astype(F32)
                sq = jnp.broadcast_to(jnp.sum(t * t, axis=1, keepdims=True), (HALF, 128))
                sq_ref[0][:, k * HALF:(k + 1) * HALF] = jnp.transpose(sq)[:8]
    g = g_ref[...]
    hg = jnp.concatenate([(own_ref[...].astype(F32) * g).astype(BF16), (recv_ref[...].astype(F32) * g).astype(BF16)], axis=0)
    n = wg_ref.shape[1]
    out_ref[:, :n] = jnp.dot(hg, wg_ref[...], preferred_element_type=F32).astype(BF16)
    out_ref[:, n:] = jnp.dot(hg, wu_ref[...], preferred_element_type=F32).astype(BF16)


def act_body(d_model, keep_ref, recv_ref, sq_ref, sq_recv_ref, a_ref):
    n = a_ref.shape[1]
    r = lax.rsqrt((sq_ref[...] + sq_recv_ref[...]) / d_model + 1e-5)[:1]
    r = jnp.transpose(jnp.broadcast_to(r, (128, BLK)))[:, :1]
    both = ((keep_ref[...].astype(F32) + recv_ref[...].astype(F32)) * r).astype(BF16).astype(F32)
    g, e = both[:, :n], both[:, n:]
    a_ref[...] = (g * jax.nn.sigmoid(g) * e).astype(BF16)


def down_body(h_ref, own_ref, recv_ref, w_ref, send_ref, keep_ref):
    n = own_ref.shape[1]
    h = h_ref[0]
    y = jnp.dot(own_ref[...], w_ref[pl.ds(pl.multiple_of(h * n, n), n), :], preferred_element_type=F32)
    y += jnp.dot(recv_ref[...], w_ref[pl.ds(pl.multiple_of((1 - h) * n, n), n), :], preferred_element_type=F32)
    keep_ref[...] = y[:HALF].astype(BF16)
    send_ref[...] = y[HALF:].astype(BF16)


def solution(mesh):
    def over_hid(t):
        return lax.ppermute(t, 'hid', [(0, 1), (1, 0)])

    def over_x(t):
        return lax.ppermute(t, 'tp', [(0, 2), (2, 0), (1, 3), (3, 1)])

    def over_core(t):
        return lax.ppermute(t, 'tp', [(0, 1), (1, 0), (2, 3), (3, 2)])

    def layer(hidden, rms_attn, rms_mlp, w_q, w_k, w_v, w_o, w_gate, w_up, w_down, k_cache, v_cache, past_len):
        new_len, width = hidden.shape
        d_model = width * 2
        blocks = new_len // BLK
        half_spec = whole(HALF, width)
        h = lax.axis_index('hid').reshape(1)
        c = (lax.axis_index('tp') % 2).reshape(1)
        g1 = rms_attn.reshape(1, width)
        g2 = rms_mlp.reshape(1, width)

        sends, keeps, recvs = [], [], []
        for i in range(blocks):
            send, keep = call(
                qkv_body, (sds(BLK, 512), sds(BLK, 256)), grid=(1,), nscalar=1,
                in_specs=[pl.BlockSpec((BLK, width), lambda *_, i=i: (i, 0)), whole(1, width), whole(*w_q.shape),
                          whole(*w_k.shape), whole(*w_v.shape)],
                out_specs=(whole(BLK, 512), whole(BLK, 256)), flops=2 * BLK * width * 768,
            )(h, hidden, g1, w_q, w_k, w_v)
            sends.append(send)
            keeps.append(keep)
            recvs.append(over_hid(send))

        late_hidden, late_k, late_v, late_pos, _ = lax.optimization_barrier((hidden, k_cache, v_cache, past_len, sends[1]))
        pos_start = late_pos[0]
        x_f32 = late_hidden.astype(F32)
        sq = jnp.sum(x_f32 * x_f32, axis=1)
        r1 = lax.rsqrt((sq + over_hid(sq)) / d_model + 1e-5)
        r1 = jnp.broadcast_to(r1[:, None], (new_len, 128))
        lane = jnp.arange(128)
        positions = (pos_start + jnp.arange(new_len)).astype(F32)
        inv_freq = jnp.exp((lane % 32).astype(F32) * (-2.0 * math.log(ROPE_BASE) / 64))
        angles = positions[:, None] * inv_freq[None, :]
        cos_t = jnp.cos(angles)
        sin_t = jnp.sin(angles) * jnp.where(lane % 64 < 32, -1.0, 1.0)
        k_flat = late_k.reshape(-1, 128)
        v_flat = late_v.reshape(-1, 128)

        def reduce_tp(send, keep, residual, spec):
            part = call(add2_body, sds(HALF, width), grid=(1,), in_specs=[half_spec] * 2, out_specs=half_spec,
                        flops=1 << 20)(keep, over_core(send))
            own = call(add3_body, sds(HALF, width), grid=(1,), nscalar=1, in_specs=[spec, half_spec, half_spec],
                       out_specs=half_spec, flops=1 << 20,
                       )(c, residual, part, over_x(part))
            return own, over_core(own)

        row = lambda i: pl.BlockSpec((BLK, 128), lambda *_: (i, 0))
        prev, kvs, mids = [], [], []
        for i in range(blocks):
            main = PAST_MAX + i * BLK
            o, kv, kh, vh = call(
                functools.partial(att_body, i), (sds(BLK, 256), sds(BLK, 256), sds(BLK, 64), sds(BLK, 64)), grid=(1,), nscalar=2,
                in_specs=[whole(BLK, 512), whole(BLK, 256), whole(BLK, 512), row(i), row(i), row(i),
                          whole(PAST_MAX, 128), whole(PAST_MAX, 128)] + [whole(BLK, 64)] * (2 * i),
                out_specs=(whole(BLK, 256), whole(BLK, 256), whole(BLK, 64), whole(BLK, 64)),
                scratch=[pltpu.VMEM((main, 64), BF16)] * 2, flops=4 * 4 * BLK * (main + BLK) * 64 * 4,
            )(h, past_len, sends[i], keeps[i], recvs[i], r1, cos_t, sin_t, k_flat, v_flat, *prev)
            prev += [kh, vh]
            kvs.append(kv)
            o_recv = over_hid(o)
            send, keep = call(
                wo_body, (sds(HALF, width), sds(HALF, width)), grid=(1,), nscalar=2,
                in_specs=[whole(BLK, 256), whole(BLK, 256), whole(*w_o.shape)],
                out_specs=(half_spec, half_spec), scratch=[pltpu.VMEM((BLK, width), F32)],
                flops=2 * BLK * 512 * width,
            )(h, c, o, o_recv, w_o)
            own_rows = pl.BlockSpec((HALF, width), lambda j, c_ref, i=i: (2 * i + c_ref[0], 0))
            mids.append(reduce_tp(send, keep, hidden, own_rows))

        kv_new = jnp.concatenate(kvs, axis=0)
        k_full = lax.dynamic_update_slice(k_flat, kv_new[:, :128], (pos_start, 0)).reshape(k_cache.shape)
        v_full = lax.dynamic_update_slice(v_flat, kv_new[:, 128:], (pos_start, 0)).reshape(v_cache.shape)

        tile = 512
        cols = w_gate.shape[1] // 2
        steps = cols // tile
        out = None
        for i in range(blocks):
            own, other = mids[i]

            def gate_up(flip):
                def col(j, h_ref):
                    return (0, (h_ref[0] + flip - 2 * flip * h_ref[0]) * steps + j)

                return call(
                    gu_body, (sds(BLK, 2 * cols), sds(8, BLK, dtype=F32))[:1 + flip], grid=(steps,), nscalar=1,
                    in_specs=[half_spec, half_spec, whole(1, width),
                              pl.BlockSpec((width, tile), col), pl.BlockSpec((width, tile), col)],
                    out_specs=(pl.BlockSpec((BLK, 2 * tile), lambda j, *_: (0, j)), whole(8, BLK))[:1 + flip],
                    flops=2 * BLK * width * 2 * cols,
                )(h, own, other, g2, w_gate, w_up)

            gu_send, sq2 = gate_up(1)
            gu_recv = over_hid(gu_send)
            sq2_recv = over_hid(sq2)
            gu_keep, = gate_up(0)
            if i == 1:
                gu_keep, k_full, v_full = lax.optimization_barrier((gu_keep, k_full, v_full))
            a = call(
                functools.partial(act_body, d_model), sds(BLK, cols), grid=(steps,),
                in_specs=[pl.BlockSpec((BLK, 2 * tile), lambda j: (0, j)), pl.BlockSpec((BLK, 2 * tile), lambda j: (0, j)),
                          whole(8, BLK), whole(8, BLK)],
                out_specs=pl.BlockSpec((BLK, tile), lambda j: (0, j)), flops=BLK * cols * 2000,
            )(gu_keep, gu_recv, sq2, sq2_recv)
            a_recv = over_hid(a)
            wide = w_down.shape[1] // 4
            send, keep = call(
                down_body, (sds(HALF, width), sds(HALF, width)), grid=(4,), nscalar=1,
                in_specs=[whole(BLK, cols), whole(BLK, cols), pl.BlockSpec((2 * cols, wide), lambda j, *_: (0, j))],
                out_specs=(pl.BlockSpec((HALF, wide), lambda j, *_: (0, j)), pl.BlockSpec((HALF, wide), lambda j, *_: (0, j))),
                flops=2 * BLK * 2 * cols * width,
            )(h, a, a_recv, w_down)
            fin, fin_other = reduce_tp(send, keep, own, half_spec)
            out = call(
                write_body, sds(new_len, width), grid=(2,), nscalar=1,
                in_specs=[half_spec, half_spec] + ([pl.BlockSpec(memory_space=pl.ANY)] if i else []),
                out_specs=pl.BlockSpec((HALF, width), lambda j, c_ref, i=i: (2 * i + (c_ref[0] + j) % 2, 0)),
                flops=1 << 20, alias={3: 0} if i else None,
            )(c, fin, fin_other, *([out] if i else []))
        return out, k_full, v_full

    row_split = P('hid', 'tp')
    col_split = P('tp', 'hid')
    cache_spec = P('dp', 'tp', None)
    in_specs = (P('dp', 'hid'), P('hid'), P('hid'), row_split, row_split, row_split, col_split,
                row_split, row_split, col_split, cache_spec, cache_spec, P('dp'))
    out_specs = (P('dp', 'hid'), cache_spec, cache_spec)
    return jax.shard_map(layer, mesh=mesh, in_specs=in_specs, out_specs=out_specs, check_vma=False)
```

```python
import math
import jax
import jax.numpy as jnp
from jax import lax
from jax.experimental import pallas as pl
from jax.experimental.pallas import tpu as pltpu
from jax.sharding import PartitionSpec as P

ROPE_BASE = 10000.0
F32, BF16 = jnp.float32, jnp.bfloat16
NEG = -1e30
BLK = 256
HALF = BLK // 2
PAST_MAX = 1024
NB = 4
CH = 4
CW = 256
MESH = pl.DeviceIdType.MESH
NT = (((1,), (1,)), ((), ()))

Q, R, O, C, X, D, T, E, Y, F, G, A = 0, 4, 5, 9, 13, 17, 21, 25, 29, 33, 37, 53
N_REMOTE = 69


def rope(t, cos_t, sin_t):
    width = t.shape[1]
    lane = lax.broadcasted_iota(jnp.int32, t.shape, 1)
    swapped = jnp.where((lane & 63) < 32, pltpu.roll(t, width - 32, 1), pltpu.roll(t, 32, 1))
    cos_w = jnp.concatenate([cos_t] * (width // 128), axis=1)
    sin_w = jnp.concatenate([sin_t] * (width // 128), axis=1)
    return (t * cos_w + swapped * sin_w).astype(BF16)


def row_sums(t):
    sq = jnp.broadcast_to(jnp.sum(t * t, axis=1, keepdims=True), (t.shape[0], 128))
    return jnp.transpose(sq)[:8]


def as_column(row):
    return jnp.transpose(jnp.broadcast_to(row[:1], (128, row.shape[1])))[:, :1]


def kernel(d_model, p_ref, x_hbm, g1_ref, g2_ref, freq_ref, wq_hbm, wk_hbm, wv_hbm, wo_hbm, wg_hbm, wu_hbm, wd_hbm, kc_hbm, vc_hbm,
           out_hbm, ko_hbm, vo_hbm,
           x, wq, wk, wv, wo, wg, wu, wd, kc, vc, qsend, qkeep, qrecv, sq1, sq1r, cos_b, sin_b, kk, vv, qs, kvn, ob, orecv,
           csend, ckeep, crecv, part, xrecv, mid, sq2, sq2r, hg, gsend, gkeep, grecv, ab, arecv, acc,
           esend, ekeep, erecv, part2, yrecv, fin, lsem, osem, ssem, rsem):
    h = lax.axis_index('hid')
    t = lax.axis_index('tp')
    c = lax.rem(t, 2)
    hid_dev = {'hid': 1 - h}
    core_dev = {'tp': t + 1 - 2 * c}
    x_dev = {'tp': lax.rem(t + 2, 4)}
    own = h == 0

    loads = []

    def load(src, dst):
        n = len(loads)
        cp = pltpu.make_async_copy(src, dst, lsem.at[n])
        cp.start()
        loads.append(cp)
        return cp

    ld_x = [load(x_hbm.at[pl.ds(0, BLK)], x.at[pl.ds(0, BLK)])]
    ld_q = [load(wq_hbm, wq), load(wk_hbm, wk), load(wv_hbm, wv)]
    ld_x += [load(x_hbm.at[pl.ds(i * BLK, BLK)], x.at[pl.ds(i * BLK, BLK)]) for i in range(1, NB)]
    ld_kc, ld_vc = load(kc_hbm, kc), load(vc_hbm, vc)
    ld_wo = load(wo_hbm, wo)
    ld_gu = [load(wg_hbm, wg), load(wu_hbm, wu)]
    ld_wd = load(wd_hbm, wd)

    barrier = pltpu.get_barrier_semaphore()
    for dev in (hid_dev, core_dev, x_dev):
        pl.semaphore_signal(barrier, inc=1, device_id=dev, device_id_type=MESH)
    pl.semaphore_wait(barrier, 3)

    def remote(src, dst, n, dev):
        return pltpu.make_async_remote_copy(src_ref=src, dst_ref=dst, send_sem=ssem.at[n], recv_sem=rsem.at[n],
                                            device_id=dev, device_id_type=MESH)

    def q_copy(i): return remote(qsend.at[i], qrecv.at[i], Q + i, hid_dev)
    def r_copy(): return remote(sq1, sq1r, R, hid_dev)
    def o_copy(i): return remote(ob.at[i], orecv.at[i], O + i, hid_dev)
    def c_copy(i): return remote(csend.at[i], crecv.at[i], C + i, core_dev)
    def x_copy(i): return remote(part.at[i], xrecv.at[i], X + i, x_dev)
    def d_copy(i): return remote(mid.at[i, 0], mid.at[i, 1], D + i, core_dev)
    def t_copy(i): return remote(sq2.at[i], sq2r.at[i], T + i, hid_dev)
    def g_copy(i, j): return remote(gsend.at[i, j], grecv.at[i, j], G + CH * i + j, hid_dev)
    def a_copy(i, j): return remote(ab.at[i, j], arecv.at[i, j], A + CH * i + j, hid_dev)
    def e_copy(i): return remote(esend.at[i], erecv.at[i], E + i, core_dev)
    def y_copy(i): return remote(part2.at[i], yrecv.at[i], Y + i, x_dev)
    def f_copy(i): return remote(fin.at[i, 0], fin.at[i, 1], F + i, core_dev)

    def qkv(i):
        xf = x[pl.ds(i * BLK, BLK), :].astype(F32)
        sq1[:, i * BLK:(i + 1) * BLK] = row_sums(xf)
        xg = (xf * g1_ref[...]).astype(BF16)
        q = jnp.dot(xg, wq[...], preferred_element_type=F32).astype(BF16)
        qsend[i, :, :256] = jnp.where(own, q[:, 256:], q[:, :256])
        qkeep[i] = jnp.where(own, q[:, :256], q[:, 256:])
        qsend[i, :, 256:384] = jnp.dot(xg, wk[...], preferred_element_type=F32).astype(BF16)
        qsend[i, :, 384:] = jnp.dot(xg, wv[...], preferred_element_type=F32).astype(BF16)

    def tables(i):
        pos = (p_ref[0] + i * BLK + lax.broadcasted_iota(jnp.int32, (BLK, 128), 0)).astype(F32)
        ang = pos * freq_ref[...]
        lane = lax.broadcasted_iota(jnp.int32, (BLK, 128), 1)
        cos_b[pl.ds(i * BLK, BLK), :] = jnp.cos(ang)
        sin = jnp.sin(ang)
        sin_b[pl.ds(i * BLK, BLK), :] = jnp.where((lane & 63) < 32, -sin, sin)

    def att(i):
        rows = slice(i * BLK, (i + 1) * BLK)
        q_copy(i).wait_recv()
        r = as_column(lax.rsqrt((sq1[:, rows] + sq1r[:, rows]) / d_model + 1e-5))
        cos_t, sin_t = cos_b[rows, :], sin_b[rows, :]
        q = ((qkeep[i].astype(F32) + qrecv[i, :, :256].astype(F32)) * r).astype(BF16)
        kv = ((qsend[i, :, 256:].astype(F32) + qrecv[i, :, 256:].astype(F32)) * r).astype(BF16)
        qs[...] = (rope(q.astype(F32), cos_t, sin_t).astype(F32) * 0.125).astype(BF16)
        k = rope(kv[:, :128].astype(F32), cos_t, sin_t)
        v = kv[:, 128:]
        kvn[rows, :128] = k
        kvn[rows, 128:] = v
        main = PAST_MAX + i * BLK
        kk[main:main + BLK, :] = jnp.where(own, k[:, :64], k[:, 64:])
        vv[main:main + BLK, :] = jnp.where(own, v[:, :64], v[:, 64:])
        col = lax.broadcasted_iota(jnp.int32, (1, main), 1)
        bias = jnp.where((col >= p_ref[0]) & (col < PAST_MAX), NEG, 0.0)
        causal = lax.broadcasted_iota(jnp.int32, (BLK, BLK), 1) <= lax.broadcasted_iota(jnp.int32, (BLK, BLK), 0)

        def pair(n, carry):
            lanes = pl.ds(pl.multiple_of(n * 128, 128), 128)
            qp = qs[:, lanes]
            done = []
            for s in range(2):
                qn = qp[:, s * 64:(s + 1) * 64]
                s_main = lax.dot_general(qn, kk[:main, :], NT, preferred_element_type=F32) + bias
                s_diag = jnp.where(causal, lax.dot_general(qn, kk[main:main + BLK, :], NT, preferred_element_type=F32), NEG)
                top = jnp.maximum(jnp.max(s_main, axis=1, keepdims=True), jnp.max(s_diag, axis=1, keepdims=True))
                e_main = jnp.exp(s_main - top)
                e_diag = jnp.exp(s_diag - top)
                inv = 1.0 / (jnp.sum(e_main, axis=1, keepdims=True) + jnp.sum(e_diag, axis=1, keepdims=True))
                o = jnp.dot((e_main * inv).astype(BF16), vv[:main, :], preferred_element_type=F32)
                o += jnp.dot((e_diag * inv).astype(BF16), vv[main:main + BLK, :], preferred_element_type=F32)
                done.append(o.astype(BF16))
            ob[i, :, lanes] = jnp.concatenate(done, axis=1)
            return carry
        lax.fori_loop(0, 2, pair, 0)
        o_copy(i).start()

    def wo_step(i):
        o_copy(i).wait_recv()
        acc[...] = jnp.dot(ob[i], wo[pl.ds(pl.multiple_of(h * 256, 256), 256), :], preferred_element_type=F32)
        acc[...] += jnp.dot(orecv[i], wo[pl.ds(pl.multiple_of((1 - h) * 256, 256), 256), :], preferred_element_type=F32)
        ckeep[i] = acc[pl.ds(pl.multiple_of(c * HALF, HALF), HALF), :].astype(BF16)
        csend[i] = acc[pl.ds(pl.multiple_of((1 - c) * HALF, HALF), HALF), :].astype(BF16)
        c_copy(i).start()

    def add(a, b):
        return (a.astype(F32) + b.astype(F32)).astype(BF16)

    def c_step(i):
        c_copy(i).wait_recv()
        part[i] = add(ckeep[i], crecv[i])
        x_copy(i).start()

    def x_step(i):
        x_copy(i).wait_recv()
        res = x[pl.ds(pl.multiple_of(i * BLK + c * HALF, HALF), HALF), :]
        mid[i, 0] = add(res, add(part[i], xrecv[i]))
        d_copy(i).start()

    def d_step(i):
        d_copy(i).wait_recv()
        for k in range(2):
            m = mid[i, k].astype(F32)
            sq2[i, :, k * HALF:(k + 1) * HALF] = row_sums(m)
            hg[k * HALF:(k + 1) * HALF, :] = (m * g2_ref[...]).astype(BF16)

    def gate_up(side, j, dst):
        cols = pl.ds(pl.multiple_of(side * (CH * CW) + j * CW, CW), CW)
        dst[:, :CW] = jnp.dot(hg[...], wg[:, cols], preferred_element_type=F32).astype(BF16)
        dst[:, CW:] = jnp.dot(hg[...], wu[:, cols], preferred_element_type=F32).astype(BF16)

    def u_step(i, j):
        gate_up(1 - h, j, gsend.at[i, j])
        g_copy(i, j).start()
        gate_up(h, j, gkeep.at[i % 2, j])

    def v_step(i, j):
        g_copy(i, j).wait_recv()
        r = as_column(lax.rsqrt((sq2[i] + sq2r[i]) / d_model + 1e-5))
        both = ((gkeep[i % 2, j].astype(F32) + grecv[i, j].astype(F32)) * r).astype(BF16).astype(F32)
        g, e = both[:, :CW], both[:, CW:]
        ab[i, j] = (g * jax.nn.sigmoid(g) * e).astype(BF16)
        a_copy(i, j).start()

    def w_step(i, j):
        a_copy(i, j).wait_recv()
        mine = wd[pl.ds(pl.multiple_of(h * (CH * CW) + j * CW, CW), CW), :]
        theirs = wd[pl.ds(pl.multiple_of((1 - h) * (CH * CW) + j * CW, CW), CW), :]
        y = jnp.dot(ab[i, j], mine, preferred_element_type=F32) + jnp.dot(arecv[i, j], theirs, preferred_element_type=F32)
        acc[...] = jnp.where(j == 0, 0.0, acc[...]) + y

    def e_start(i):
        ekeep[i] = acc[:HALF].astype(BF16)
        esend[i] = acc[HALF:].astype(BF16)
        e_copy(i).start()

    def e_step(i):
        e_copy(i).wait_recv()
        part2[i] = add(ekeep[i], erecv[i])
        y_copy(i).start()

    def y_step(i):
        y_copy(i).wait_recv()
        fin[i, 0] = add(mid[i, 0], add(part2[i], yrecv[i]))
        f_copy(i).start()

    def out_copy(i, k):
        at = pl.multiple_of(i * BLK + (c * HALF if k == 0 else (1 - c) * HALF), HALF)
        return pltpu.make_async_copy(fin.at[i, k], out_hbm.at[pl.ds(at, HALF), :], osem.at[2 * i + k])

    def f_step(i):
        out_copy(i, 0).start()
        f_copy(i).wait_recv()
        out_copy(i, 1).start()

    def loop(*steps):
        def body(j, carry):
            for step, i in steps:
                step(i, j)
            return carry
        lax.fori_loop(0, CH, body, 0)

    def cache_rows():
        def tile(n, carry):
            rows = pl.ds(pl.multiple_of(n * BLK, BLK), BLK)
            at = n * BLK - p_ref[0] + lax.broadcasted_iota(jnp.int32, (BLK, NB * BLK), 0)
            pick = jnp.where(at == lax.broadcasted_iota(jnp.int32, (BLK, NB * BLK), 1), 1.0, 0.0).astype(BF16)
            new = jnp.dot(pick, kvn[...], preferred_element_type=F32)
            where = n * BLK - p_ref[0] + lax.broadcasted_iota(jnp.int32, (BLK, 128), 0)
            fresh = (where >= 0) & (where < NB * BLK)
            kc[rows, :] = jnp.where(fresh, new[:, :128], kc[rows, :].astype(F32)).astype(BF16)
            vc[rows, :] = jnp.where(fresh, new[:, 128:], vc[rows, :].astype(F32)).astype(BF16)
            return carry
        lax.fori_loop(0, kc.shape[0] // BLK, tile, 0)

    for cp in ld_q:
        cp.wait()
    for i in range(NB):
        ld_x[i].wait()
        qkv(i)
        if i < 2:
            q_copy(i).start()
    r_copy().start()
    for i in range(NB):
        tables(i)
    ld_kc.wait()
    ld_vc.wait()
    kk[:PAST_MAX, :] = jnp.where(own, kc[:PAST_MAX, :64], kc[:PAST_MAX, 64:])
    vv[:PAST_MAX, :] = jnp.where(own, vc[:PAST_MAX, :64], vc[:PAST_MAX, 64:])
    r_copy().wait_recv()
    att(0)
    q_copy(2).start()
    att(1)
    q_copy(3).start()
    ld_wo.wait()
    wo_step(0)
    c_step(0)
    att(2)
    x_step(0)
    wo_step(1)
    d_step(0)
    for cp in ld_gu:
        cp.wait()
    t_copy(0).start()
    loop((u_step, 0))
    c_step(1)
    att(3)
    x_step(1)
    wo_step(2)
    d_step(1)
    t_copy(1).start()
    t_copy(0).wait_recv()
    c_step(2)
    loop((u_step, 1), (v_step, 0))
    x_step(2)
    wo_step(3)
    c_step(3)
    d_step(2)
    t_copy(2).start()
    t_copy(1).wait_recv()
    ld_wd.wait()
    loop((u_step, 2), (v_step, 1), (w_step, 0))
    e_start(0)
    x_step(3)
    d_step(3)
    t_copy(3).start()
    e_step(0)
    t_copy(2).wait_recv()
    cache_rows()
    ko = pltpu.make_async_copy(kc, ko_hbm, osem.at[8])
    vo = pltpu.make_async_copy(vc, vo_hbm, osem.at[9])
    ko.start()
    vo.start()
    loop((u_step, 3), (v_step, 2), (w_step, 1))
    e_start(1)
    y_step(0)
    e_step(1)
    f_step(0)
    t_copy(3).wait_recv()
    loop((v_step, 3), (w_step, 2))
    e_start(2)
    y_step(1)
    e_step(2)
    f_step(1)
    loop((w_step, 3))
    e_start(3)
    y_step(2)
    e_step(3)
    f_step(2)
    y_step(3)
    f_step(3)

    r_copy().wait_send()
    for i in range(NB):
        for cp in (q_copy, o_copy, c_copy, x_copy, d_copy, t_copy, e_copy, y_copy, f_copy):
            cp(i).wait_send()

        def drain(j, carry, i=i):
            g_copy(i, j).wait_send()
            a_copy(i, j).wait_send()
            return carry
        lax.fori_loop(0, CH, drain, 0)
        out_copy(i, 0).wait()
        out_copy(i, 1).wait()
    ko.wait()
    vo.wait()


def solution(mesh):
    def local_layer(hidden, rms_attn, rms_mlp, w_q, w_k, w_v, w_o, w_gate, w_up, w_down, k_cache, v_cache, past_len):
        new_len, width = hidden.shape
        freq = jnp.exp((jnp.arange(128) % 32).astype(F32) * (-2.0 * math.log(ROPE_BASE) / 64)).reshape(1, 128)
        k_flat = k_cache.reshape(-1, 128)
        v_flat = v_cache.reshape(-1, 128)
        any_spec = pl.BlockSpec(memory_space=pl.ANY)
        vmem_spec = pl.BlockSpec(memory_space=pltpu.VMEM)

        def v(*shape, dtype=BF16):
            return pltpu.VMEM(shape, dtype)
        tok = v(NB, HALF, width)
        scratch = [
            v(new_len, width), v(*w_q.shape), v(*w_k.shape), v(*w_v.shape), v(*w_o.shape), v(*w_gate.shape), v(*w_up.shape), v(*w_down.shape),
            v(*k_flat.shape), v(*v_flat.shape),
            v(NB, BLK, 512), v(NB, BLK, 256), v(NB, BLK, 512), v(8, new_len, dtype=F32), v(8, new_len, dtype=F32),
            v(new_len, 128, dtype=F32), v(new_len, 128, dtype=F32), v(PAST_MAX + new_len, 64), v(PAST_MAX + new_len, 64),
            v(BLK, 256), v(new_len, 256), v(NB, BLK, 256), v(NB, BLK, 256),
            tok, tok, tok, tok, tok, v(NB, 2, HALF, width), v(NB, 8, BLK, dtype=F32), v(NB, 8, BLK, dtype=F32), v(BLK, width),
            v(NB, CH, BLK, 2 * CW), v(2, CH, BLK, 2 * CW), v(NB, CH, BLK, 2 * CW), v(NB, CH, BLK, CW), v(NB, CH, BLK, CW),
            v(BLK, width, dtype=F32),
            tok, tok, tok, tok, tok, v(NB, 2, HALF, width),
            pltpu.SemaphoreType.DMA((13,)), pltpu.SemaphoreType.DMA((10,)),
            pltpu.SemaphoreType.DMA((N_REMOTE,)), pltpu.SemaphoreType.DMA((N_REMOTE,)),
        ]
        out, k_full, v_full = pl.pallas_call(
            lambda *refs: kernel(2 * width, *refs),
            out_shape=(jax.ShapeDtypeStruct((new_len, width), BF16), jax.ShapeDtypeStruct(k_flat.shape, BF16),
                       jax.ShapeDtypeStruct(v_flat.shape, BF16)),
            in_specs=[pl.BlockSpec(memory_space=pltpu.SMEM), any_spec, vmem_spec, vmem_spec, vmem_spec] + [any_spec] * 9,
            out_specs=(any_spec,) * 3,
            scratch_shapes=scratch,
            compiler_params=pltpu.CompilerParams(collective_id=0, has_side_effects=True, vmem_limit_bytes=67043328),
            name="layer",
        )(past_len, hidden, rms_attn.reshape(1, width), rms_mlp.reshape(1, width), freq, w_q, w_k, w_v, w_o, w_gate, w_up, w_down,
          k_flat, v_flat)
        return out, k_full.reshape(k_cache.shape), v_full.reshape(v_cache.shape)

    row_split = P('hid', 'tp')
    col_split = P('tp', 'hid')
    cache_spec = P('dp', 'tp', None)
    in_specs = (P('dp', 'hid'), P('hid'), P('hid'), row_split, row_split, row_split, col_split,
                row_split, row_split, col_split, cache_spec, cache_spec, P('dp'))
    out_specs = (P('dp', 'hid'), cache_spec, cache_spec)
    return jax.shard_map(local_layer, mesh=mesh, in_specs=in_specs, out_specs=out_specs, check_vma=False)
```

```python
import math
import jax
import jax.numpy as jnp
from jax import lax
from jax.experimental import pallas as pl
from jax.experimental.pallas import tpu as pltpu
from jax.sharding import PartitionSpec as P

ROPE_BASE = 10000.0
F32, BF16 = jnp.float32, jnp.bfloat16
NEG = -1e30
BLK = 256
HALF = BLK // 2
PAST_MAX = 1024
NB = 4
CH = 4
CW = 256
MESH = pl.DeviceIdType.MESH

UNITS = ((0, 0, 256), (1, 0, 256), (2, 0, 256), (3, 0, 128), (3, 1, 128))
NU = len(UNITS)
Q, R, O, C, X, D, T = 0, 4, 5, 9, 13, 17, 21
E, Y, F, G = 25, 25 + NU, 25 + 2 * NU, 25 + 3 * NU
A = G + CH * NU
N_REMOTE = A + CH * NU


def rope(t, cos_t, sin_t):
    width = t.shape[1]
    lane = lax.broadcasted_iota(jnp.int32, t.shape, 1)
    swapped = jnp.where((lane & 63) < 32, pltpu.roll(t, width - 32, 1), pltpu.roll(t, 32, 1))
    cos_w = jnp.concatenate([cos_t] * (width // 128), axis=1)
    sin_w = jnp.concatenate([sin_t] * (width // 128), axis=1)
    return (t * cos_w + swapped * sin_w).astype(BF16)


def row_sums(t):
    sq = jnp.broadcast_to(jnp.sum(t * t, axis=1, keepdims=True), (t.shape[0], 128))
    return jnp.transpose(sq)[:8]


def as_column(row):
    return jnp.transpose(jnp.broadcast_to(row[:1], (128, row.shape[1])))[:, :1]


def kernel(d_model, p_ref, x_hbm, g1_ref, g2_ref, wq_hbm, wk_hbm, wv_hbm, wo_hbm, wg_hbm, wu_hbm, wd_hbm, kc_hbm, vc_hbm,
           out_hbm, ko_hbm, vo_hbm,
           x, wq, wk, wv, wo, wg, wu, wd, kc, vc, qsend, qkeep, qrecv, sq1, sq1r, cos_b, sin_b, kt, vv, qs, kvn, ob, orecv,
           csend, ckeep, crecv, part, xrecv, mid, sq2, sq2r, hg, sums, gsend, gkeep, grecv, ab, arecv, acc,
           esend, ekeep, erecv, part2, yrecv, fin, lsem, osem, ssem, rsem):
    h = lax.axis_index('hid')
    t = lax.axis_index('tp')
    c = lax.rem(t, 2)
    hid_dev = {'hid': 1 - h}
    core_dev = {'tp': t + 1 - 2 * c}
    x_dev = {'tp': lax.rem(t + 2, 4)}
    own = h == 0

    loads = []

    def load(src, dst):
        n = len(loads)
        cp = pltpu.make_async_copy(src, dst, lsem.at[n])
        cp.start()
        loads.append(cp)
        return cp

    ld_q = [load(wq_hbm, wq), load(wk_hbm, wk), load(wv_hbm, wv)]
    ld_x = [load(x_hbm.at[pl.ds(i * BLK, BLK)], x.at[pl.ds(i * BLK, BLK)]) for i in range(2)]

    barrier = pltpu.get_barrier_semaphore()
    for dev in (hid_dev, core_dev, x_dev):
        pl.semaphore_signal(barrier, inc=1, device_id=dev, device_id_type=MESH)
    pl.semaphore_wait(barrier, 3)

    def remote(src, dst, n, dev):
        return pltpu.make_async_remote_copy(src_ref=src, dst_ref=dst, send_sem=ssem.at[n], recv_sem=rsem.at[n],
                                            device_id=dev, device_id_type=MESH)

    def q_copy(i): return remote(qsend.at[i], qrecv.at[i], Q + i, hid_dev)
    def r_copy(): return remote(sq1, sq1r, R, hid_dev)
    def o_copy(i): return remote(ob.at[i], orecv.at[i], O + i, hid_dev)
    def c_copy(i): return remote(csend.at[i], crecv.at[i], C + i, core_dev)
    def x_copy(i): return remote(part.at[i], xrecv.at[i], X + i, x_dev)
    def d_copy(i): return remote(mid.at[i, 0], mid.at[i, 1], D + i, core_dev)
    def t_copy(i): return remote(sq2.at[i], sq2r.at[i], T + i, hid_dev)

    def whole(u):
        return pl.ds(UNITS[u][1] * UNITS[u][2], UNITS[u][2])

    def half(u):
        return pl.ds(UNITS[u][1] * UNITS[u][2] // 2, UNITS[u][2] // 2)

    def g_copy(u, j): return remote(gsend.at[UNITS[u][0], j, whole(u)], grecv.at[UNITS[u][0], j, whole(u)], G + CH * u + j, hid_dev)
    def a_copy(u, j): return remote(ab.at[UNITS[u][0], j, whole(u)], arecv.at[UNITS[u][0], j, whole(u)], A + CH * u + j, hid_dev)
    def e_copy(u): return remote(esend.at[UNITS[u][0], half(u)], erecv.at[UNITS[u][0], half(u)], E + u, core_dev)
    def y_copy(u): return remote(part2.at[UNITS[u][0], half(u)], yrecv.at[UNITS[u][0], half(u)], Y + u, x_dev)
    def f_copy(u): return remote(fin.at[UNITS[u][0], 0, half(u)], fin.at[UNITS[u][0], 1, half(u)], F + u, core_dev)

    def qkv(i, send):
        xf = x[pl.ds(i * BLK, BLK), :].astype(F32)
        xg = (xf * g1_ref[...]).astype(BF16)
        theirs = wq[:, pl.ds(pl.multiple_of((1 - h) * 256, 256), 256)]
        qsend[i, :, :256] = jnp.dot(xg, theirs, preferred_element_type=F32).astype(BF16)
        qsend[i, :, 256:384] = jnp.dot(xg, wk[...], preferred_element_type=F32).astype(BF16)
        qsend[i, :, 384:] = jnp.dot(xg, wv[...], preferred_element_type=F32).astype(BF16)
        if send:
            q_copy(i).start()
        mine = wq[:, pl.ds(pl.multiple_of(h * 256, 256), 256)]
        qkeep[i] = jnp.dot(xg, mine, preferred_element_type=F32).astype(BF16)
        sq1[:, i * BLK:(i + 1) * BLK] = row_sums(xf)

    def tables(i):
        pos = (p_ref[0] + i * BLK + lax.broadcasted_iota(jnp.int32, (BLK, 128), 0)).astype(F32)
        lane = lax.broadcasted_iota(jnp.int32, (BLK, 128), 1)
        freq = jnp.exp((lane[:8] & 31).astype(F32) * (-2.0 * math.log(ROPE_BASE) / 64))[:1]
        ang = pos * freq
        cos_b[pl.ds(i * BLK, BLK), :] = jnp.cos(ang)
        sin = jnp.sin(ang)
        sin_b[pl.ds(i * BLK, BLK), :] = jnp.where((lane & 63) < 32, -sin, sin)

    def att(i):
        rows = slice(i * BLK, (i + 1) * BLK)
        q_copy(i).wait_recv()
        r = as_column(lax.rsqrt((sq1[:, rows] + sq1r[:, rows]) / d_model + 1e-5))
        cos_t, sin_t = cos_b[rows, :], sin_b[rows, :]
        q = ((qkeep[i].astype(F32) + qrecv[i, :, :256].astype(F32)) * r).astype(BF16)
        kv = ((qsend[i, :, 256:].astype(F32) + qrecv[i, :, 256:].astype(F32)) * r).astype(BF16)
        qs[...] = (rope(q.astype(F32), cos_t, sin_t).astype(F32) * 0.125).astype(BF16)
        k = rope(kv[:, :128].astype(F32), cos_t, sin_t)
        v = kv[:, 128:]
        k_t = jnp.transpose(k.astype(F32)).astype(BF16)
        kvn[:128, rows] = k_t
        kvn[128:, rows] = jnp.transpose(v.astype(F32)).astype(BF16)
        main = PAST_MAX + i * BLK
        kt[:, main:main + BLK] = jnp.where(own, k_t[:64], k_t[64:])
        vv[main:main + BLK, :] = jnp.where(own, v[:, :64], v[:, 64:])
        col = lax.broadcasted_iota(jnp.int32, (1, main), 1)
        bias = jnp.where((col >= p_ref[0]) & (col < PAST_MAX), NEG, 0.0)
        causal = lax.broadcasted_iota(jnp.int32, (BLK, BLK), 1) <= lax.broadcasted_iota(jnp.int32, (BLK, BLK), 0)

        def pair(n, carry):
            lanes = pl.ds(pl.multiple_of(n * 128, 128), 128)
            qp = qs[:, lanes]
            done = []
            for s in range(2):
                qn = qp[:, s * 64:(s + 1) * 64]
                s_main = jnp.dot(qn, kt[:, :main], preferred_element_type=F32) + bias
                s_diag = jnp.where(causal, jnp.dot(qn, kt[:, main:main + BLK], preferred_element_type=F32), NEG)
                top = jnp.maximum(jnp.max(s_main, axis=1, keepdims=True), jnp.max(s_diag, axis=1, keepdims=True))
                e_main = jnp.exp(s_main - top)
                e_diag = jnp.exp(s_diag - top)
                inv = 1.0 / (jnp.sum(e_main, axis=1, keepdims=True) + jnp.sum(e_diag, axis=1, keepdims=True))
                o = jnp.dot((e_main * inv).astype(BF16), vv[:main, :], preferred_element_type=F32)
                o += jnp.dot((e_diag * inv).astype(BF16), vv[main:main + BLK, :], preferred_element_type=F32)
                done.append(o.astype(BF16))
            ob[i, :, lanes] = jnp.concatenate(done, axis=1)
            return carry
        lax.fori_loop(0, 2, pair, 0)
        o_copy(i).start()

    def wo_step(i):
        o_copy(i).wait_recv()
        acc[...] = jnp.dot(ob[i], wo[pl.ds(pl.multiple_of(h * 256, 256), 256), :], preferred_element_type=F32)
        acc[...] += jnp.dot(orecv[i], wo[pl.ds(pl.multiple_of((1 - h) * 256, 256), 256), :], preferred_element_type=F32)
        ckeep[i] = acc[pl.ds(pl.multiple_of(c * HALF, HALF), HALF), :].astype(BF16)
        csend[i] = acc[pl.ds(pl.multiple_of((1 - c) * HALF, HALF), HALF), :].astype(BF16)
        c_copy(i).start()

    def add(a, b):
        return (a.astype(F32) + b.astype(F32)).astype(BF16)

    def c_step(i):
        c_copy(i).wait_recv()
        part[i] = add(ckeep[i], crecv[i])
        x_copy(i).start()

    def x_step(i):
        x_copy(i).wait_recv()
        res = x[pl.ds(pl.multiple_of(i * BLK + c * HALF, HALF), HALF), :]
        mid[i, 0] = add(res, add(part[i], xrecv[i]))
        d_copy(i).start()

    def d_step(i):
        d_copy(i).wait_recv()
        at = 0
        for u in range(NU):
            if UNITS[u][0] != i:
                continue
            for k in range(2):
                n = UNITS[u][2] // 2
                m = mid[i, k, half(u), :].astype(F32)
                sq = jnp.broadcast_to(jnp.sum(m * m, axis=1, keepdims=True), (n, 128))
                sums[at:at + n, :] = sq
                hg[at:at + n, :] = (m * g2_ref[...]).astype(BF16)
                at += n
        sq2[i] = jnp.transpose(sums[...])[:8]

    def gate_up(u, side, j, dst):
        cols = pl.ds(pl.multiple_of(side * (CH * CW) + j * CW, CW), CW)
        rows = hg[whole(u), :]
        dst[:, :CW] = jnp.dot(rows, wg[:, cols], preferred_element_type=F32).astype(BF16)
        dst[:, CW:] = jnp.dot(rows, wu[:, cols], preferred_element_type=F32).astype(BF16)

    def u_step(u, j):
        i = UNITS[u][0]
        gate_up(u, 1 - h, j, gsend.at[i, j, whole(u)])
        g_copy(u, j).start()
        gate_up(u, h, j, gkeep.at[i % 2, j, whole(u)])

    def v_step(u, j):
        i = UNITS[u][0]
        g_copy(u, j).wait_recv()
        r = as_column(lax.rsqrt((sq2[i, :, whole(u)] + sq2r[i, :, whole(u)]) / d_model + 1e-5))
        both = ((gkeep[i % 2, j, whole(u), :].astype(F32) + grecv[i, j, whole(u), :].astype(F32)) * r).astype(BF16).astype(F32)
        g, e = both[:, :CW], both[:, CW:]
        ab[i, j, whole(u), :] = (g * jax.nn.sigmoid(g) * e).astype(BF16)
        a_copy(u, j).start()

    def w_step(u, j):
        i = UNITS[u][0]
        a_copy(u, j).wait_recv()
        mine = wd[pl.ds(pl.multiple_of(h * (CH * CW) + j * CW, CW), CW), :]
        theirs = wd[pl.ds(pl.multiple_of((1 - h) * (CH * CW) + j * CW, CW), CW), :]
        y = jnp.dot(ab[i, j, whole(u), :], mine, preferred_element_type=F32)
        y += jnp.dot(arecv[i, j, whole(u), :], theirs, preferred_element_type=F32)
        acc[whole(u), :] = jnp.where(j == 0, 0.0, acc[whole(u), :]) + y

    def e_start(u):
        i, k, n = UNITS[u]
        ekeep[i, half(u), :] = acc[k * n:k * n + n // 2, :].astype(BF16)
        esend[i, half(u), :] = acc[k * n + n // 2:k * n + n, :].astype(BF16)
        e_copy(u).start()

    def e_step(u):
        i = UNITS[u][0]
        e_copy(u).wait_recv()
        part2[i, half(u), :] = add(ekeep[i, half(u), :], erecv[i, half(u), :])
        y_copy(u).start()

    def y_step(u):
        i = UNITS[u][0]
        y_copy(u).wait_recv()
        down = add(part2[i, half(u), :], yrecv[i, half(u), :])
        fin[i, 0, half(u), :] = add(mid[i, 0, half(u), :], down)
        f_copy(u).start()

    def out_copy(u, k):
        i, part_no, n = UNITS[u]
        at = pl.multiple_of(i * BLK + (c if k == 0 else 1 - c) * HALF + part_no * (n // 2), 64)
        return pltpu.make_async_copy(fin.at[i, k, half(u)], out_hbm.at[pl.ds(at, n // 2), :], osem.at[2 * u + k])

    def f_step(u):
        out_copy(u, 0).start()
        f_copy(u).wait_recv()
        out_copy(u, 1).start()

    def loop(*steps):
        def body(j, carry):
            for step, i in steps:
                step(i, j)
            return carry
        lax.fori_loop(0, CH, body, 0)

    def cache_rows():
        def tile(n, carry):
            cols = pl.ds(pl.multiple_of(n * BLK, BLK), BLK)
            at = n * BLK - p_ref[0] + lax.broadcasted_iota(jnp.int32, (NB * BLK, BLK), 1)
            pick = jnp.where(at == lax.broadcasted_iota(jnp.int32, (NB * BLK, BLK), 0), 1.0, 0.0).astype(BF16)
            new = jnp.dot(kvn[...], pick, preferred_element_type=F32)
            where = n * BLK - p_ref[0] + lax.broadcasted_iota(jnp.int32, (128, BLK), 1)
            fresh = (where >= 0) & (where < NB * BLK)
            kc[:, cols] = jnp.where(fresh, new[:128], kc[:, cols].astype(F32)).astype(BF16)
            vc[:, cols] = jnp.where(fresh, new[128:], vc[:, cols].astype(F32)).astype(BF16)
            return carry
        lax.fori_loop(0, kc.shape[1] // BLK, tile, 0)

    for cp in ld_q:
        cp.wait()
    ld_x[0].wait()
    qkv(0, True)
    ld_x += [load(x_hbm.at[pl.ds(i * BLK, BLK)], x.at[pl.ds(i * BLK, BLK)]) for i in range(2, NB)]
    ld_kc, ld_vc = load(kc_hbm, kc), load(vc_hbm, vc)
    ld_wo = load(wo_hbm, wo)
    ld_gu = [load(wg_hbm, wg), load(wu_hbm, wu)]
    ld_wd = load(wd_hbm, wd)
    for i in range(1, NB):
        ld_x[i].wait()
        qkv(i, i < 2)
    r_copy().start()
    for i in range(NB):
        tables(i)
    ld_kc.wait()
    ld_vc.wait()
    kt[:, :PAST_MAX] = kc[pl.ds(pl.multiple_of(h * 64, 64), 64), :PAST_MAX]
    v_old = jnp.transpose(vc[:, :PAST_MAX].astype(F32)).astype(BF16)
    vv[:PAST_MAX, :] = jnp.where(own, v_old[:, :64], v_old[:, 64:])
    r_copy().wait_recv()
    att(0)
    q_copy(2).start()
    att(1)
    q_copy(3).start()
    ld_wo.wait()
    wo_step(0)
    c_step(0)
    att(2)
    x_step(0)
    wo_step(1)
    d_step(0)
    for cp in ld_gu:
        cp.wait()
    t_copy(0).start()
    loop((u_step, 0))
    c_step(1)
    att(3)
    x_step(1)
    wo_step(2)
    d_step(1)
    t_copy(1).start()
    t_copy(0).wait_recv()
    c_step(2)
    loop((u_step, 1), (v_step, 0))
    x_step(2)
    wo_step(3)
    c_step(3)
    d_step(2)
    t_copy(2).start()
    t_copy(1).wait_recv()
    ld_wd.wait()
    loop((u_step, 2), (v_step, 1), (w_step, 0))
    e_start(0)
    x_step(3)
    d_step(3)
    t_copy(3).start()
    e_step(0)
    t_copy(2).wait_recv()
    cache_rows()
    ko = pltpu.make_async_copy(kc, ko_hbm, osem.at[2 * NU])
    vo = pltpu.make_async_copy(vc, vo_hbm, osem.at[2 * NU + 1])
    ko.start()
    vo.start()
    loop((u_step, 3), (v_step, 2), (w_step, 1))
    loop((u_step, 4))
    e_start(1)
    y_step(0)
    e_step(1)
    f_step(0)
    t_copy(3).wait_recv()
    loop((v_step, 3), (w_step, 2))
    e_start(2)
    y_step(1)
    e_step(2)
    f_step(1)
    loop((v_step, 4))
    y_step(2)
    loop((w_step, 3))
    e_start(3)
    f_step(2)
    w_step(4, 0)
    e_step(3)
    for j in range(1, CH):
        w_step(4, j)
    e_start(4)
    y_step(3)
    e_step(4)
    f_step(3)
    y_step(4)
    f_step(4)

    r_copy().wait_send()
    for i in range(NB):
        for cp in (q_copy, o_copy, c_copy, x_copy, d_copy, t_copy):
            cp(i).wait_send()
    for u in range(NU):
        for cp in (e_copy, y_copy, f_copy):
            cp(u).wait_send()

        def drain(j, carry, u=u):
            g_copy(u, j).wait_send()
            a_copy(u, j).wait_send()
            return carry
        lax.fori_loop(0, CH, drain, 0)
        out_copy(u, 0).wait()
        out_copy(u, 1).wait()
    ko.wait()
    vo.wait()


def results_body(pieces, *refs):
    n = len(pieces)
    srcs, dsts, bufs, isem, osem = refs[:3], refs[3:6], refs[6:9], refs[9], refs[10]

    def read(k):
        a, start, size = pieces[k]
        part = pl.ds(start, size)
        return pltpu.make_async_copy(srcs[a].at[part], bufs[a].at[part], isem.at[k])

    def write(k):
        a, start, size = pieces[k]
        part = pl.ds(start, size)
        return pltpu.make_async_copy(bufs[a].at[part], dsts[a].at[part], osem.at[k])
    for k in range(n):
        read(k).start()
    for k in range(n):
        read(k).wait()
        write(k).start()
    for k in range(n):
        write(k).wait()


def solution(mesh):
    def local_layer(hidden, rms_attn, rms_mlp, w_q, w_k, w_v, w_o, w_gate, w_up, w_down, k_cache, v_cache, past_len):
        new_len, width = hidden.shape
        tokens = k_cache.shape[0]
        k_flat = k_cache.transpose(1, 2, 0).reshape(-1, tokens)
        v_flat = v_cache.transpose(1, 2, 0).reshape(-1, tokens)
        any_spec = pl.BlockSpec(memory_space=pl.ANY)
        vmem_spec = pl.BlockSpec(memory_space=pltpu.VMEM)

        def v(*shape, dtype=BF16):
            return pltpu.VMEM(shape, dtype)
        tok = v(NB, HALF, width)
        scratch = [
            v(new_len, width), v(*w_q.shape), v(*w_k.shape), v(*w_v.shape), v(*w_o.shape), v(*w_gate.shape), v(*w_up.shape), v(*w_down.shape),
            v(*k_flat.shape), v(*v_flat.shape),
            v(NB, BLK, 512), v(NB, BLK, 256), v(NB, BLK, 512), v(8, new_len, dtype=F32), v(8, new_len, dtype=F32),
            v(new_len, 128, dtype=F32), v(new_len, 128, dtype=F32), v(64, PAST_MAX + new_len), v(PAST_MAX + new_len, 64),
            v(BLK, 256), v(256, new_len), v(NB, BLK, 256), v(NB, BLK, 256),
            tok, tok, tok, tok, tok, v(NB, 2, HALF, width), v(NB, 8, BLK, dtype=F32), v(NB, 8, BLK, dtype=F32), v(BLK, width), v(BLK, 128, dtype=F32),
            v(NB, CH, BLK, 2 * CW), v(2, CH, BLK, 2 * CW), v(NB, CH, BLK, 2 * CW), v(NB, CH, BLK, CW), v(NB, CH, BLK, CW),
            v(BLK, width, dtype=F32),
            tok, tok, tok, tok, tok, v(NB, 2, HALF, width),
            pltpu.SemaphoreType.DMA((13,)), pltpu.SemaphoreType.DMA((2 * NU + 2,)),
            pltpu.SemaphoreType.DMA((N_REMOTE,)), pltpu.SemaphoreType.DMA((N_REMOTE,)),
        ]
        shapes = tuple(jax.ShapeDtypeStruct(a, BF16) for a in (hidden.shape, k_flat.shape, v_flat.shape))
        done = pl.pallas_call(
            lambda *refs: kernel(2 * width, *refs),
            out_shape=shapes,
            in_specs=[pl.BlockSpec(memory_space=pltpu.SMEM), any_spec, vmem_spec, vmem_spec] + [any_spec] * 9,
            out_specs=(any_spec,) * 3,
            scratch_shapes=scratch,
            compiler_params=pltpu.CompilerParams(collective_id=0, has_side_effects=True, vmem_limit_bytes=67043328),
            name="layer",
        )(past_len, hidden, rms_attn.reshape(1, width), rms_mlp.reshape(1, width), w_q, w_k, w_v, w_o, w_gate, w_up, w_down,
          k_flat, v_flat)
        pieces = [(0, k * 128, 128) for k in range(new_len // 128)] + [(a, k * 64, 64) for a in (1, 2) for k in range(2)]
        out, k_full, v_full = pl.pallas_call(
            lambda *refs: results_body(pieces, *refs),
            out_shape=shapes, in_specs=[any_spec] * 3, out_specs=(any_spec,) * 3,
            scratch_shapes=[v(*a.shape) for a in shapes] + [pltpu.SemaphoreType.DMA((len(pieces),))] * 2,
            compiler_params=pltpu.CompilerParams(vmem_limit_bytes=60 << 20),
            name="results",
        )(*done)
        heads, dim = k_cache.shape[1:]
        return (out, k_full.reshape(heads, dim, tokens).transpose(2, 0, 1), v_full.reshape(heads, dim, tokens).transpose(2, 0, 1))

    row_split = P('hid', 'tp')
    col_split = P('tp', 'hid')
    cache_spec = P('dp', 'tp', None)
    in_specs = (P('dp', 'hid'), P('hid'), P('hid'), row_split, row_split, row_split, col_split,
                row_split, row_split, col_split, cache_spec, cache_spec, P('dp'))
    out_specs = (P('dp', 'hid'), cache_spec, cache_spec)
    return jax.shard_map(local_layer, mesh=mesh, in_specs=in_specs, out_specs=out_specs, check_vma=False)
```

```python
import math
import jax
import jax.numpy as jnp
from jax import lax
from jax.experimental import pallas as pl
from jax.experimental.pallas import tpu as pltpu
from jax.sharding import PartitionSpec as P

ROPE_BASE = 10000.0
F32, BF16 = jnp.float32, jnp.bfloat16
NEG = -1e30
BLK = 256
HALF = BLK // 2
PAST_MAX = 1024
NB = 4
CH = 4
CW = 256
MESH = pl.DeviceIdType.MESH

UNITS = ((0, 0, 256), (1, 0, 256), (2, 0, 256), (3, 0, 128), (3, 1, 128))
NU = len(UNITS)
Q, R, O, C, X, D, T = 0, 4, 8, 12, 16, 20, 24
E, Y, F, G = 28, 28 + NU, 28 + 2 * NU, 28 + 3 * NU
A = G + CH * NU
N_REMOTE = A + CH * NU


def rope(t, cos_t, sin_t):
    width = t.shape[1]
    lane = lax.broadcasted_iota(jnp.int32, t.shape, 1)
    swapped = jnp.where((lane & 63) < 32, pltpu.roll(t, width - 32, 1), pltpu.roll(t, 32, 1))
    cos_w = jnp.concatenate([cos_t] * (width // 128), axis=1)
    sin_w = jnp.concatenate([sin_t] * (width // 128), axis=1)
    return (t * cos_w + swapped * sin_w).astype(BF16)


def row_sums(t):
    sq = jnp.broadcast_to(jnp.sum(t * t, axis=1, keepdims=True), (t.shape[0], 128))
    return jnp.transpose(sq)[:8]


def as_column(row):
    return jnp.transpose(jnp.broadcast_to(row[:1], (128, row.shape[1])))[:, :1]


def kernel(d_model, p_hbm, x_hbm, g1_hbm, g2_hbm, wq_hbm, wk_hbm, wv_hbm, wo_hbm, wg_hbm, wu_hbm, wd_hbm, kc_hbm, vc_hbm,
           out_hbm, ko_hbm, vo_hbm,
           p_ref, g1_ref, g2_ref, x, wq, wk, wv, wo, wg, wu, wd, kc, vc, qsend, qkeep, qrecv, sq1, sq1r, cos_b, sin_b, kt, vv, qs, kvn, ob, orecv,
           csend, ckeep, crecv, part, xrecv, mid, sq2, sq2r, hg, sums, gsend, gkeep, grecv, ab, arecv, acc,
           esend, ekeep, erecv, part2, yrecv, fin, lsem, osem, ssem, rsem):
    h = lax.axis_index('hid')
    t = lax.axis_index('tp')
    c = lax.rem(t, 2)
    hid_dev = {'hid': 1 - h}
    core_dev = {'tp': t + 1 - 2 * c}
    x_dev = {'tp': lax.rem(t + 2, 4)}
    own = h == 0

    loads = []

    def load(src, dst):
        n = len(loads)
        cp = pltpu.make_async_copy(src, dst, lsem.at[n])
        cp.start()
        loads.append(cp)
        return cp

    ld_x = [load(x_hbm.at[pl.ds(0, BLK)], x.at[pl.ds(0, BLK)])]
    ld_q = [load(g1_hbm, g1_ref), load(wq_hbm, wq), load(wk_hbm, wk), load(wv_hbm, wv)]
    ld_x += [load(x_hbm.at[pl.ds(BLK, BLK)], x.at[pl.ds(BLK, BLK)])]
    ld_small = [load(p_hbm, p_ref), load(g2_hbm, g2_ref)]

    barrier = pltpu.get_barrier_semaphore()
    for dev in (hid_dev, core_dev, x_dev):
        pl.semaphore_signal(barrier, inc=1, device_id=dev, device_id_type=MESH)
    pl.semaphore_wait(barrier, 3)

    def remote(src, dst, n, dev):
        return pltpu.make_async_remote_copy(src_ref=src, dst_ref=dst, send_sem=ssem.at[n], recv_sem=rsem.at[n],
                                            device_id=dev, device_id_type=MESH)

    def q_copy(i): return remote(qsend.at[i], qrecv.at[i], Q + i, hid_dev)
    def r_copy(i): return remote(sq1.at[i], sq1r.at[i], R + i, hid_dev)
    def o_copy(i): return remote(ob.at[i], orecv.at[i], O + i, hid_dev)
    def c_copy(i): return remote(csend.at[i], crecv.at[i], C + i, core_dev)
    def x_copy(i): return remote(part.at[i], xrecv.at[i], X + i, x_dev)
    def d_copy(i): return remote(mid.at[i, 0], mid.at[i, 1], D + i, core_dev)
    def t_copy(i): return remote(sq2.at[i], sq2r.at[i], T + i, hid_dev)

    def whole(u):
        return pl.ds(UNITS[u][1] * UNITS[u][2], UNITS[u][2])

    def half(u):
        return pl.ds(UNITS[u][1] * UNITS[u][2] // 2, UNITS[u][2] // 2)

    def g_copy(u, j): return remote(gsend.at[UNITS[u][0], j, whole(u)], grecv.at[UNITS[u][0], j, whole(u)], G + CH * u + j, hid_dev)
    def a_copy(u, j): return remote(ab.at[UNITS[u][0], j, whole(u)], arecv.at[UNITS[u][0], j, whole(u)], A + CH * u + j, hid_dev)
    def e_copy(u): return remote(esend.at[UNITS[u][0], half(u)], erecv.at[UNITS[u][0], half(u)], E + u, core_dev)
    def y_copy(u): return remote(part2.at[UNITS[u][0], half(u)], yrecv.at[UNITS[u][0], half(u)], Y + u, x_dev)
    def f_copy(u): return remote(fin.at[UNITS[u][0], 0, half(u)], fin.at[UNITS[u][0], 1, half(u)], F + u, core_dev)

    def qkv(i, send):
        xf = x[pl.ds(i * BLK, BLK), :].astype(F32)
        xg = (xf * g1_ref[...]).astype(BF16)
        theirs = wq[:, pl.ds(pl.multiple_of((1 - h) * 256, 256), 256)]
        qsend[i, :, :256] = jnp.dot(xg, theirs, preferred_element_type=F32).astype(BF16)
        qsend[i, :, 256:384] = jnp.dot(xg, wk[...], preferred_element_type=F32).astype(BF16)
        qsend[i, :, 384:] = jnp.dot(xg, wv[...], preferred_element_type=F32).astype(BF16)
        if send:
            q_copy(i).start()
        mine = wq[:, pl.ds(pl.multiple_of(h * 256, 256), 256)]
        qkeep[i] = jnp.dot(xg, mine, preferred_element_type=F32).astype(BF16)
        sq1[i] = row_sums(xf)
        if send:
            r_copy(i).start()

    def tables(i):
        pos = (p_ref[0] + i * BLK + lax.broadcasted_iota(jnp.int32, (BLK, 128), 0)).astype(F32)
        lane = lax.broadcasted_iota(jnp.int32, (BLK, 128), 1)
        freq = jnp.exp((lane[:8] & 31).astype(F32) * (-2.0 * math.log(ROPE_BASE) / 64))[:1]
        ang = pos * freq
        cos_b[pl.ds(i * BLK, BLK), :] = jnp.cos(ang)
        sin = jnp.sin(ang)
        sin_b[pl.ds(i * BLK, BLK), :] = jnp.where((lane & 63) < 32, -sin, sin)

    def att(i):
        rows = slice(i * BLK, (i + 1) * BLK)
        q_copy(i).wait_recv()
        r_copy(i).wait_recv()
        r = as_column(lax.rsqrt((sq1[i] + sq1r[i]) / d_model + 1e-5))
        cos_t, sin_t = cos_b[rows, :], sin_b[rows, :]
        q = ((qkeep[i].astype(F32) + qrecv[i, :, :256].astype(F32)) * r).astype(BF16)
        kv = ((qsend[i, :, 256:].astype(F32) + qrecv[i, :, 256:].astype(F32)) * r).astype(BF16)
        qs[...] = (rope(q.astype(F32), cos_t, sin_t).astype(F32) * 0.125).astype(BF16)
        k = rope(kv[:, :128].astype(F32), cos_t, sin_t)
        v = kv[:, 128:]
        k_t = jnp.transpose(k.astype(F32)).astype(BF16)
        kvn[:128, rows] = k_t
        kvn[128:, rows] = jnp.transpose(v.astype(F32)).astype(BF16)
        main = PAST_MAX + i * BLK
        kt[:, main:main + BLK] = jnp.where(own, k_t[:64], k_t[64:])
        vv[main:main + BLK, :] = jnp.where(own, v[:, :64], v[:, 64:])
        col = lax.broadcasted_iota(jnp.int32, (1, main), 1)
        bias = jnp.where((col >= p_ref[0]) & (col < PAST_MAX), NEG, 0.0)
        causal = lax.broadcasted_iota(jnp.int32, (BLK, BLK), 1) <= lax.broadcasted_iota(jnp.int32, (BLK, BLK), 0)

        def pair(n, carry):
            lanes = pl.ds(pl.multiple_of(n * 128, 128), 128)
            qp = qs[:, lanes]
            done = []
            for s in range(2):
                qn = qp[:, s * 64:(s + 1) * 64]
                s_main = jnp.dot(qn, kt[:, :main], preferred_element_type=F32) + bias
                s_diag = jnp.where(causal, jnp.dot(qn, kt[:, main:main + BLK], preferred_element_type=F32), NEG)
                top = jnp.maximum(jnp.max(s_main, axis=1, keepdims=True), jnp.max(s_diag, axis=1, keepdims=True))
                e_main = jnp.exp(s_main - top)
                e_diag = jnp.exp(s_diag - top)
                inv = 1.0 / (jnp.sum(e_main, axis=1, keepdims=True) + jnp.sum(e_diag, axis=1, keepdims=True))
                o = jnp.dot((e_main * inv).astype(BF16), vv[:main, :], preferred_element_type=F32)
                o += jnp.dot((e_diag * inv).astype(BF16), vv[main:main + BLK, :], preferred_element_type=F32)
                done.append(o.astype(BF16))
            ob[i, :, lanes] = jnp.concatenate(done, axis=1)
            return carry
        lax.fori_loop(0, 2, pair, 0)
        o_copy(i).start()

    def wo_step(i):
        o_copy(i).wait_recv()
        acc[...] = jnp.dot(ob[i], wo[pl.ds(pl.multiple_of(h * 256, 256), 256), :], preferred_element_type=F32)
        acc[...] += jnp.dot(orecv[i], wo[pl.ds(pl.multiple_of((1 - h) * 256, 256), 256), :], preferred_element_type=F32)
        ckeep[i] = acc[pl.ds(pl.multiple_of(c * HALF, HALF), HALF), :].astype(BF16)
        csend[i] = acc[pl.ds(pl.multiple_of((1 - c) * HALF, HALF), HALF), :].astype(BF16)
        c_copy(i).start()

    def add(a, b):
        return (a.astype(F32) + b.astype(F32)).astype(BF16)

    def c_step(i):
        c_copy(i).wait_recv()
        part[i] = add(ckeep[i], crecv[i])
        x_copy(i).start()

    def x_step(i):
        x_copy(i).wait_recv()
        res = x[pl.ds(pl.multiple_of(i * BLK + c * HALF, HALF), HALF), :]
        mid[i, 0] = add(res, add(part[i], xrecv[i]))
        d_copy(i).start()

    def d_step(i):
        d_copy(i).wait_recv()
        at = 0
        for u in range(NU):
            if UNITS[u][0] != i:
                continue
            for k in range(2):
                n = UNITS[u][2] // 2
                m = mid[i, k, half(u), :].astype(F32)
                sq = jnp.broadcast_to(jnp.sum(m * m, axis=1, keepdims=True), (n, 128))
                sums[at:at + n, :] = sq
                hg[at:at + n, :] = (m * g2_ref[...]).astype(BF16)
                at += n
        sq2[i] = jnp.transpose(sums[...])[:8]

    def gate_up(u, side, j, dst):
        cols = pl.ds(pl.multiple_of(side * (CH * CW) + j * CW, CW), CW)
        rows = hg[whole(u), :]
        dst[:, :CW] = jnp.dot(rows, wg[:, cols], preferred_element_type=F32).astype(BF16)
        dst[:, CW:] = jnp.dot(rows, wu[:, cols], preferred_element_type=F32).astype(BF16)

    def u_step(u, j):
        i = UNITS[u][0]
        gate_up(u, 1 - h, j, gsend.at[i, j, whole(u)])
        g_copy(u, j).start()
        gate_up(u, h, j, gkeep.at[i % 2, j, whole(u)])

    def v_step(u, j):
        i = UNITS[u][0]
        g_copy(u, j).wait_recv()
        r = as_column(lax.rsqrt((sq2[i, :, whole(u)] + sq2r[i, :, whole(u)]) / d_model + 1e-5))
        both = ((gkeep[i % 2, j, whole(u), :].astype(F32) + grecv[i, j, whole(u), :].astype(F32)) * r).astype(BF16).astype(F32)
        g, e = both[:, :CW], both[:, CW:]
        ab[i, j, whole(u), :] = (g * jax.nn.sigmoid(g) * e).astype(BF16)
        a_copy(u, j).start()

    def w_step(u, j):
        i = UNITS[u][0]
        a_copy(u, j).wait_recv()
        mine = wd[pl.ds(pl.multiple_of(h * (CH * CW) + j * CW, CW), CW), :]
        theirs = wd[pl.ds(pl.multiple_of((1 - h) * (CH * CW) + j * CW, CW), CW), :]
        y = jnp.dot(ab[i, j, whole(u), :], mine, preferred_element_type=F32)
        y += jnp.dot(arecv[i, j, whole(u), :], theirs, preferred_element_type=F32)
        acc[whole(u), :] = jnp.where(j == 0, 0.0, acc[whole(u), :]) + y

    def e_start(u):
        i, k, n = UNITS[u]
        ekeep[i, half(u), :] = acc[k * n:k * n + n // 2, :].astype(BF16)
        esend[i, half(u), :] = acc[k * n + n // 2:k * n + n, :].astype(BF16)
        e_copy(u).start()

    def e_step(u):
        i = UNITS[u][0]
        e_copy(u).wait_recv()
        part2[i, half(u), :] = add(ekeep[i, half(u), :], erecv[i, half(u), :])
        y_copy(u).start()

    def y_step(u):
        i = UNITS[u][0]
        y_copy(u).wait_recv()
        down = add(part2[i, half(u), :], yrecv[i, half(u), :])
        fin[i, 0, half(u), :] = add(mid[i, 0, half(u), :], down)
        f_copy(u).start()

    def out_copy(u, k):
        i, part_no, n = UNITS[u]
        at = pl.multiple_of(i * BLK + (c if k == 0 else 1 - c) * HALF + part_no * (n // 2), 64)
        return pltpu.make_async_copy(fin.at[i, k, half(u)], out_hbm.at[pl.ds(at, n // 2), :], osem.at[2 * u + k])

    def f_step(u):
        out_copy(u, 0).start()
        f_copy(u).wait_recv()
        out_copy(u, 1).start()

    def loop(*steps):
        def body(j, carry):
            for step, i in steps:
                step(i, j)
            return carry
        lax.fori_loop(0, CH, body, 0)

    def cache_rows():
        def tile(n, carry):
            cols = pl.ds(pl.multiple_of(n * BLK, BLK), BLK)
            at = n * BLK - p_ref[0] + lax.broadcasted_iota(jnp.int32, (NB * BLK, BLK), 1)
            pick = jnp.where(at == lax.broadcasted_iota(jnp.int32, (NB * BLK, BLK), 0), 1.0, 0.0).astype(BF16)
            new = jnp.dot(kvn[...], pick, preferred_element_type=F32)
            where = n * BLK - p_ref[0] + lax.broadcasted_iota(jnp.int32, (128, BLK), 1)
            fresh = (where >= 0) & (where < NB * BLK)
            kc[:, cols] = jnp.where(fresh, new[:128], kc[:, cols].astype(F32)).astype(BF16)
            vc[:, cols] = jnp.where(fresh, new[128:], vc[:, cols].astype(F32)).astype(BF16)
            return carry
        lax.fori_loop(0, kc.shape[1] // BLK, tile, 0)

    for cp in ld_q:
        cp.wait()
    ld_x[0].wait()
    qkv(0, True)
    ld_x += [load(x_hbm.at[pl.ds(i * BLK, BLK)], x.at[pl.ds(i * BLK, BLK)]) for i in range(2, NB)]
    ld_kc, ld_vc = load(kc_hbm, kc), load(vc_hbm, vc)
    ld_wo = load(wo_hbm, wo)
    ld_gu = [load(wg_hbm, wg), load(wu_hbm, wu)]
    ld_wd = load(wd_hbm, wd)
    for i in range(1, NB):
        ld_x[i].wait()
        qkv(i, i < 2)
    for cp in ld_small:
        cp.wait()
    for i in range(NB):
        tables(i)
    ld_kc.wait()
    ld_vc.wait()
    kt[:, :PAST_MAX] = kc[pl.ds(pl.multiple_of(h * 64, 64), 64), :PAST_MAX]
    v_old = jnp.transpose(vc[:, :PAST_MAX].astype(F32)).astype(BF16)
    vv[:PAST_MAX, :] = jnp.where(own, v_old[:, :64], v_old[:, 64:])
    att(0)
    q_copy(2).start()
    r_copy(2).start()
    att(1)
    q_copy(3).start()
    r_copy(3).start()
    ld_wo.wait()
    wo_step(0)
    c_step(0)
    att(2)
    x_step(0)
    wo_step(1)
    d_step(0)
    for cp in ld_gu:
        cp.wait()
    t_copy(0).start()
    loop((u_step, 0))
    c_step(1)
    att(3)
    x_step(1)
    wo_step(2)
    d_step(1)
    t_copy(1).start()
    t_copy(0).wait_recv()
    c_step(2)
    loop((u_step, 1), (v_step, 0))
    x_step(2)
    wo_step(3)
    c_step(3)
    d_step(2)
    t_copy(2).start()
    t_copy(1).wait_recv()
    ld_wd.wait()
    loop((u_step, 2), (v_step, 1), (w_step, 0))
    e_start(0)
    x_step(3)
    d_step(3)
    t_copy(3).start()
    e_step(0)
    t_copy(2).wait_recv()
    cache_rows()
    ko = pltpu.make_async_copy(kc, ko_hbm, osem.at[2 * NU])
    vo = pltpu.make_async_copy(vc, vo_hbm, osem.at[2 * NU + 1])
    ko.start()
    vo.start()
    loop((u_step, 3), (v_step, 2), (w_step, 1))
    loop((u_step, 4))
    e_start(1)
    y_step(0)
    e_step(1)
    f_step(0)
    t_copy(3).wait_recv()
    loop((v_step, 3), (w_step, 2))
    e_start(2)
    y_step(1)
    e_step(2)
    f_step(1)
    loop((v_step, 4))
    y_step(2)
    loop((w_step, 3))
    e_start(3)
    f_step(2)
    w_step(4, 0)
    e_step(3)
    for j in range(1, CH):
        w_step(4, j)
    e_start(4)
    y_step(3)
    e_step(4)
    f_step(3)
    y_step(4)
    f_step(4)

    for i in range(NB):
        for cp in (q_copy, r_copy, o_copy, c_copy, x_copy, d_copy, t_copy):
            cp(i).wait_send()
    for u in range(NU):
        for cp in (e_copy, y_copy, f_copy):
            cp(u).wait_send()

        def drain(j, carry, u=u):
            g_copy(u, j).wait_send()
            a_copy(u, j).wait_send()
            return carry
        lax.fori_loop(0, CH, drain, 0)
        out_copy(u, 0).wait()
        out_copy(u, 1).wait()
    ko.wait()
    vo.wait()


def results_body(pieces, *refs):
    n = len(pieces)
    srcs, dsts, bufs, isem, osem = refs[:3], refs[3:6], refs[6:9], refs[9], refs[10]

    def read(k):
        a, start, size = pieces[k]
        part = pl.ds(start, size)
        return pltpu.make_async_copy(srcs[a].at[part], bufs[a].at[part], isem.at[k])

    def write(k):
        a, start, size = pieces[k]
        part = pl.ds(start, size)
        return pltpu.make_async_copy(bufs[a].at[part], dsts[a].at[part], osem.at[k])
    for k in range(n):
        read(k).start()
    for k in range(n):
        read(k).wait()
        write(k).start()
    for k in range(n):
        write(k).wait()


def solution(mesh):
    def local_layer(hidden, rms_attn, rms_mlp, w_q, w_k, w_v, w_o, w_gate, w_up, w_down, k_cache, v_cache, past_len):
        new_len, width = hidden.shape
        tokens = k_cache.shape[0]
        k_flat = k_cache.transpose(1, 2, 0).reshape(-1, tokens)
        v_flat = v_cache.transpose(1, 2, 0).reshape(-1, tokens)
        any_spec = pl.BlockSpec(memory_space=pl.ANY)

        def v(*shape, dtype=BF16):
            return pltpu.VMEM(shape, dtype)
        tok = v(NB, HALF, width)
        scratch = [
            pltpu.SMEM((1,), jnp.int32), v(1, width, dtype=F32), v(1, width, dtype=F32),
            v(new_len, width), v(*w_q.shape), v(*w_k.shape), v(*w_v.shape), v(*w_o.shape), v(*w_gate.shape), v(*w_up.shape), v(*w_down.shape),
            v(*k_flat.shape), v(*v_flat.shape),
            v(NB, BLK, 512), v(NB, BLK, 256), v(NB, BLK, 512), v(NB, 8, BLK, dtype=F32), v(NB, 8, BLK, dtype=F32),
            v(new_len, 128, dtype=F32), v(new_len, 128, dtype=F32), v(64, PAST_MAX + new_len), v(PAST_MAX + new_len, 64),
            v(BLK, 256), v(256, new_len), v(NB, BLK, 256), v(NB, BLK, 256),
            tok, tok, tok, tok, tok, v(NB, 2, HALF, width), v(NB, 8, BLK, dtype=F32), v(NB, 8, BLK, dtype=F32), v(BLK, width), v(BLK, 128, dtype=F32),
            v(NB, CH, BLK, 2 * CW), v(2, CH, BLK, 2 * CW), v(NB, CH, BLK, 2 * CW), v(NB, CH, BLK, CW), v(NB, CH, BLK, CW),
            v(BLK, width, dtype=F32),
            tok, tok, tok, tok, tok, v(NB, 2, HALF, width),
            pltpu.SemaphoreType.DMA((16,)), pltpu.SemaphoreType.DMA((2 * NU + 2,)),
            pltpu.SemaphoreType.DMA((N_REMOTE,)), pltpu.SemaphoreType.DMA((N_REMOTE,)),
        ]
        shapes = tuple(jax.ShapeDtypeStruct(a, BF16) for a in (hidden.shape, k_flat.shape, v_flat.shape))
        done = pl.pallas_call(
            lambda *refs: kernel(2 * width, *refs),
            out_shape=shapes,
            in_specs=[any_spec] * 13,
            out_specs=(any_spec,) * 3,
            scratch_shapes=scratch,
            compiler_params=pltpu.CompilerParams(collective_id=0, has_side_effects=True, vmem_limit_bytes=67043328),
            name="layer",
        )(past_len, hidden, rms_attn.reshape(1, width), rms_mlp.reshape(1, width), w_q, w_k, w_v, w_o, w_gate, w_up, w_down,
          k_flat, v_flat)
        pieces = [(0, k * 128, 128) for k in range(new_len // 128)] + [(a, k * 64, 64) for a in (1, 2) for k in range(2)]
        out, k_full, v_full = pl.pallas_call(
            lambda *refs: results_body(pieces, *refs),
            out_shape=shapes, in_specs=[any_spec] * 3, out_specs=(any_spec,) * 3,
            scratch_shapes=[v(*a.shape) for a in shapes] + [pltpu.SemaphoreType.DMA((len(pieces),))] * 2,
            compiler_params=pltpu.CompilerParams(vmem_limit_bytes=60 << 20),
            name="results",
        )(*done)
        heads, dim = k_cache.shape[1:]
        return (out, k_full.reshape(heads, dim, tokens).transpose(2, 0, 1), v_full.reshape(heads, dim, tokens).transpose(2, 0, 1))

    row_split = P('hid', 'tp')
    col_split = P('tp', 'hid')
    cache_spec = P('dp', 'tp', None)
    in_specs = (P('dp', 'hid'), P('hid'), P('hid'), row_split, row_split, row_split, col_split,
                row_split, row_split, col_split, cache_spec, cache_spec, P('dp'))
    out_specs = (P('dp', 'hid'), cache_spec, cache_spec)
    return jax.shard_map(local_layer, mesh=mesh, in_specs=in_specs, out_specs=out_specs, check_vma=False)
```

```python
import math
import jax
import jax.numpy as jnp
from jax import lax
from jax.experimental import pallas as pl
from jax.experimental.pallas import tpu as pltpu
from jax.sharding import PartitionSpec as P

ROPE_BASE = 10000.0
F32, BF16 = jnp.float32, jnp.bfloat16
NEG = -1e30
BLK = 256
HALF = BLK // 2
PAST_MAX = 1024
NB = 4
CH = 4
CW = 256
MESH = pl.DeviceIdType.MESH

UNITS = ((0, 0, 256), (1, 0, 256), (2, 0, 256), (3, 0, 128), (3, 2, 64), (3, 3, 64))
NU = len(UNITS)
Q, R, O, C, X, D, T = 0, 4, 8, 12, 16, 20, 24
E, Y, F, G = 28, 28 + NU, 28 + 2 * NU, 28 + 3 * NU
A = G + CH * NU
N_REMOTE = A + CH * NU


def rope(t, cos_t, sin_t):
    width = t.shape[1]
    lane = lax.broadcasted_iota(jnp.int32, t.shape, 1)
    swapped = jnp.where((lane & 63) < 32, pltpu.roll(t, width - 32, 1), pltpu.roll(t, 32, 1))
    cos_w = jnp.concatenate([cos_t] * (width // 128), axis=1)
    sin_w = jnp.concatenate([sin_t] * (width // 128), axis=1)
    return (t * cos_w + swapped * sin_w).astype(BF16)


def row_sums(t):
    sq = jnp.broadcast_to(jnp.sum(t * t, axis=1, keepdims=True), (t.shape[0], 128))
    return jnp.transpose(sq)[:8]


def as_column(row):
    return jnp.transpose(jnp.broadcast_to(row[:1], (128, row.shape[1])))[:, :1]


def kernel(d_model, p_hbm, x_hbm, g1_hbm, g2_hbm, wq_hbm, wk_hbm, wv_hbm, wo_hbm, wg_hbm, wu_hbm, wd_hbm, kc_hbm, vc_hbm,
           fin, kc, vc,
           p_ref, g1_ref, g2_ref, x, wq, wk, wv, wo, wg, wu, wd, qsend, qkeep, qrecv, sq1, sq1r, cos_b, sin_b, kt, vv, qs, kvn, ob, orecv,
           csend, ckeep, crecv, part, xrecv, mid, sq2, sq2r, hg, sums, gsend, gkeep, grecv, ab, arecv, acc,
           esend, ekeep, erecv, part2, yrecv, lsem, ssem, rsem):
    h = lax.axis_index('hid')
    t = lax.axis_index('tp')
    c = lax.rem(t, 2)
    hid_dev = {'hid': 1 - h}
    core_dev = {'tp': t + 1 - 2 * c}
    x_dev = {'tp': lax.rem(t + 2, 4)}
    own = h == 0

    loads = []

    def load(src, dst):
        n = len(loads)
        cp = pltpu.make_async_copy(src, dst, lsem.at[n])
        cp.start()
        loads.append(cp)
        return cp

    ld_x = [load(x_hbm.at[pl.ds(0, BLK)], x.at[pl.ds(0, BLK)])]
    ld_q = [load(g1_hbm, g1_ref), load(wq_hbm, wq), load(wk_hbm, wk), load(wv_hbm, wv)]
    ld_x += [load(x_hbm.at[pl.ds(BLK, BLK)], x.at[pl.ds(BLK, BLK)])]
    ld_small = [load(p_hbm, p_ref), load(g2_hbm, g2_ref)]

    barrier = pltpu.get_barrier_semaphore()
    for dev in (hid_dev, core_dev, x_dev):
        pl.semaphore_signal(barrier, inc=1, device_id=dev, device_id_type=MESH)

    def remote(src, dst, n, dev):
        return pltpu.make_async_remote_copy(src_ref=src, dst_ref=dst, send_sem=ssem.at[n], recv_sem=rsem.at[n],
                                            device_id=dev, device_id_type=MESH)

    def q_copy(i): return remote(qsend.at[i], qrecv.at[i], Q + i, hid_dev)
    def r_copy(i): return remote(sq1.at[i], sq1r.at[i], R + i, hid_dev)
    def o_copy(i): return remote(ob.at[i], orecv.at[i], O + i, hid_dev)
    def c_copy(i): return remote(csend.at[i], crecv.at[i], C + i, core_dev)
    def x_copy(i): return remote(part.at[i], xrecv.at[i], X + i, x_dev)
    def d_copy(i): return remote(mid.at[i, 0], mid.at[i, 1], D + i, core_dev)
    def t_copy(i): return remote(sq2.at[i], sq2r.at[i], T + i, hid_dev)

    def whole(u):
        return pl.ds(UNITS[u][1] * UNITS[u][2], UNITS[u][2])

    def half(u):
        return pl.ds(UNITS[u][1] * UNITS[u][2] // 2, UNITS[u][2] // 2)

    def g_copy(u, j): return remote(gsend.at[UNITS[u][0], j, whole(u)], grecv.at[UNITS[u][0], j, whole(u)], G + CH * u + j, hid_dev)
    def a_copy(u, j): return remote(ab.at[UNITS[u][0], j, whole(u)], arecv.at[UNITS[u][0], j, whole(u)], A + CH * u + j, hid_dev)
    def e_copy(u): return remote(esend.at[UNITS[u][0], half(u)], erecv.at[UNITS[u][0], half(u)], E + u, core_dev)
    def y_copy(u): return remote(part2.at[UNITS[u][0], half(u)], yrecv.at[UNITS[u][0], half(u)], Y + u, x_dev)
    def f_copy(u): return remote(fin.at[UNITS[u][0], 0, half(u)], fin.at[UNITS[u][0], 1, half(u)], F + u, core_dev)

    def qkv(i, send):
        xf = x[pl.ds(i * BLK, BLK), :].astype(F32)
        xg = (xf * g1_ref[...]).astype(BF16)
        theirs = wq[:, pl.ds(pl.multiple_of((1 - h) * 256, 256), 256)]
        qsend[i, :, :256] = jnp.dot(xg, theirs, preferred_element_type=F32).astype(BF16)
        qsend[i, :, 256:384] = jnp.dot(xg, wk[...], preferred_element_type=F32).astype(BF16)
        qsend[i, :, 384:] = jnp.dot(xg, wv[...], preferred_element_type=F32).astype(BF16)
        if i == 0:
            pl.semaphore_wait(barrier, 3)
        if send:
            q_copy(i).start()
        mine = wq[:, pl.ds(pl.multiple_of(h * 256, 256), 256)]
        qkeep[i] = jnp.dot(xg, mine, preferred_element_type=F32).astype(BF16)
        sq1[i] = row_sums(xf)
        if send:
            r_copy(i).start()

    def tables(i):
        pos = (p_ref[0] + i * BLK + lax.broadcasted_iota(jnp.int32, (BLK, 128), 0)).astype(F32)
        lane = lax.broadcasted_iota(jnp.int32, (BLK, 128), 1)
        freq = jnp.exp((lane[:8] & 31).astype(F32) * (-2.0 * math.log(ROPE_BASE) / 64))[:1]
        ang = pos * freq
        cos_b[pl.ds(i * BLK, BLK), :] = jnp.cos(ang)
        sin = jnp.sin(ang)
        sin_b[pl.ds(i * BLK, BLK), :] = jnp.where((lane & 63) < 32, -sin, sin)

    def att(i):
        rows = slice(i * BLK, (i + 1) * BLK)
        q_copy(i).wait_recv()
        r_copy(i).wait_recv()
        r = as_column(lax.rsqrt((sq1[i] + sq1r[i]) / d_model + 1e-5))
        cos_t, sin_t = cos_b[rows, :], sin_b[rows, :]
        q = ((qkeep[i].astype(F32) + qrecv[i, :, :256].astype(F32)) * r).astype(BF16)
        kv = ((qsend[i, :, 256:].astype(F32) + qrecv[i, :, 256:].astype(F32)) * r).astype(BF16)
        qs[...] = (rope(q.astype(F32), cos_t, sin_t).astype(F32) * 0.125).astype(BF16)
        k = rope(kv[:, :128].astype(F32), cos_t, sin_t)
        v = kv[:, 128:]
        k_t = jnp.transpose(k.astype(F32)).astype(BF16)
        kvn[:128, rows] = k_t
        kvn[128:, rows] = jnp.transpose(v.astype(F32)).astype(BF16)
        main = PAST_MAX + i * BLK
        kt[:, main:main + BLK] = jnp.where(own, k_t[:64], k_t[64:])
        vv[main:main + BLK, :] = jnp.where(own, v[:, :64], v[:, 64:])
        col = lax.broadcasted_iota(jnp.int32, (1, main), 1)
        bias = jnp.where((col >= p_ref[0]) & (col < PAST_MAX), NEG, 0.0)
        causal = lax.broadcasted_iota(jnp.int32, (BLK, BLK), 1) <= lax.broadcasted_iota(jnp.int32, (BLK, BLK), 0)

        def pair(n, carry):
            lanes = pl.ds(pl.multiple_of(n * 128, 128), 128)
            qp = qs[:, lanes]
            done = []
            for s in range(2):
                qn = qp[:, s * 64:(s + 1) * 64]
                s_main = jnp.dot(qn, kt[:, :main], preferred_element_type=F32) + bias
                s_diag = jnp.where(causal, jnp.dot(qn, kt[:, main:main + BLK], preferred_element_type=F32), NEG)
                top = jnp.maximum(jnp.max(s_main, axis=1, keepdims=True), jnp.max(s_diag, axis=1, keepdims=True))
                e_main = jnp.exp(s_main - top)
                e_diag = jnp.exp(s_diag - top)
                inv = 1.0 / (jnp.sum(e_main, axis=1, keepdims=True) + jnp.sum(e_diag, axis=1, keepdims=True))
                o = jnp.dot((e_main * inv).astype(BF16), vv[:main, :], preferred_element_type=F32)
                o += jnp.dot((e_diag * inv).astype(BF16), vv[main:main + BLK, :], preferred_element_type=F32)
                done.append(o.astype(BF16))
            ob[i, :, lanes] = jnp.concatenate(done, axis=1)
            return carry
        lax.fori_loop(0, 2, pair, 0)
        o_copy(i).start()

    def wo_step(i):
        o_copy(i).wait_recv()
        acc[...] = jnp.dot(ob[i], wo[pl.ds(pl.multiple_of(h * 256, 256), 256), :], preferred_element_type=F32)
        acc[...] += jnp.dot(orecv[i], wo[pl.ds(pl.multiple_of((1 - h) * 256, 256), 256), :], preferred_element_type=F32)
        ckeep[i] = acc[pl.ds(pl.multiple_of(c * HALF, HALF), HALF), :].astype(BF16)
        csend[i] = acc[pl.ds(pl.multiple_of((1 - c) * HALF, HALF), HALF), :].astype(BF16)
        c_copy(i).start()

    def add(a, b):
        return (a.astype(F32) + b.astype(F32)).astype(BF16)

    def c_step(i):
        c_copy(i).wait_recv()
        part[i] = add(ckeep[i], crecv[i])
        x_copy(i).start()

    def x_step(i):
        x_copy(i).wait_recv()
        res = x[pl.ds(pl.multiple_of(i * BLK + c * HALF, HALF), HALF), :]
        mid[i, 0] = add(res, add(part[i], xrecv[i]))
        d_copy(i).start()

    def d_step(i):
        d_copy(i).wait_recv()
        at = 0
        for u in range(NU):
            if UNITS[u][0] != i:
                continue
            for k in range(2):
                n = UNITS[u][2] // 2
                m = mid[i, k, half(u), :].astype(F32)
                sq = jnp.broadcast_to(jnp.sum(m * m, axis=1, keepdims=True), (n, 128))
                sums[at:at + n, :] = sq
                hg[at:at + n, :] = (m * g2_ref[...]).astype(BF16)
                at += n
        sq2[i] = jnp.transpose(sums[...])[:8]

    def gate_up(u, side, j, dst):
        cols = pl.ds(pl.multiple_of(side * (CH * CW) + j * CW, CW), CW)
        rows = hg[whole(u), :]
        dst[:, :CW] = jnp.dot(rows, wg[:, cols], preferred_element_type=F32).astype(BF16)
        dst[:, CW:] = jnp.dot(rows, wu[:, cols], preferred_element_type=F32).astype(BF16)

    def u_step(u, j):
        i = UNITS[u][0]
        gate_up(u, 1 - h, j, gsend.at[i, j, whole(u)])
        g_copy(u, j).start()
        gate_up(u, h, j, gkeep.at[i % 2, j, whole(u)])

    def v_step(u, j):
        i = UNITS[u][0]
        g_copy(u, j).wait_recv()
        r = as_column(lax.rsqrt((sq2[i] + sq2r[i]) / d_model + 1e-5))[UNITS[u][1] * UNITS[u][2]:(UNITS[u][1] + 1) * UNITS[u][2]]
        both = ((gkeep[i % 2, j, whole(u), :].astype(F32) + grecv[i, j, whole(u), :].astype(F32)) * r).astype(BF16).astype(F32)
        g, e = both[:, :CW], both[:, CW:]
        ab[i, j, whole(u), :] = (g * jax.nn.sigmoid(g) * e).astype(BF16)
        a_copy(u, j).start()

    def w_step(u, j):
        i = UNITS[u][0]
        a_copy(u, j).wait_recv()
        mine = wd[pl.ds(pl.multiple_of(h * (CH * CW) + j * CW, CW), CW), :]
        theirs = wd[pl.ds(pl.multiple_of((1 - h) * (CH * CW) + j * CW, CW), CW), :]
        y = jnp.dot(ab[i, j, whole(u), :], mine, preferred_element_type=F32)
        y += jnp.dot(arecv[i, j, whole(u), :], theirs, preferred_element_type=F32)
        acc[whole(u), :] = jnp.where(j == 0, 0.0, acc[whole(u), :]) + y

    def e_start(u):
        i, k, n = UNITS[u]
        ekeep[i, half(u), :] = acc[k * n:k * n + n // 2, :].astype(BF16)
        esend[i, half(u), :] = acc[k * n + n // 2:k * n + n, :].astype(BF16)
        e_copy(u).start()

    def e_step(u):
        i = UNITS[u][0]
        e_copy(u).wait_recv()
        part2[i, half(u), :] = add(ekeep[i, half(u), :], erecv[i, half(u), :])
        y_copy(u).start()

    def y_step(u):
        i = UNITS[u][0]
        y_copy(u).wait_recv()
        down = add(part2[i, half(u), :], yrecv[i, half(u), :])
        fin[i, 0, half(u), :] = add(mid[i, 0, half(u), :], down)
        f_copy(u).start()

    def f_step(u):
        f_copy(u).wait_recv()

    def loop(*steps):
        def body(j, carry):
            for step, i in steps:
                step(i, j)
            return carry
        lax.fori_loop(0, CH, body, 0)

    def cache_rows():
        def tile(n, carry):
            cols = pl.ds(pl.multiple_of(n * BLK, BLK), BLK)
            at = n * BLK - p_ref[0] + lax.broadcasted_iota(jnp.int32, (NB * BLK, BLK), 1)
            pick = jnp.where(at == lax.broadcasted_iota(jnp.int32, (NB * BLK, BLK), 0), 1.0, 0.0).astype(BF16)
            new = jnp.dot(kvn[...], pick, preferred_element_type=F32)
            where = n * BLK - p_ref[0] + lax.broadcasted_iota(jnp.int32, (128, BLK), 1)
            fresh = (where >= 0) & (where < NB * BLK)
            kc[:, cols] = jnp.where(fresh, new[:128], kc[:, cols].astype(F32)).astype(BF16)
            vc[:, cols] = jnp.where(fresh, new[128:], vc[:, cols].astype(F32)).astype(BF16)
            return carry
        lax.fori_loop(0, kc.shape[1] // BLK, tile, 0)

    for cp in ld_q:
        cp.wait()
    ld_x[0].wait()
    qkv(0, True)
    ld_x += [load(x_hbm.at[pl.ds(i * BLK, BLK)], x.at[pl.ds(i * BLK, BLK)]) for i in range(2, NB)]
    ld_kc, ld_vc = load(kc_hbm, kc), load(vc_hbm, vc)
    ld_wo = load(wo_hbm, wo)
    ld_gu = [load(wg_hbm, wg), load(wu_hbm, wu)]
    ld_wd = load(wd_hbm, wd)
    for i in range(1, NB):
        ld_x[i].wait()
        qkv(i, i < 2)
    for cp in ld_small:
        cp.wait()
    for i in range(NB):
        tables(i)
    ld_kc.wait()
    ld_vc.wait()
    kt[:, :PAST_MAX] = kc[pl.ds(pl.multiple_of(h * 64, 64), 64), :PAST_MAX]
    v_old = jnp.transpose(vc[:, :PAST_MAX].astype(F32)).astype(BF16)
    vv[:PAST_MAX, :] = jnp.where(own, v_old[:, :64], v_old[:, 64:])
    att(0)
    q_copy(2).start()
    r_copy(2).start()
    att(1)
    q_copy(3).start()
    r_copy(3).start()
    ld_wo.wait()
    wo_step(0)
    c_step(0)
    att(2)
    x_step(0)
    wo_step(1)
    d_step(0)
    for cp in ld_gu:
        cp.wait()
    t_copy(0).start()
    loop((u_step, 0))
    c_step(1)
    att(3)
    x_step(1)
    wo_step(2)
    d_step(1)
    t_copy(1).start()
    t_copy(0).wait_recv()
    c_step(2)
    loop((u_step, 1), (v_step, 0))
    x_step(2)
    wo_step(3)
    c_step(3)
    d_step(2)
    t_copy(2).start()
    t_copy(1).wait_recv()
    ld_wd.wait()
    loop((u_step, 2), (v_step, 1), (w_step, 0))
    e_start(0)
    x_step(3)
    d_step(3)
    t_copy(3).start()
    e_step(0)
    t_copy(2).wait_recv()
    cache_rows()
    loop((u_step, 3), (v_step, 2), (w_step, 1))
    loop((u_step, 4))
    loop((u_step, 5))
    e_start(1)
    y_step(0)
    e_step(1)
    f_step(0)
    t_copy(3).wait_recv()
    loop((v_step, 3), (w_step, 2))
    e_start(2)
    y_step(1)
    e_step(2)
    f_step(1)
    loop((v_step, 4))
    loop((v_step, 5))
    y_step(2)
    loop((w_step, 3))
    e_start(3)
    f_step(2)
    w_step(4, 0)
    e_step(3)
    for j in range(1, CH):
        w_step(4, j)
    e_start(4)
    w_step(5, 0)
    e_step(4)
    for j in range(1, CH):
        w_step(5, j)
    e_start(5)
    y_step(3)
    e_step(5)
    y_step(4)
    f_step(3)
    y_step(5)
    f_step(4)
    f_step(5)

    for i in range(NB):
        for cp in (q_copy, r_copy, o_copy, c_copy, x_copy, d_copy, t_copy):
            cp(i).wait_send()
    for u in range(NU):
        for cp in (e_copy, y_copy, f_copy):
            cp(u).wait_send()

        def drain(j, carry, u=u):
            g_copy(u, j).wait_send()
            a_copy(u, j).wait_send()
            return carry
        lax.fori_loop(0, CH, drain, 0)


def results_body(fin, kc, vc, out_hbm, ko_hbm, vo_hbm, sem):
    c = lax.rem(lax.axis_index('tp'), 2)
    copies = [pltpu.make_async_copy(kc, ko_hbm, sem.at[2 * NB]), pltpu.make_async_copy(vc, vo_hbm, sem.at[2 * NB + 1])]
    for i in range(NB):
        for k in range(2):
            at = pl.multiple_of(i * BLK + (c if k == 0 else 1 - c) * HALF, HALF)
            copies.append(pltpu.make_async_copy(fin.at[i, k], out_hbm.at[pl.ds(at, HALF)], sem.at[2 * i + k]))
    for cp in copies:
        cp.start()
    for cp in copies:
        cp.wait()


def solution(mesh):
    def local_layer(hidden, rms_attn, rms_mlp, w_q, w_k, w_v, w_o, w_gate, w_up, w_down, k_cache, v_cache, past_len):
        new_len, width = hidden.shape
        tokens = k_cache.shape[0]
        k_flat = k_cache.transpose(1, 2, 0).reshape(-1, tokens)
        v_flat = v_cache.transpose(1, 2, 0).reshape(-1, tokens)
        any_spec = pl.BlockSpec(memory_space=pl.ANY)

        def v(*shape, dtype=BF16):
            return pltpu.VMEM(shape, dtype)
        tok = v(NB, HALF, width)
        scratch = [
            pltpu.SMEM((1,), jnp.int32), v(1, width, dtype=F32), v(1, width, dtype=F32),
            v(new_len, width), v(*w_q.shape), v(*w_k.shape), v(*w_v.shape), v(*w_o.shape), v(*w_gate.shape), v(*w_up.shape), v(*w_down.shape),
            v(NB, BLK, 512), v(NB, BLK, 256), v(NB, BLK, 512), v(NB, 8, BLK, dtype=F32), v(NB, 8, BLK, dtype=F32),
            v(new_len, 128, dtype=F32), v(new_len, 128, dtype=F32), v(64, PAST_MAX + new_len), v(PAST_MAX + new_len, 64),
            v(BLK, 256), v(256, new_len), v(NB, BLK, 256), v(NB, BLK, 256),
            tok, tok, tok, tok, tok, v(NB, 2, HALF, width), v(NB, 8, BLK, dtype=F32), v(NB, 8, BLK, dtype=F32), v(BLK, width), v(BLK, 128, dtype=F32),
            v(NB, CH, BLK, 2 * CW), v(2, CH, BLK, 2 * CW), v(NB, CH, BLK, 2 * CW), v(NB, CH, BLK, CW), v(NB, CH, BLK, CW),
            v(BLK, width, dtype=F32),
            tok, tok, tok, tok, tok,
            pltpu.SemaphoreType.DMA((16,)),
            pltpu.SemaphoreType.DMA((N_REMOTE,)), pltpu.SemaphoreType.DMA((N_REMOTE,)),
        ]
        kept = ((NB, 2, HALF, width), k_flat.shape, v_flat.shape)
        vmem_spec = pl.BlockSpec(memory_space=pltpu.VMEM)
        done = pl.pallas_call(
            lambda *refs: kernel(2 * width, *refs),
            out_shape=tuple(v(*a) for a in kept),
            in_specs=[any_spec] * 13,
            out_specs=(vmem_spec,) * 3,
            scratch_shapes=scratch,
            compiler_params=pltpu.CompilerParams(collective_id=0, has_side_effects=True, vmem_limit_bytes=60 << 20),
            name="layer",
        )(past_len, hidden, rms_attn.reshape(1, width), rms_mlp.reshape(1, width), w_q, w_k, w_v, w_o, w_gate, w_up, w_down,
          k_flat, v_flat)
        out, k_full, v_full = pl.pallas_call(
            results_body,
            out_shape=tuple(jax.ShapeDtypeStruct(a, BF16) for a in (hidden.shape, k_flat.shape, v_flat.shape)),
            in_specs=[vmem_spec] * 3, out_specs=(any_spec,) * 3,
            scratch_shapes=[pltpu.SemaphoreType.DMA((2 * NB + 2,))],
            compiler_params=pltpu.CompilerParams(vmem_limit_bytes=1 << 20),
            name="results",
        )(*done)
        heads, dim = k_cache.shape[1:]
        return (out, k_full.reshape(heads, dim, tokens).transpose(2, 0, 1), v_full.reshape(heads, dim, tokens).transpose(2, 0, 1))

    row_split = P('hid', 'tp')
    col_split = P('tp', 'hid')
    cache_spec = P('dp', 'tp', None)
    in_specs = (P('dp', 'hid'), P('hid'), P('hid'), row_split, row_split, row_split, col_split,
                row_split, row_split, col_split, cache_spec, cache_spec, P('dp'))
    out_specs = (P('dp', 'hid'), cache_spec, cache_spec)
    return jax.shard_map(local_layer, mesh=mesh, in_specs=in_specs, out_specs=out_specs, check_vma=False)
```

```python
import math
import jax
import jax.numpy as jnp
from jax import lax
from jax.experimental import pallas as pl
from jax.experimental.pallas import tpu as pltpu
from jax.sharding import PartitionSpec as P

ROPE_BASE = 10000.0
F32, BF16 = jnp.float32, jnp.bfloat16
NEG = -1e30
BLK = 256
HALF = BLK // 2
PAST_MAX = 1024
NB = 4
CH = 4
CW = 256
MESH = pl.DeviceIdType.MESH

UNITS = ((0, 0, 256), (1, 0, 256), (2, 0, 256), (3, 0, 128), (3, 2, 64), (3, 3, 64))
NU = len(UNITS)
Q, R, O, C, X, D, T = 0, 4, 8, 12, 16, 20, 24
E, Y, F, G = 28, 28 + NU, 28 + 2 * NU, 28 + 3 * NU
A = G + CH * NU
KV = A + CH * NU
N_REMOTE = KV + NB


def rope(t, cos_t, sin_t):
    width = t.shape[1]
    lane = lax.broadcasted_iota(jnp.int32, t.shape, 1)
    swapped = jnp.where((lane & 63) < 32, pltpu.roll(t, width - 32, 1), pltpu.roll(t, 32, 1))
    cos_w = jnp.concatenate([cos_t] * (width // 128), axis=1)
    sin_w = jnp.concatenate([sin_t] * (width // 128), axis=1)
    return (t * cos_w + swapped * sin_w).astype(BF16)


def row_sums(t):
    sq = jnp.broadcast_to(jnp.sum(t * t, axis=1, keepdims=True), (t.shape[0], 128))
    return jnp.transpose(sq)[:8]


def as_column(row):
    return jnp.transpose(jnp.broadcast_to(row[:1], (128, row.shape[1])))[:, :1]


def kernel(d_model, p_hbm, x_hbm, g1_hbm, g2_hbm, wq_hbm, wk_hbm, wv_hbm, wo_hbm, wg_hbm, wu_hbm, wd_hbm, kc_hbm, vc_hbm,
           fin, kc, vc,
           p_ref, g1_ref, g2_ref, x, wq, wk, wv, wo, wg, wu, wd, qsend, qkeep, qrecv, sq1, sq1r, cos_b, sin_b, kt, vv, qs, kvn, kvsend, kvrecv, ob, orecv,
           csend, ckeep, crecv, part, xrecv, mid, sq2, sq2r, hg, sums, gsend, gkeep, grecv, ab, arecv, acc,
           esend, ekeep, erecv, part2, yrecv, lsem, ssem, rsem):
    h = lax.axis_index('hid')
    t = lax.axis_index('tp')
    c = lax.rem(t, 2)
    hid_dev = {'hid': 1 - h}
    core_dev = {'tp': t + 1 - 2 * c}
    x_dev = {'tp': lax.rem(t + 2, 4)}
    own = h == 0

    loads = []

    def load(src, dst):
        n = len(loads)
        cp = pltpu.make_async_copy(src, dst, lsem.at[n])
        cp.start()
        loads.append(cp)
        return cp

    ld_x = [load(x_hbm.at[pl.ds(0, BLK)], x.at[pl.ds(0, BLK)])]
    ld_q = [load(g1_hbm, g1_ref), load(wq_hbm, wq), load(wk_hbm, wk), load(wv_hbm, wv)]
    ld_x += [load(x_hbm.at[pl.ds(BLK, BLK)], x.at[pl.ds(BLK, BLK)])]
    ld_small = [load(p_hbm, p_ref), load(g2_hbm, g2_ref)]

    barrier = pltpu.get_barrier_semaphore()
    for dev in (hid_dev, core_dev, x_dev):
        pl.semaphore_signal(barrier, inc=1, device_id=dev, device_id_type=MESH)

    def remote(src, dst, n, dev):
        return pltpu.make_async_remote_copy(src_ref=src, dst_ref=dst, send_sem=ssem.at[n], recv_sem=rsem.at[n],
                                            device_id=dev, device_id_type=MESH)

    def q_copy(i): return remote(qsend.at[i], qrecv.at[i], Q + i, hid_dev)
    def r_copy(i): return remote(sq1.at[i], sq1r.at[i], R + i, hid_dev)
    def o_copy(i): return remote(ob.at[i], orecv.at[i], O + i, hid_dev)
    def kv_copy(i): return remote(kvsend.at[i], kvrecv.at[i], KV + i, hid_dev)
    def c_copy(i): return remote(csend.at[i], crecv.at[i], C + i, core_dev)
    def x_copy(i): return remote(part.at[i], xrecv.at[i], X + i, x_dev)
    def d_copy(i): return remote(mid.at[i, 0], mid.at[i, 1], D + i, core_dev)
    def t_copy(i): return remote(sq2.at[i], sq2r.at[i], T + i, hid_dev)

    def whole(u):
        return pl.ds(UNITS[u][1] * UNITS[u][2], UNITS[u][2])

    def half(u):
        return pl.ds(UNITS[u][1] * UNITS[u][2] // 2, UNITS[u][2] // 2)

    def g_copy(u, j): return remote(gsend.at[UNITS[u][0], j, whole(u)], grecv.at[UNITS[u][0], j, whole(u)], G + CH * u + j, hid_dev)
    def a_copy(u, j): return remote(ab.at[UNITS[u][0], j, whole(u)], arecv.at[UNITS[u][0], j, whole(u)], A + CH * u + j, hid_dev)
    def e_copy(u): return remote(esend.at[UNITS[u][0], half(u)], erecv.at[UNITS[u][0], half(u)], E + u, core_dev)
    def y_copy(u): return remote(part2.at[UNITS[u][0], half(u)], yrecv.at[UNITS[u][0], half(u)], Y + u, x_dev)
    def f_copy(u): return remote(fin.at[UNITS[u][0], 0, half(u)], fin.at[UNITS[u][0], 1, half(u)], F + u, core_dev)

    def qkv(i, send):
        xf = x[pl.ds(i * BLK, BLK), :].astype(F32)
        xg = (xf * g1_ref[...]).astype(BF16)
        theirs = wq[:, pl.ds(pl.multiple_of((1 - h) * 256, 256), 256)]
        qsend[i, :, :256] = jnp.dot(xg, theirs, preferred_element_type=F32).astype(BF16)
        k = jnp.dot(xg, wk[...], preferred_element_type=F32).astype(BF16)
        v = jnp.dot(xg, wv[...], preferred_element_type=F32).astype(BF16)
        low = jnp.concatenate([k[:, :64], v[:, :64]], axis=1)
        high = jnp.concatenate([k[:, 64:], v[:, 64:]], axis=1)
        qsend[i, :, 256:] = jnp.where(own, high, low)
        if i == 0:
            pl.semaphore_wait(barrier, 3)
        if send:
            q_copy(i).start()
        kvsend[i] = jnp.where(own, low, high)
        mine = wq[:, pl.ds(pl.multiple_of(h * 256, 256), 256)]
        qkeep[i] = jnp.dot(xg, mine, preferred_element_type=F32).astype(BF16)
        sq1[i] = row_sums(xf)
        if send:
            r_copy(i).start()

    def tables(i):
        pos = (p_ref[0] + i * BLK + lax.broadcasted_iota(jnp.int32, (BLK, 128), 0)).astype(F32)
        lane = lax.broadcasted_iota(jnp.int32, (BLK, 128), 1)
        freq = jnp.exp((lane[:8] & 31).astype(F32) * (-2.0 * math.log(ROPE_BASE) / 64))[:1]
        ang = pos * freq
        cos_b[pl.ds(i * BLK, BLK), :] = jnp.cos(ang)
        sin = jnp.sin(ang)
        sin_b[pl.ds(i * BLK, BLK), :] = jnp.where((lane & 63) < 32, -sin, sin)

    def row_factor(i):
        return as_column(lax.rsqrt((sq1[i] + sq1r[i]) / d_model + 1e-5))

    def keys_values(i, r, mine, theirs):
        rows = slice(i * BLK, (i + 1) * BLK)
        kv = ((mine.astype(F32) + theirs.astype(F32)) * r).astype(BF16)
        lane = lax.broadcasted_iota(jnp.int32, kv.shape, 1)
        return jnp.where(lane < 64, rope(kv.astype(F32), cos_b[rows, :], sin_b[rows, :]), kv)

    def att(i):
        rows = slice(i * BLK, (i + 1) * BLK)
        q_copy(i).wait_recv()
        r_copy(i).wait_recv()
        r = row_factor(i)
        cos_t, sin_t = cos_b[rows, :], sin_b[rows, :]
        q = ((qkeep[i].astype(F32) + qrecv[i, :, :256].astype(F32)) * r).astype(BF16)
        kv = keys_values(i, r, kvsend[i], qrecv[i, :, 256:])
        qs[...] = (rope(q.astype(F32), cos_t, sin_t).astype(F32) * 0.125).astype(BF16)
        kv_t = jnp.transpose(kv.astype(F32)).astype(BF16)
        kvn[i] = kv_t
        main = PAST_MAX + i * BLK
        kt[:, main:main + BLK] = kv_t[:64]
        vv[main:main + BLK, :] = kv[:, 64:]
        col = lax.broadcasted_iota(jnp.int32, (1, main), 1)
        bias = jnp.where((col >= p_ref[0]) & (col < PAST_MAX), NEG, 0.0)
        causal = lax.broadcasted_iota(jnp.int32, (BLK, BLK), 1) <= lax.broadcasted_iota(jnp.int32, (BLK, BLK), 0)

        def pair(n, carry):
            lanes = pl.ds(pl.multiple_of(n * 128, 128), 128)
            qp = qs[:, lanes]
            done = []
            for s in range(2):
                qn = qp[:, s * 64:(s + 1) * 64]
                s_main = jnp.dot(qn, kt[:, :main], preferred_element_type=F32) + bias
                s_diag = jnp.where(causal, jnp.dot(qn, kt[:, main:main + BLK], preferred_element_type=F32), NEG)
                top = jnp.maximum(jnp.max(s_main, axis=1, keepdims=True), jnp.max(s_diag, axis=1, keepdims=True))
                e_main = jnp.exp(s_main - top)
                e_diag = jnp.exp(s_diag - top)
                inv = 1.0 / (jnp.sum(e_main, axis=1, keepdims=True) + jnp.sum(e_diag, axis=1, keepdims=True))
                o = jnp.dot((e_main * inv).astype(BF16), vv[:main, :], preferred_element_type=F32)
                o += jnp.dot((e_diag * inv).astype(BF16), vv[main:main + BLK, :], preferred_element_type=F32)
                done.append(o.astype(BF16))
            ob[i, :, lanes] = jnp.concatenate(done, axis=1)
            return carry
        lax.fori_loop(0, 2, pair, 0)
        o_copy(i).start()

    def wo_step(i):
        o_copy(i).wait_recv()
        acc[...] = jnp.dot(ob[i], wo[pl.ds(pl.multiple_of(h * 256, 256), 256), :], preferred_element_type=F32)
        acc[...] += jnp.dot(orecv[i], wo[pl.ds(pl.multiple_of((1 - h) * 256, 256), 256), :], preferred_element_type=F32)
        ckeep[i] = acc[pl.ds(pl.multiple_of(c * HALF, HALF), HALF), :].astype(BF16)
        csend[i] = acc[pl.ds(pl.multiple_of((1 - c) * HALF, HALF), HALF), :].astype(BF16)
        c_copy(i).start()

    def add(a, b):
        return (a.astype(F32) + b.astype(F32)).astype(BF16)

    def c_step(i):
        c_copy(i).wait_recv()
        part[i] = add(ckeep[i], crecv[i])
        x_copy(i).start()

    def x_step(i):
        x_copy(i).wait_recv()
        res = x[pl.ds(pl.multiple_of(i * BLK + c * HALF, HALF), HALF), :]
        mid[i, 0] = add(res, add(part[i], xrecv[i]))
        d_copy(i).start()

    def d_step(i):
        d_copy(i).wait_recv()
        at = 0
        for u in range(NU):
            if UNITS[u][0] != i:
                continue
            for k in range(2):
                n = UNITS[u][2] // 2
                m = mid[i, k, half(u), :].astype(F32)
                sq = jnp.broadcast_to(jnp.sum(m * m, axis=1, keepdims=True), (n, 128))
                sums[at:at + n, :] = sq
                hg[at:at + n, :] = (m * g2_ref[...]).astype(BF16)
                at += n
        sq2[i] = jnp.transpose(sums[...])[:8]

    def gate_up(u, side, j, dst):
        cols = pl.ds(pl.multiple_of(side * (CH * CW) + j * CW, CW), CW)
        rows = hg[whole(u), :]
        dst[:, :CW] = jnp.dot(rows, wg[:, cols], preferred_element_type=F32).astype(BF16)
        dst[:, CW:] = jnp.dot(rows, wu[:, cols], preferred_element_type=F32).astype(BF16)

    def u_step(u, j):
        i = UNITS[u][0]
        gate_up(u, 1 - h, j, gsend.at[i, j, whole(u)])
        g_copy(u, j).start()
        gate_up(u, h, j, gkeep.at[i % 2, j, whole(u)])

    def v_step(u, j):
        i = UNITS[u][0]
        g_copy(u, j).wait_recv()
        r = as_column(lax.rsqrt((sq2[i] + sq2r[i]) / d_model + 1e-5))[UNITS[u][1] * UNITS[u][2]:(UNITS[u][1] + 1) * UNITS[u][2]]
        both = ((gkeep[i % 2, j, whole(u), :].astype(F32) + grecv[i, j, whole(u), :].astype(F32)) * r).astype(BF16).astype(F32)
        g, e = both[:, :CW], both[:, CW:]
        ab[i, j, whole(u), :] = (g * jax.nn.sigmoid(g) * e).astype(BF16)
        a_copy(u, j).start()

    def w_step(u, j):
        i = UNITS[u][0]
        a_copy(u, j).wait_recv()
        mine = wd[pl.ds(pl.multiple_of(h * (CH * CW) + j * CW, CW), CW), :]
        theirs = wd[pl.ds(pl.multiple_of((1 - h) * (CH * CW) + j * CW, CW), CW), :]
        y = jnp.dot(ab[i, j, whole(u), :], mine, preferred_element_type=F32)
        y += jnp.dot(arecv[i, j, whole(u), :], theirs, preferred_element_type=F32)
        acc[whole(u), :] = jnp.where(j == 0, 0.0, acc[whole(u), :]) + y

    def e_start(u):
        i, k, n = UNITS[u]
        ekeep[i, half(u), :] = acc[k * n:k * n + n // 2, :].astype(BF16)
        esend[i, half(u), :] = acc[k * n + n // 2:k * n + n, :].astype(BF16)
        e_copy(u).start()

    def e_step(u):
        i = UNITS[u][0]
        e_copy(u).wait_recv()
        part2[i, half(u), :] = add(ekeep[i, half(u), :], erecv[i, half(u), :])
        y_copy(u).start()

    def y_step(u):
        i = UNITS[u][0]
        y_copy(u).wait_recv()
        down = add(part2[i, half(u), :], yrecv[i, half(u), :])
        fin[i, 0, half(u), :] = add(mid[i, 0, half(u), :], down)
        f_copy(u).start()

    def f_step(u):
        f_copy(u).wait_recv()

    def loop(*steps):
        def body(j, carry):
            for step, i in steps:
                step(i, j)
            return carry
        lax.fori_loop(0, CH, body, 0)

    def place(i, head, kv_t):
        lanes = pl.ds(pl.multiple_of(head * 64, 64), 64)

        def tile(n, carry):
            cols = pl.ds(pl.multiple_of(n * BLK, BLK), BLK)
            first = (n - i) * BLK - p_ref[0]
            at = first + lax.broadcasted_iota(jnp.int32, (BLK, BLK), 1)
            pick = jnp.where(at == lax.broadcasted_iota(jnp.int32, (BLK, BLK), 0), 1.0, 0.0).astype(BF16)
            new = jnp.dot(kv_t, pick, preferred_element_type=F32)
            where = first + lax.broadcasted_iota(jnp.int32, (64, BLK), 1)
            fresh = (where >= 0) & (where < BLK)
            kc[lanes, cols] = jnp.where(fresh, new[:64], kc[lanes, cols].astype(F32)).astype(BF16)
            vc[lanes, cols] = jnp.where(fresh, new[64:], vc[lanes, cols].astype(F32)).astype(BF16)
            return carry
        lax.fori_loop(i + 1, i + 1 + PAST_MAX // BLK, tile, 0)

    def kv_step(i):
        kv_copy(i).wait_recv()
        kv = keys_values(i, row_factor(i), qsend[i, :, 256:], kvrecv[i])
        place(i, 1 - h, jnp.transpose(kv.astype(F32)).astype(BF16))

    for cp in ld_q:
        cp.wait()
    ld_x[0].wait()
    qkv(0, True)
    ld_x += [load(x_hbm.at[pl.ds(i * BLK, BLK)], x.at[pl.ds(i * BLK, BLK)]) for i in range(2, NB)]
    ld_kc, ld_vc = load(kc_hbm, kc), load(vc_hbm, vc)
    ld_wo = load(wo_hbm, wo)
    ld_gu = [load(wg_hbm, wg), load(wu_hbm, wu)]
    ld_wd = load(wd_hbm, wd)
    for i in range(1, NB):
        ld_x[i].wait()
        qkv(i, i < 2)
    for cp in ld_small:
        cp.wait()
    for i in range(NB):
        tables(i)
    ld_kc.wait()
    ld_vc.wait()
    kt[:, :PAST_MAX] = kc[pl.ds(pl.multiple_of(h * 64, 64), 64), :PAST_MAX]
    v_old = jnp.transpose(vc[:, :PAST_MAX].astype(F32)).astype(BF16)
    vv[:PAST_MAX, :] = jnp.where(own, v_old[:, :64], v_old[:, 64:])
    att(0)
    q_copy(2).start()
    r_copy(2).start()
    att(1)
    q_copy(3).start()
    r_copy(3).start()
    ld_wo.wait()
    wo_step(0)
    c_step(0)
    att(2)
    x_step(0)
    wo_step(1)
    d_step(0)
    for cp in ld_gu:
        cp.wait()
    t_copy(0).start()
    loop((u_step, 0))
    c_step(1)
    att(3)
    x_step(1)
    wo_step(2)
    d_step(1)
    t_copy(1).start()
    t_copy(0).wait_recv()
    c_step(2)
    loop((u_step, 1), (v_step, 0))
    x_step(2)
    wo_step(3)
    c_step(3)
    d_step(2)
    t_copy(2).start()
    t_copy(1).wait_recv()
    ld_wd.wait()
    loop((u_step, 2), (v_step, 1), (w_step, 0))
    e_start(0)
    x_step(3)
    d_step(3)
    t_copy(3).start()
    e_step(0)
    t_copy(2).wait_recv()
    for i in range(NB):
        place(i, h, kvn[i])
    loop((u_step, 3), (v_step, 2), (w_step, 1))
    loop((u_step, 4))
    loop((u_step, 5))
    e_start(1)
    y_step(0)
    e_step(1)
    f_step(0)
    t_copy(3).wait_recv()
    loop((v_step, 3), (w_step, 2))
    e_start(2)
    y_step(1)
    e_step(2)
    f_step(1)
    loop((v_step, 4))
    loop((v_step, 5))
    for i in range(NB):
        kv_copy(i).start()
    y_step(2)
    loop((w_step, 3))
    e_start(3)
    f_step(2)
    w_step(4, 0)
    e_step(3)
    for j in range(1, CH):
        w_step(4, j)
    e_start(4)
    w_step(5, 0)
    e_step(4)
    for j in range(1, CH):
        w_step(5, j)
    e_start(5)
    y_step(3)
    e_step(5)
    kv_step(0)
    y_step(4)
    f_step(3)
    kv_step(1)
    kv_step(2)
    y_step(5)
    f_step(4)
    kv_step(3)
    f_step(5)

    for i in range(NB):
        for cp in (q_copy, r_copy, kv_copy, o_copy, c_copy, x_copy, d_copy, t_copy):
            cp(i).wait_send()
    for u in range(NU):
        for cp in (e_copy, y_copy, f_copy):
            cp(u).wait_send()

        def drain(j, carry, u=u):
            g_copy(u, j).wait_send()
            a_copy(u, j).wait_send()
            return carry
        lax.fori_loop(0, CH, drain, 0)


def results_body(fin, kc, vc, out_hbm, ko_hbm, vo_hbm, sem):
    c = lax.rem(lax.axis_index('tp'), 2)
    copies = [pltpu.make_async_copy(kc, ko_hbm, sem.at[2 * NB]), pltpu.make_async_copy(vc, vo_hbm, sem.at[2 * NB + 1])]
    for i in range(NB):
        for k in range(2):
            at = pl.multiple_of(i * BLK + (c if k == 0 else 1 - c) * HALF, HALF)
            copies.append(pltpu.make_async_copy(fin.at[i, k], out_hbm.at[pl.ds(at, HALF)], sem.at[2 * i + k]))
    for cp in copies:
        cp.start()
    for cp in copies:
        cp.wait()


def solution(mesh):
    def local_layer(hidden, rms_attn, rms_mlp, w_q, w_k, w_v, w_o, w_gate, w_up, w_down, k_cache, v_cache, past_len):
        new_len, width = hidden.shape
        tokens = k_cache.shape[0]
        k_flat = k_cache.transpose(1, 2, 0).reshape(-1, tokens)
        v_flat = v_cache.transpose(1, 2, 0).reshape(-1, tokens)
        any_spec = pl.BlockSpec(memory_space=pl.ANY)

        def v(*shape, dtype=BF16):
            return pltpu.VMEM(shape, dtype)
        tok = v(NB, HALF, width)
        scratch = [
            pltpu.SMEM((1,), jnp.int32), v(1, width, dtype=F32), v(1, width, dtype=F32),
            v(new_len, width), v(*w_q.shape), v(*w_k.shape), v(*w_v.shape), v(*w_o.shape), v(*w_gate.shape), v(*w_up.shape), v(*w_down.shape),
            v(NB, BLK, 384), v(NB, BLK, 256), v(NB, BLK, 384), v(NB, 8, BLK, dtype=F32), v(NB, 8, BLK, dtype=F32),
            v(new_len, 128, dtype=F32), v(new_len, 128, dtype=F32), v(64, PAST_MAX + new_len), v(PAST_MAX + new_len, 64),
            v(BLK, 256), v(NB, 128, BLK), v(NB, BLK, 128), v(NB, BLK, 128), v(NB, BLK, 256), v(NB, BLK, 256),
            tok, tok, tok, tok, tok, v(NB, 2, HALF, width), v(NB, 8, BLK, dtype=F32), v(NB, 8, BLK, dtype=F32), v(BLK, width), v(BLK, 128, dtype=F32),
            v(NB, CH, BLK, 2 * CW), v(2, CH, BLK, 2 * CW), v(NB, CH, BLK, 2 * CW), v(NB, CH, BLK, CW), v(NB, CH, BLK, CW),
            v(BLK, width, dtype=F32),
            tok, tok, tok, tok, tok,
            pltpu.SemaphoreType.DMA((16,)),
            pltpu.SemaphoreType.DMA((N_REMOTE,)), pltpu.SemaphoreType.DMA((N_REMOTE,)),
        ]
        kept = ((NB, 2, HALF, width), k_flat.shape, v_flat.shape)
        vmem_spec = pl.BlockSpec(memory_space=pltpu.VMEM)
        done = pl.pallas_call(
            lambda *refs: kernel(2 * width, *refs),
            out_shape=tuple(v(*a) for a in kept),
            in_specs=[any_spec] * 13,
            out_specs=(vmem_spec,) * 3,
            scratch_shapes=scratch,
            compiler_params=pltpu.CompilerParams(collective_id=0, has_side_effects=True, vmem_limit_bytes=60 << 20),
            name="layer",
        )(past_len, hidden, rms_attn.reshape(1, width), rms_mlp.reshape(1, width), w_q, w_k, w_v, w_o, w_gate, w_up, w_down,
          k_flat, v_flat)
        out, k_full, v_full = pl.pallas_call(
            results_body,
            out_shape=tuple(jax.ShapeDtypeStruct(a, BF16) for a in (hidden.shape, k_flat.shape, v_flat.shape)),
            in_specs=[vmem_spec] * 3, out_specs=(any_spec,) * 3,
            scratch_shapes=[pltpu.SemaphoreType.DMA((2 * NB + 2,))],
            compiler_params=pltpu.CompilerParams(vmem_limit_bytes=1 << 20),
            name="results",
        )(*done)
        heads, dim = k_cache.shape[1:]
        return (out, k_full.reshape(heads, dim, tokens).transpose(2, 0, 1), v_full.reshape(heads, dim, tokens).transpose(2, 0, 1))

    row_split = P('hid', 'tp')
    col_split = P('tp', 'hid')
    cache_spec = P('dp', 'tp', None)
    in_specs = (P('dp', 'hid'), P('hid'), P('hid'), row_split, row_split, row_split, col_split,
                row_split, row_split, col_split, cache_spec, cache_spec, P('dp'))
    out_specs = (P('dp', 'hid'), cache_spec, cache_spec)
    return jax.shard_map(local_layer, mesh=mesh, in_specs=in_specs, out_specs=out_specs, check_vma=False)
```

```python
import math
import jax
import jax.numpy as jnp
from jax import lax
from jax.experimental import pallas as pl
from jax.experimental.pallas import tpu as pltpu
from jax.sharding import PartitionSpec as P

ROPE_BASE = 10000.0
F32, BF16 = jnp.float32, jnp.bfloat16
NEG = -1e30
BLK = 256
HALF = BLK // 2
PAST_MAX = 1024
NB = 4
CH = 4
CW = 256
MESH = pl.DeviceIdType.MESH

UNITS = ((0, 0, 256), (1, 0, 256), (2, 0, 256), (3, 0, 128), (3, 2, 64), (3, 3, 64))
NU = len(UNITS)
Q, R, C, X, D, T, O = 0, 4, 8, 12, 16, 20, 24
E, Y, F, G = 32, 32 + NU, 32 + 2 * NU, 32 + 3 * NU
A = G + CH * NU
KV = A + CH * NU
N_REMOTE = KV + NB


def rope(t, cos_t, sin_t):
    width = t.shape[1]
    lane = lax.broadcasted_iota(jnp.int32, t.shape, 1)
    swapped = jnp.where((lane & 63) < 32, pltpu.roll(t, width - 32, 1), pltpu.roll(t, 32, 1))
    cos_w = jnp.concatenate([cos_t] * (width // 128), axis=1)
    sin_w = jnp.concatenate([sin_t] * (width // 128), axis=1)
    return (t * cos_w + swapped * sin_w).astype(BF16)


def row_sums(t):
    sq = jnp.broadcast_to(jnp.sum(t * t, axis=1, keepdims=True), (t.shape[0], 128))
    return jnp.transpose(sq)[:8]


def as_column(row):
    return jnp.transpose(jnp.broadcast_to(row[:1], (128, row.shape[1])))[:, :1]


def kernel(d_model, p_hbm, x_hbm, g1_hbm, g2_hbm, wq_hbm, wk_hbm, wv_hbm, wo_hbm, wg_hbm, wu_hbm, wd_hbm, kc_hbm, vc_hbm,
           fin, kc, vc,
           p_ref, g1_ref, g2_ref, x, wq, wk, wv, wo, wg, wu, wd, qsend, qkeep, qrecv, sq1, sq1r, cos_b, sin_b, kt, vv, qs, kvn, kvsend, kvrecv, ob, orecv,
           csend, ckeep, crecv, part, xrecv, mid, sq2, sq2r, hg, sums, gsend, gkeep, grecv, ab, arecv, acc,
           esend, ekeep, erecv, part2, yrecv, lsem, ssem, rsem):
    h = lax.axis_index('hid')
    t = lax.axis_index('tp')
    c = lax.rem(t, 2)
    hid_dev = {'hid': 1 - h}
    core_dev = {'tp': t + 1 - 2 * c}
    x_dev = {'tp': lax.rem(t + 2, 4)}
    own = h == 0

    loads = []

    def load(src, dst):
        n = len(loads)
        cp = pltpu.make_async_copy(src, dst, lsem.at[n])
        cp.start()
        loads.append(cp)
        return cp

    ld_x = [load(x_hbm.at[pl.ds(0, BLK)], x.at[pl.ds(0, BLK)])]
    ld_q = [load(g1_hbm, g1_ref), load(wq_hbm, wq), load(wk_hbm, wk), load(wv_hbm, wv)]
    ld_x += [load(x_hbm.at[pl.ds(BLK, BLK)], x.at[pl.ds(BLK, BLK)])]
    ld_small = [load(p_hbm, p_ref), load(g2_hbm, g2_ref)]

    barrier = pltpu.get_barrier_semaphore()
    for dev in (hid_dev, core_dev, x_dev):
        pl.semaphore_signal(barrier, inc=1, device_id=dev, device_id_type=MESH)

    def remote(src, dst, n, dev):
        return pltpu.make_async_remote_copy(src_ref=src, dst_ref=dst, send_sem=ssem.at[n], recv_sem=rsem.at[n],
                                            device_id=dev, device_id_type=MESH)

    def q_copy(i): return remote(qsend.at[i], qrecv.at[i], Q + i, hid_dev)
    def r_copy(i): return remote(sq1.at[i], sq1r.at[i], R + i, hid_dev)
    def o_copy(i, n): return remote(ob.at[i, n], orecv.at[i, n], O + 2 * i + n, hid_dev)
    def kv_copy(i): return remote(kvsend.at[i], kvrecv.at[i], KV + i, hid_dev)
    def c_copy(i): return remote(csend.at[i], crecv.at[i], C + i, core_dev)
    def x_copy(i): return remote(part.at[i], xrecv.at[i], X + i, x_dev)
    def d_copy(i): return remote(mid.at[i, 0], mid.at[i, 1], D + i, core_dev)
    def t_copy(i): return remote(sq2.at[i], sq2r.at[i], T + i, hid_dev)

    def whole(u):
        return pl.ds(UNITS[u][1] * UNITS[u][2], UNITS[u][2])

    def half(u):
        return pl.ds(UNITS[u][1] * UNITS[u][2] // 2, UNITS[u][2] // 2)

    def g_copy(u, j): return remote(gsend.at[UNITS[u][0], j, whole(u)], grecv.at[UNITS[u][0], j, whole(u)], G + CH * u + j, hid_dev)
    def a_copy(u, j): return remote(ab.at[UNITS[u][0], j, whole(u)], arecv.at[UNITS[u][0], j, whole(u)], A + CH * u + j, hid_dev)
    def e_copy(u): return remote(esend.at[UNITS[u][0], half(u)], erecv.at[UNITS[u][0], half(u)], E + u, core_dev)
    def y_copy(u): return remote(part2.at[UNITS[u][0], half(u)], yrecv.at[UNITS[u][0], half(u)], Y + u, x_dev)
    def f_copy(u): return remote(fin.at[UNITS[u][0], 0, half(u)], fin.at[UNITS[u][0], 1, half(u)], F + u, core_dev)

    def qkv(i, send):
        xf = x[pl.ds(i * BLK, BLK), :].astype(F32)
        xg = (xf * g1_ref[...]).astype(BF16)
        theirs = wq[:, pl.ds(pl.multiple_of((1 - h) * 256, 256), 256)]
        qsend[i, :, :256] = jnp.dot(xg, theirs, preferred_element_type=F32).astype(BF16)
        k = jnp.dot(xg, wk[...], preferred_element_type=F32).astype(BF16)
        v = jnp.dot(xg, wv[...], preferred_element_type=F32).astype(BF16)
        low = jnp.concatenate([k[:, :64], v[:, :64]], axis=1)
        high = jnp.concatenate([k[:, 64:], v[:, 64:]], axis=1)
        qsend[i, :, 256:] = jnp.where(own, high, low)
        if i == 0:
            pl.semaphore_wait(barrier, 3)
        if send:
            q_copy(i).start()
        kvsend[i] = jnp.where(own, low, high)
        mine = wq[:, pl.ds(pl.multiple_of(h * 256, 256), 256)]
        qkeep[i] = jnp.dot(xg, mine, preferred_element_type=F32).astype(BF16)
        sq1[i] = row_sums(xf)
        if send:
            r_copy(i).start()

    def tables(i):
        pos = (p_ref[0] + i * BLK + lax.broadcasted_iota(jnp.int32, (BLK, 128), 0)).astype(F32)
        lane = lax.broadcasted_iota(jnp.int32, (BLK, 128), 1)
        freq = jnp.exp((lane[:8] & 31).astype(F32) * (-2.0 * math.log(ROPE_BASE) / 64))[:1]
        ang = pos * freq
        cos_b[pl.ds(i * BLK, BLK), :] = jnp.cos(ang)
        sin = jnp.sin(ang)
        sin_b[pl.ds(i * BLK, BLK), :] = jnp.where((lane & 63) < 32, -sin, sin)

    def row_factor(i):
        return as_column(lax.rsqrt((sq1[i] + sq1r[i]) / d_model + 1e-5))

    def keys_values(i, r, mine, theirs):
        rows = slice(i * BLK, (i + 1) * BLK)
        kv = ((mine.astype(F32) + theirs.astype(F32)) * r).astype(BF16)
        lane = lax.broadcasted_iota(jnp.int32, kv.shape, 1)
        return jnp.where(lane < 64, rope(kv.astype(F32), cos_b[rows, :], sin_b[rows, :]), kv)

    def att(i):
        rows = slice(i * BLK, (i + 1) * BLK)
        q_copy(i).wait_recv()
        r_copy(i).wait_recv()
        r = row_factor(i)
        cos_t, sin_t = cos_b[rows, :], sin_b[rows, :]
        q = ((qkeep[i].astype(F32) + qrecv[i, :, :256].astype(F32)) * r).astype(BF16)
        kv = keys_values(i, r, kvsend[i], qrecv[i, :, 256:])
        qs[...] = (rope(q.astype(F32), cos_t, sin_t).astype(F32) * 0.125).astype(BF16)
        kv_t = jnp.transpose(kv.astype(F32)).astype(BF16)
        kvn[i] = kv_t
        main = PAST_MAX + i * BLK
        kt[:, main:main + BLK] = kv_t[:64]
        vv[main:main + BLK, :] = kv[:, 64:]
        col = lax.broadcasted_iota(jnp.int32, (1, main), 1)
        bias = jnp.where((col >= p_ref[0]) & (col < PAST_MAX), NEG, 0.0)
        causal = lax.broadcasted_iota(jnp.int32, (BLK, BLK), 1) <= lax.broadcasted_iota(jnp.int32, (BLK, BLK), 0)

        def pair(n, carry):
            lanes = pl.ds(pl.multiple_of(n * 128, 128), 128)
            qp = qs[:, lanes]
            done = []
            for s in range(2):
                qn = qp[:, s * 64:(s + 1) * 64]
                s_main = jnp.dot(qn, kt[:, :main], preferred_element_type=F32) + bias
                s_diag = jnp.where(causal, jnp.dot(qn, kt[:, main:main + BLK], preferred_element_type=F32), NEG)
                top = jnp.maximum(jnp.max(s_main, axis=1, keepdims=True), jnp.max(s_diag, axis=1, keepdims=True))
                e_main = jnp.exp(s_main - top)
                e_diag = jnp.exp(s_diag - top)
                inv = 1.0 / (jnp.sum(e_main, axis=1, keepdims=True) + jnp.sum(e_diag, axis=1, keepdims=True))
                o = jnp.dot((e_main * inv).astype(BF16), vv[:main, :], preferred_element_type=F32)
                o += jnp.dot((e_diag * inv).astype(BF16), vv[main:main + BLK, :], preferred_element_type=F32)
                done.append(o.astype(BF16))
            ob[i, n] = jnp.concatenate(done, axis=1)
            o_copy(i, n).start()
            return carry
        lax.fori_loop(0, 2, pair, 0)

    def wo_step(i):
        o_copy(i, 0).wait_recv()
        o_copy(i, 1).wait_recv()
        mine = jnp.concatenate([ob[i, 0], ob[i, 1]], axis=1)
        theirs = jnp.concatenate([orecv[i, 0], orecv[i, 1]], axis=1)
        acc[...] = jnp.dot(mine, wo[pl.ds(pl.multiple_of(h * 256, 256), 256), :], preferred_element_type=F32)
        acc[...] += jnp.dot(theirs, wo[pl.ds(pl.multiple_of((1 - h) * 256, 256), 256), :], preferred_element_type=F32)
        ckeep[i] = acc[pl.ds(pl.multiple_of(c * HALF, HALF), HALF), :].astype(BF16)
        csend[i] = acc[pl.ds(pl.multiple_of((1 - c) * HALF, HALF), HALF), :].astype(BF16)
        c_copy(i).start()

    def add(a, b):
        return (a.astype(F32) + b.astype(F32)).astype(BF16)

    def c_step(i):
        c_copy(i).wait_recv()
        part[i] = add(ckeep[i], crecv[i])
        x_copy(i).start()

    def x_step(i):
        x_copy(i).wait_recv()
        res = x[pl.ds(pl.multiple_of(i * BLK + c * HALF, HALF), HALF), :]
        mid[i, 0] = add(res, add(part[i], xrecv[i]))
        d_copy(i).start()

    def d_step(i):
        d_copy(i).wait_recv()
        at = 0
        for u in range(NU):
            if UNITS[u][0] != i:
                continue
            for k in range(2):
                n = UNITS[u][2] // 2
                m = mid[i, k, half(u), :].astype(F32)
                sq = jnp.broadcast_to(jnp.sum(m * m, axis=1, keepdims=True), (n, 128))
                sums[at:at + n, :] = sq
                hg[at:at + n, :] = (m * g2_ref[...]).astype(BF16)
                at += n
        sq2[i] = jnp.transpose(sums[...])[:8]

    def gate_up(u, side, j, dst):
        cols = pl.ds(pl.multiple_of(side * (CH * CW) + j * CW, CW), CW)
        rows = hg[whole(u), :]
        dst[:, :CW] = jnp.dot(rows, wg[:, cols], preferred_element_type=F32).astype(BF16)
        dst[:, CW:] = jnp.dot(rows, wu[:, cols], preferred_element_type=F32).astype(BF16)

    def u_step(u, j):
        i = UNITS[u][0]
        gate_up(u, 1 - h, j, gsend.at[i, j, whole(u)])
        g_copy(u, j).start()
        gate_up(u, h, j, gkeep.at[i % 2, j, whole(u)])

    def v_step(u, j):
        i = UNITS[u][0]
        g_copy(u, j).wait_recv()
        r = as_column(lax.rsqrt((sq2[i] + sq2r[i]) / d_model + 1e-5))[UNITS[u][1] * UNITS[u][2]:(UNITS[u][1] + 1) * UNITS[u][2]]
        both = ((gkeep[i % 2, j, whole(u), :].astype(F32) + grecv[i, j, whole(u), :].astype(F32)) * r).astype(BF16).astype(F32)
        g, e = both[:, :CW], both[:, CW:]
        ab[i, j, whole(u), :] = (g * jax.nn.sigmoid(g) * e).astype(BF16)
        a_copy(u, j).start()

    def w_step(u, j):
        i = UNITS[u][0]
        a_copy(u, j).wait_recv()
        mine = wd[pl.ds(pl.multiple_of(h * (CH * CW) + j * CW, CW), CW), :]
        theirs = wd[pl.ds(pl.multiple_of((1 - h) * (CH * CW) + j * CW, CW), CW), :]
        y = jnp.dot(ab[i, j, whole(u), :], mine, preferred_element_type=F32)
        y += jnp.dot(arecv[i, j, whole(u), :], theirs, preferred_element_type=F32)
        acc[whole(u), :] = jnp.where(j == 0, 0.0, acc[whole(u), :]) + y

    def e_start(u):
        i, k, n = UNITS[u]
        ekeep[i, half(u), :] = acc[k * n:k * n + n // 2, :].astype(BF16)
        esend[i, half(u), :] = acc[k * n + n // 2:k * n + n, :].astype(BF16)
        e_copy(u).start()

    def e_step(u):
        i = UNITS[u][0]
        e_copy(u).wait_recv()
        part2[i, half(u), :] = add(ekeep[i, half(u), :], erecv[i, half(u), :])
        y_copy(u).start()

    def y_step(u):
        i = UNITS[u][0]
        y_copy(u).wait_recv()
        down = add(part2[i, half(u), :], yrecv[i, half(u), :])
        fin[i, 0, half(u), :] = add(mid[i, 0, half(u), :], down)
        f_copy(u).start()

    def f_step(u):
        f_copy(u).wait_recv()

    def loop(*steps):
        def body(j, carry):
            for step, i in steps:
                step(i, j)
            return carry
        lax.fori_loop(0, CH, body, 0)

    def place(i, head, kv_t):
        lanes = pl.ds(pl.multiple_of(head * 64, 64), 64)

        def tile(n, carry):
            cols = pl.ds(pl.multiple_of(n * BLK, BLK), BLK)
            first = (n - i) * BLK - p_ref[0]
            at = first + lax.broadcasted_iota(jnp.int32, (BLK, BLK), 1)
            pick = jnp.where(at == lax.broadcasted_iota(jnp.int32, (BLK, BLK), 0), 1.0, 0.0).astype(BF16)
            new = jnp.dot(kv_t, pick, preferred_element_type=F32)
            where = first + lax.broadcasted_iota(jnp.int32, (64, BLK), 1)
            fresh = (where >= 0) & (where < BLK)
            kc[lanes, cols] = jnp.where(fresh, new[:64], kc[lanes, cols].astype(F32)).astype(BF16)
            vc[lanes, cols] = jnp.where(fresh, new[64:], vc[lanes, cols].astype(F32)).astype(BF16)
            return carry
        lax.fori_loop(i + 1, i + 1 + PAST_MAX // BLK, tile, 0)

    def kv_step(i):
        kv_copy(i).wait_recv()
        kv = keys_values(i, row_factor(i), qsend[i, :, 256:], kvrecv[i])
        place(i, 1 - h, jnp.transpose(kv.astype(F32)).astype(BF16))

    for cp in ld_q:
        cp.wait()
    ld_x[0].wait()
    qkv(0, True)
    ld_x += [load(x_hbm.at[pl.ds(i * BLK, BLK)], x.at[pl.ds(i * BLK, BLK)]) for i in range(2, NB)]
    ld_kc, ld_vc = load(kc_hbm, kc), load(vc_hbm, vc)
    ld_wo = load(wo_hbm, wo)
    ld_gu = [load(wg_hbm, wg), load(wu_hbm, wu)]
    ld_wd = load(wd_hbm, wd)
    for i in range(1, NB):
        ld_x[i].wait()
        qkv(i, i < 2)
    for cp in ld_small:
        cp.wait()
    for i in range(NB):
        tables(i)
    ld_kc.wait()
    ld_vc.wait()
    kt[:, :PAST_MAX] = kc[pl.ds(pl.multiple_of(h * 64, 64), 64), :PAST_MAX]
    v_old = jnp.transpose(vc[:, :PAST_MAX].astype(F32)).astype(BF16)
    vv[:PAST_MAX, :] = jnp.where(own, v_old[:, :64], v_old[:, 64:])
    att(0)
    q_copy(2).start()
    r_copy(2).start()
    att(1)
    q_copy(3).start()
    r_copy(3).start()
    ld_wo.wait()
    wo_step(0)
    c_step(0)
    att(2)
    x_step(0)
    wo_step(1)
    d_step(0)
    for cp in ld_gu:
        cp.wait()
    t_copy(0).start()
    loop((u_step, 0))
    c_step(1)
    att(3)
    x_step(1)
    wo_step(2)
    d_step(1)
    t_copy(1).start()
    t_copy(0).wait_recv()
    c_step(2)
    loop((u_step, 1), (v_step, 0))
    x_step(2)
    wo_step(3)
    c_step(3)
    d_step(2)
    t_copy(2).start()
    t_copy(1).wait_recv()
    ld_wd.wait()
    loop((u_step, 2), (v_step, 1), (w_step, 0))
    e_start(0)
    x_step(3)
    d_step(3)
    t_copy(3).start()
    e_step(0)
    t_copy(2).wait_recv()
    for i in range(NB):
        place(i, h, kvn[i])
    loop((u_step, 3), (v_step, 2), (w_step, 1))
    loop((u_step, 4))
    loop((u_step, 5))
    e_start(1)
    y_step(0)
    e_step(1)
    f_step(0)
    t_copy(3).wait_recv()
    loop((v_step, 3), (w_step, 2))
    e_start(2)
    y_step(1)
    e_step(2)
    f_step(1)
    loop((v_step, 4))
    loop((v_step, 5))
    for i in range(NB):
        kv_copy(i).start()
    y_step(2)
    loop((w_step, 3))
    e_start(3)
    f_step(2)
    w_step(4, 0)
    e_step(3)
    for j in range(1, CH):
        w_step(4, j)
    e_start(4)
    w_step(5, 0)
    e_step(4)
    for j in range(1, CH):
        w_step(5, j)
    e_start(5)
    y_step(3)
    e_step(5)
    kv_step(0)
    y_step(4)
    f_step(3)
    kv_step(1)
    kv_step(2)
    y_step(5)
    f_step(4)
    kv_step(3)
    f_step(5)

    for i in range(NB):
        for cp in (q_copy, r_copy, kv_copy, c_copy, x_copy, d_copy, t_copy):
            cp(i).wait_send()
        for n in range(2):
            o_copy(i, n).wait_send()
    for u in range(NU):
        for cp in (e_copy, y_copy, f_copy):
            cp(u).wait_send()

        def drain(j, carry, u=u):
            g_copy(u, j).wait_send()
            a_copy(u, j).wait_send()
            return carry
        lax.fori_loop(0, CH, drain, 0)


def results_body(fin, kc, vc, out_hbm, ko_hbm, vo_hbm, sem):
    c = lax.rem(lax.axis_index('tp'), 2)
    copies = [pltpu.make_async_copy(kc, ko_hbm, sem.at[2 * NB]), pltpu.make_async_copy(vc, vo_hbm, sem.at[2 * NB + 1])]
    for i in range(NB):
        for k in range(2):
            at = pl.multiple_of(i * BLK + (c if k == 0 else 1 - c) * HALF, HALF)
            copies.append(pltpu.make_async_copy(fin.at[i, k], out_hbm.at[pl.ds(at, HALF)], sem.at[2 * i + k]))
    for cp in copies:
        cp.start()
    for cp in copies:
        cp.wait()


def solution(mesh):
    def local_layer(hidden, rms_attn, rms_mlp, w_q, w_k, w_v, w_o, w_gate, w_up, w_down, k_cache, v_cache, past_len):
        new_len, width = hidden.shape
        tokens = k_cache.shape[0]
        k_flat = k_cache.transpose(1, 2, 0).reshape(-1, tokens)
        v_flat = v_cache.transpose(1, 2, 0).reshape(-1, tokens)
        any_spec = pl.BlockSpec(memory_space=pl.ANY)

        def v(*shape, dtype=BF16):
            return pltpu.VMEM(shape, dtype)
        tok = v(NB, HALF, width)
        scratch = [
            pltpu.SMEM((1,), jnp.int32), v(1, width, dtype=F32), v(1, width, dtype=F32),
            v(new_len, width), v(*w_q.shape), v(*w_k.shape), v(*w_v.shape), v(*w_o.shape), v(*w_gate.shape), v(*w_up.shape), v(*w_down.shape),
            v(NB, BLK, 384), v(NB, BLK, 256), v(NB, BLK, 384), v(NB, 8, BLK, dtype=F32), v(NB, 8, BLK, dtype=F32),
            v(new_len, 128, dtype=F32), v(new_len, 128, dtype=F32), v(64, PAST_MAX + new_len), v(PAST_MAX + new_len, 64),
            v(BLK, 256), v(NB, 128, BLK), v(NB, BLK, 128), v(NB, BLK, 128), v(NB, 2, BLK, 128), v(NB, 2, BLK, 128),
            tok, tok, tok, tok, tok, v(NB, 2, HALF, width), v(NB, 8, BLK, dtype=F32), v(NB, 8, BLK, dtype=F32), v(BLK, width), v(BLK, 128, dtype=F32),
            v(NB, CH, BLK, 2 * CW), v(2, CH, BLK, 2 * CW), v(NB, CH, BLK, 2 * CW), v(NB, CH, BLK, CW), v(NB, CH, BLK, CW),
            v(BLK, width, dtype=F32),
            tok, tok, tok, tok, tok,
            pltpu.SemaphoreType.DMA((16,)),
            pltpu.SemaphoreType.DMA((N_REMOTE,)), pltpu.SemaphoreType.DMA((N_REMOTE,)),
        ]
        kept = ((NB, 2, HALF, width), k_flat.shape, v_flat.shape)
        vmem_spec = pl.BlockSpec(memory_space=pltpu.VMEM)
        done = pl.pallas_call(
            lambda *refs: kernel(2 * width, *refs),
            out_shape=tuple(v(*a) for a in kept),
            in_specs=[any_spec] * 13,
            out_specs=(vmem_spec,) * 3,
            scratch_shapes=scratch,
            compiler_params=pltpu.CompilerParams(collective_id=0, has_side_effects=True, vmem_limit_bytes=60 << 20),
            name="layer",
        )(past_len, hidden, rms_attn.reshape(1, width), rms_mlp.reshape(1, width), w_q, w_k, w_v, w_o, w_gate, w_up, w_down,
          k_flat, v_flat)
        out, k_full, v_full = pl.pallas_call(
            results_body,
            out_shape=tuple(jax.ShapeDtypeStruct(a, BF16) for a in (hidden.shape, k_flat.shape, v_flat.shape)),
            in_specs=[vmem_spec] * 3, out_specs=(any_spec,) * 3,
            scratch_shapes=[pltpu.SemaphoreType.DMA((2 * NB + 2,))],
            compiler_params=pltpu.CompilerParams(vmem_limit_bytes=1 << 20),
            name="results",
        )(*done)
        heads, dim = k_cache.shape[1:]
        return (out, k_full.reshape(heads, dim, tokens).transpose(2, 0, 1), v_full.reshape(heads, dim, tokens).transpose(2, 0, 1))

    row_split = P('hid', 'tp')
    col_split = P('tp', 'hid')
    cache_spec = P('dp', 'tp', None)
    in_specs = (P('dp', 'hid'), P('hid'), P('hid'), row_split, row_split, row_split, col_split,
                row_split, row_split, col_split, cache_spec, cache_spec, P('dp'))
    out_specs = (P('dp', 'hid'), cache_spec, cache_spec)
    return jax.shard_map(local_layer, mesh=mesh, in_specs=in_specs, out_specs=out_specs, check_vma=False)
```

```python
import math
import jax
import jax.numpy as jnp
from jax import lax
from jax.experimental import pallas as pl
from jax.experimental.pallas import tpu as pltpu
from jax.sharding import PartitionSpec as P

ROPE_BASE = 10000.0
F32, BF16 = jnp.float32, jnp.bfloat16
NEG = -1e30
BLK = 256
HALF = BLK // 2
PAST_MAX = 1024
NB = 4
CH = 4
CW = 256
MESH = pl.DeviceIdType.MESH

UNITS = ((0, 0, 256), (1, 0, 256), (2, 0, 256), (3, 0, 128), (3, 2, 64), (3, 3, 64))
NU = len(UNITS)
Q, R, C, X, D, T, O = 0, 4, 8, 12, 16, 20, 24
E, Y, F, G = 32, 32 + NU, 32 + 2 * NU, 32 + 3 * NU
A = G + CH * NU
KV = A + CH * NU
N_REMOTE = KV + NB


def rope(t, cos_t, sin_t):
    width = t.shape[1]
    lane = lax.broadcasted_iota(jnp.int32, t.shape, 1)
    swapped = jnp.where((lane & 63) < 32, pltpu.roll(t, width - 32, 1), pltpu.roll(t, 32, 1))
    cos_w = jnp.concatenate([cos_t] * (width // 128), axis=1)
    sin_w = jnp.concatenate([sin_t] * (width // 128), axis=1)
    return (t * cos_w + swapped * sin_w).astype(BF16)


def row_sums(t):
    sq = jnp.broadcast_to(jnp.sum(t * t, axis=1, keepdims=True), (t.shape[0], 128))
    return jnp.transpose(sq)[:8]


def as_column(row):
    return jnp.transpose(jnp.broadcast_to(row[:1], (128, row.shape[1])))[:, :1]


def kernel(d_model, p_hbm, x_hbm, g1_hbm, g2_hbm, wq_hbm, wk_hbm, wv_hbm, wo_hbm, wg_hbm, wu_hbm, wd_hbm, kc_hbm, vc_hbm,
           out, kc, vc,
           p_ref, g1_ref, g2_ref, x, wq, wk, wv, wo, wg, wu, wd, qsend, qkeep, qrecv, sq1, sq1r, cos_b, sin_b, kt, vv, qs, kvn, kvsend, kvrecv, picks, ob, orecv,
           csend, ckeep, crecv, part, xrecv, mid, sq2, sq2r, hg, sums, gsend, gkeep, grecv, ab, arecv, acc,
           esend, ekeep, erecv, part2, yrecv, lsem, ssem, rsem):
    h = lax.axis_index('hid')
    t = lax.axis_index('tp')
    c = lax.rem(t, 2)
    hid_dev = {'hid': 1 - h}
    core_dev = {'tp': t + 1 - 2 * c}
    x_dev = {'tp': lax.rem(t + 2, 4)}
    own = h == 0

    loads = []

    def load(src, dst):
        n = len(loads)
        cp = pltpu.make_async_copy(src, dst, lsem.at[n])
        cp.start()
        loads.append(cp)
        return cp

    ld_x = [load(x_hbm.at[pl.ds(0, BLK)], x.at[pl.ds(0, BLK)])]
    ld_q = [load(g1_hbm, g1_ref), load(wq_hbm, wq), load(wk_hbm, wk), load(wv_hbm, wv)]
    ld_x += [load(x_hbm.at[pl.ds(BLK, BLK)], x.at[pl.ds(BLK, BLK)])]
    ld_small = [load(p_hbm, p_ref), load(g2_hbm, g2_ref)]

    barrier = pltpu.get_barrier_semaphore()
    for dev in (hid_dev, core_dev, x_dev):
        pl.semaphore_signal(barrier, inc=1, device_id=dev, device_id_type=MESH)

    def remote(src, dst, n, dev):
        return pltpu.make_async_remote_copy(src_ref=src, dst_ref=dst, send_sem=ssem.at[n], recv_sem=rsem.at[n],
                                            device_id=dev, device_id_type=MESH)

    def q_copy(i): return remote(qsend.at[i], qrecv.at[i], Q + i, hid_dev)
    def r_copy(i): return remote(sq1.at[i], sq1r.at[i], R + i, hid_dev)
    def o_copy(i, n): return remote(ob.at[i, n], orecv.at[i, n], O + 2 * i + n, hid_dev)
    def kv_copy(i): return remote(kvsend.at[i], kvrecv.at[i], KV + i, hid_dev)
    def c_copy(i): return remote(csend.at[i], crecv.at[i], C + i, core_dev)
    def x_copy(i): return remote(part.at[i], xrecv.at[i], X + i, x_dev)
    def d_copy(i): return remote(mid.at[i, 0], mid.at[i, 1], D + i, core_dev)
    def t_copy(i): return remote(sq2.at[i], sq2r.at[i], T + i, hid_dev)

    def whole(u):
        return pl.ds(UNITS[u][1] * UNITS[u][2], UNITS[u][2])

    def half(u):
        return pl.ds(UNITS[u][1] * UNITS[u][2] // 2, UNITS[u][2] // 2)

    def own_rows(u):
        i, part_no, n = UNITS[u]
        return pl.ds(pl.multiple_of(i * BLK + c * HALF + part_no * (n // 2), 32), n // 2)

    def g_copy(u, j): return remote(gsend.at[UNITS[u][0], j, whole(u)], grecv.at[UNITS[u][0], j, whole(u)], G + CH * u + j, hid_dev)
    def a_copy(u, j): return remote(ab.at[UNITS[u][0], j, whole(u)], arecv.at[UNITS[u][0], j, whole(u)], A + CH * u + j, hid_dev)
    def e_copy(u): return remote(esend.at[UNITS[u][0], half(u)], erecv.at[UNITS[u][0], half(u)], E + u, core_dev)
    def y_copy(u): return remote(part2.at[UNITS[u][0], half(u)], yrecv.at[UNITS[u][0], half(u)], Y + u, x_dev)
    def f_copy(u):
        rows = own_rows(u)
        return remote(out.at[rows], out.at[rows], F + u, core_dev)

    def qkv(i, send):
        xf = x[pl.ds(i * BLK, BLK), :].astype(F32)
        xg = (xf * g1_ref[...]).astype(BF16)
        theirs = wq[:, pl.ds(pl.multiple_of((1 - h) * 256, 256), 256)]
        qsend[i, :, :256] = jnp.dot(xg, theirs, preferred_element_type=F32).astype(BF16)
        k = jnp.dot(xg, wk[...], preferred_element_type=F32).astype(BF16)
        v = jnp.dot(xg, wv[...], preferred_element_type=F32).astype(BF16)
        low = jnp.concatenate([k[:, :64], v[:, :64]], axis=1)
        high = jnp.concatenate([k[:, 64:], v[:, 64:]], axis=1)
        qsend[i, :, 256:] = jnp.where(own, high, low)
        if i == 0:
            pl.semaphore_wait(barrier, 3)
        if send:
            q_copy(i).start()
        kvsend[i] = jnp.where(own, low, high)
        mine = wq[:, pl.ds(pl.multiple_of(h * 256, 256), 256)]
        qkeep[i] = jnp.dot(xg, mine, preferred_element_type=F32).astype(BF16)
        sq1[i] = row_sums(xf)
        if send:
            r_copy(i).start()

    def tables(i):
        pos = (p_ref[0] + i * BLK + lax.broadcasted_iota(jnp.int32, (BLK, 128), 0)).astype(F32)
        lane = lax.broadcasted_iota(jnp.int32, (BLK, 128), 1)
        freq = jnp.exp((lane[:8] & 31).astype(F32) * (-2.0 * math.log(ROPE_BASE) / 64))[:1]
        ang = pos * freq
        cos_b[pl.ds(i * BLK, BLK), :] = jnp.cos(ang)
        sin = jnp.sin(ang)
        sin_b[pl.ds(i * BLK, BLK), :] = jnp.where((lane & 63) < 32, -sin, sin)

    def row_factor(i):
        return as_column(lax.rsqrt((sq1[i] + sq1r[i]) / d_model + 1e-5))

    def keys_values(i, r, mine, theirs):
        rows = slice(i * BLK, (i + 1) * BLK)
        kv = ((mine.astype(F32) + theirs.astype(F32)) * r).astype(BF16)
        lane = lax.broadcasted_iota(jnp.int32, kv.shape, 1)
        return jnp.where(lane < 64, rope(kv.astype(F32), cos_b[rows, :], sin_b[rows, :]), kv)

    def att(i):
        rows = slice(i * BLK, (i + 1) * BLK)
        q_copy(i).wait_recv()
        r_copy(i).wait_recv()
        r = row_factor(i)
        cos_t, sin_t = cos_b[rows, :], sin_b[rows, :]
        q = ((qkeep[i].astype(F32) + qrecv[i, :, :256].astype(F32)) * r).astype(BF16)
        kv = keys_values(i, r, kvsend[i], qrecv[i, :, 256:])
        qs[...] = (rope(q.astype(F32), cos_t, sin_t).astype(F32) * 0.125).astype(BF16)
        kv_t = jnp.transpose(kv.astype(F32)).astype(BF16)
        kvn[i] = kv_t
        main = PAST_MAX + i * BLK
        kt[:, main:main + BLK] = kv_t[:64]
        vv[main:main + BLK, :] = kv[:, 64:]
        col = lax.broadcasted_iota(jnp.int32, (1, main), 1)
        bias = jnp.where((col >= p_ref[0]) & (col < PAST_MAX), NEG, 0.0)
        causal = lax.broadcasted_iota(jnp.int32, (BLK, BLK), 1) <= lax.broadcasted_iota(jnp.int32, (BLK, BLK), 0)

        def pair(n, carry):
            lanes = pl.ds(pl.multiple_of(n * 128, 128), 128)
            qp = qs[:, lanes]
            done = []
            for s in range(2):
                qn = qp[:, s * 64:(s + 1) * 64]
                s_main = jnp.dot(qn, kt[:, :main], preferred_element_type=F32) + bias
                s_diag = jnp.where(causal, jnp.dot(qn, kt[:, main:main + BLK], preferred_element_type=F32), NEG)
                top = jnp.maximum(jnp.max(s_main, axis=1, keepdims=True), jnp.max(s_diag, axis=1, keepdims=True))
                e_main = jnp.exp(s_main - top)
                e_diag = jnp.exp(s_diag - top)
                inv = 1.0 / (jnp.sum(e_main, axis=1, keepdims=True) + jnp.sum(e_diag, axis=1, keepdims=True))
                o = jnp.dot((e_main * inv).astype(BF16), vv[:main, :], preferred_element_type=F32)
                o += jnp.dot((e_diag * inv).astype(BF16), vv[main:main + BLK, :], preferred_element_type=F32)
                done.append(o.astype(BF16))
            ob[i, n] = jnp.concatenate(done, axis=1)
            o_copy(i, n).start()
            return carry
        lax.fori_loop(0, 2, pair, 0)

    def wo_step(i):
        o_copy(i, 0).wait_recv()
        o_copy(i, 1).wait_recv()
        mine = jnp.concatenate([ob[i, 0], ob[i, 1]], axis=1)
        theirs = jnp.concatenate([orecv[i, 0], orecv[i, 1]], axis=1)
        acc[...] = jnp.dot(mine, wo[pl.ds(pl.multiple_of(h * 256, 256), 256), :], preferred_element_type=F32)
        acc[...] += jnp.dot(theirs, wo[pl.ds(pl.multiple_of((1 - h) * 256, 256), 256), :], preferred_element_type=F32)
        ckeep[i] = acc[pl.ds(pl.multiple_of(c * HALF, HALF), HALF), :].astype(BF16)
        csend[i] = acc[pl.ds(pl.multiple_of((1 - c) * HALF, HALF), HALF), :].astype(BF16)
        c_copy(i).start()

    def add(a, b):
        return (a.astype(F32) + b.astype(F32)).astype(BF16)

    def c_step(i):
        c_copy(i).wait_recv()
        part[i] = add(ckeep[i], crecv[i])
        x_copy(i).start()

    def x_step(i):
        x_copy(i).wait_recv()
        res = x[pl.ds(pl.multiple_of(i * BLK + c * HALF, HALF), HALF), :]
        mid[i, 0] = add(res, add(part[i], xrecv[i]))
        d_copy(i).start()

    def d_step(i):
        d_copy(i).wait_recv()
        at = 0
        for u in range(NU):
            if UNITS[u][0] != i:
                continue
            for k in range(2):
                n = UNITS[u][2] // 2
                m = mid[i, k, half(u), :].astype(F32)
                sq = jnp.broadcast_to(jnp.sum(m * m, axis=1, keepdims=True), (n, 128))
                sums[at:at + n, :] = sq
                hg[at:at + n, :] = (m * g2_ref[...]).astype(BF16)
                at += n
        sq2[i] = jnp.transpose(sums[...])[:8]

    def gate_up(u, side, j, dst):
        cols = pl.ds(pl.multiple_of(side * (CH * CW) + j * CW, CW), CW)
        rows = hg[whole(u), :]
        dst[:, :CW] = jnp.dot(rows, wg[:, cols], preferred_element_type=F32).astype(BF16)
        dst[:, CW:] = jnp.dot(rows, wu[:, cols], preferred_element_type=F32).astype(BF16)

    def u_step(u, j):
        i = UNITS[u][0]
        gate_up(u, 1 - h, j, gsend.at[i, j, whole(u)])
        g_copy(u, j).start()
        gate_up(u, h, j, gkeep.at[i % 2, j, whole(u)])

    def v_step(u, j):
        i = UNITS[u][0]
        g_copy(u, j).wait_recv()
        r = as_column(lax.rsqrt((sq2[i] + sq2r[i]) / d_model + 1e-5))[UNITS[u][1] * UNITS[u][2]:(UNITS[u][1] + 1) * UNITS[u][2]]
        both = ((gkeep[i % 2, j, whole(u), :].astype(F32) + grecv[i, j, whole(u), :].astype(F32)) * r).astype(BF16).astype(F32)
        g, e = both[:, :CW], both[:, CW:]
        ab[i, j, whole(u), :] = (g * jax.nn.sigmoid(g) * e).astype(BF16)
        a_copy(u, j).start()

    def w_step(u, j):
        i = UNITS[u][0]
        a_copy(u, j).wait_recv()
        mine = wd[pl.ds(pl.multiple_of(h * (CH * CW) + j * CW, CW), CW), :]
        theirs = wd[pl.ds(pl.multiple_of((1 - h) * (CH * CW) + j * CW, CW), CW), :]
        y = jnp.dot(ab[i, j, whole(u), :], mine, preferred_element_type=F32)
        y += jnp.dot(arecv[i, j, whole(u), :], theirs, preferred_element_type=F32)
        acc[whole(u), :] = jnp.where(j == 0, 0.0, acc[whole(u), :]) + y

    def e_start(u):
        i, k, n = UNITS[u]
        ekeep[i, half(u), :] = acc[k * n:k * n + n // 2, :].astype(BF16)
        esend[i, half(u), :] = acc[k * n + n // 2:k * n + n, :].astype(BF16)
        e_copy(u).start()

    def e_step(u):
        i = UNITS[u][0]
        e_copy(u).wait_recv()
        part2[i, half(u), :] = add(ekeep[i, half(u), :], erecv[i, half(u), :])
        y_copy(u).start()

    def y_step(u):
        i = UNITS[u][0]
        y_copy(u).wait_recv()
        down = add(part2[i, half(u), :], yrecv[i, half(u), :])
        out[own_rows(u), :] = add(mid[i, 0, half(u), :], down)
        f_copy(u).start()

    def f_step(u):
        f_copy(u).wait_recv()

    def loop(*steps):
        def body(j, carry):
            for step, i in steps:
                step(i, j)
            return carry
        lax.fori_loop(0, CH, body, 0)

    span = PAST_MAX

    def make_picks():
        at = BLK - p_ref[0] + lax.broadcasted_iota(jnp.int32, (BLK, span), 1)
        picks[...] = jnp.where(at == lax.broadcasted_iota(jnp.int32, (BLK, span), 0), 1.0, 0.0).astype(BF16)

    def place(i, head, kv_t):
        lanes = pl.ds(pl.multiple_of(head * 64, 64), 64)
        cols = slice((i + 1) * BLK, (i + 1) * BLK + span)
        where = BLK - p_ref[0] + lax.broadcasted_iota(jnp.int32, (1, span), 1)
        fresh = (where >= 0) & (where < BLK)
        new = jnp.dot(kv_t, picks[...], preferred_element_type=F32)
        kc[lanes, cols] = jnp.where(fresh, new[:64], kc[lanes, cols].astype(F32)).astype(BF16)
        vc[lanes, cols] = jnp.where(fresh, new[64:], vc[lanes, cols].astype(F32)).astype(BF16)

    def kv_step(i):
        r = row_factor(i)
        kv_copy(i).wait_recv()
        kv = keys_values(i, r, qsend[i, :, 256:], kvrecv[i])
        place(i, 1 - h, jnp.transpose(kv.astype(F32)).astype(BF16))

    for cp in ld_q:
        cp.wait()
    ld_x[0].wait()
    qkv(0, True)
    ld_x += [load(x_hbm.at[pl.ds(i * BLK, BLK)], x.at[pl.ds(i * BLK, BLK)]) for i in range(2, NB)]
    ld_kc, ld_vc = load(kc_hbm, kc), load(vc_hbm, vc)
    ld_wo = load(wo_hbm, wo)
    ld_gu = [load(wg_hbm, wg), load(wu_hbm, wu)]
    ld_wd = load(wd_hbm, wd)
    for i in range(1, NB):
        ld_x[i].wait()
        qkv(i, i < 2)
    for cp in ld_small:
        cp.wait()
    for i in range(NB):
        tables(i)
    ld_kc.wait()
    ld_vc.wait()
    kt[:, :PAST_MAX] = kc[pl.ds(pl.multiple_of(h * 64, 64), 64), :PAST_MAX]
    v_old = jnp.transpose(vc[:, :PAST_MAX].astype(F32)).astype(BF16)
    vv[:PAST_MAX, :] = jnp.where(own, v_old[:, :64], v_old[:, 64:])
    att(0)
    q_copy(2).start()
    r_copy(2).start()
    att(1)
    q_copy(3).start()
    r_copy(3).start()
    ld_wo.wait()
    wo_step(0)
    c_step(0)
    att(2)
    x_step(0)
    wo_step(1)
    d_step(0)
    for cp in ld_gu:
        cp.wait()
    t_copy(0).start()
    loop((u_step, 0))
    c_step(1)
    att(3)
    x_step(1)
    wo_step(2)
    d_step(1)
    t_copy(1).start()
    t_copy(0).wait_recv()
    c_step(2)
    loop((u_step, 1), (v_step, 0))
    x_step(2)
    wo_step(3)
    c_step(3)
    d_step(2)
    t_copy(2).start()
    t_copy(1).wait_recv()
    ld_wd.wait()
    loop((u_step, 2), (v_step, 1), (w_step, 0))
    e_start(0)
    x_step(3)
    d_step(3)
    t_copy(3).start()
    e_step(0)
    t_copy(2).wait_recv()
    make_picks()
    for i in range(NB):
        place(i, h, kvn[i])
    loop((u_step, 3), (v_step, 2), (w_step, 1))
    loop((u_step, 4))
    loop((u_step, 5))
    e_start(1)
    y_step(0)
    e_step(1)
    f_step(0)
    t_copy(3).wait_recv()
    loop((v_step, 3), (w_step, 2))
    e_start(2)
    y_step(1)
    e_step(2)
    f_step(1)
    loop((v_step, 4))
    loop((v_step, 5))
    for i in range(NB):
        kv_copy(i).start()
    y_step(2)
    loop((w_step, 3))
    e_start(3)
    f_step(2)
    w_step(4, 0)
    e_step(3)
    for j in range(1, CH):
        w_step(4, j)
    e_start(4)
    w_step(5, 0)
    e_step(4)
    for j in range(1, CH):
        w_step(5, j)
    e_start(5)
    y_step(3)
    e_step(5)
    kv_step(0)
    y_step(4)
    f_step(3)
    kv_step(1)
    kv_step(2)
    y_step(5)
    f_step(4)
    for i in range(NB):
        for cp in (q_copy, r_copy, c_copy, x_copy, d_copy, t_copy):
            cp(i).wait_send()
        for n in range(2):
            o_copy(i, n).wait_send()
    for u in range(NU):
        def drain(j, carry, u=u):
            g_copy(u, j).wait_send()
            a_copy(u, j).wait_send()
            return carry
        lax.fori_loop(0, CH, drain, 0)
        for cp in (e_copy, y_copy, f_copy):
            cp(u).wait_send()
    f_step(5)
    kv_step(3)
    for i in range(NB):
        kv_copy(i).wait_send()


def results_body(out, kc, vc, out_hbm, ko_hbm, vo_hbm, sem):
    copies = [pltpu.make_async_copy(out.at[pl.ds(i * BLK, BLK)], out_hbm.at[pl.ds(i * BLK, BLK)], sem.at[i]) for i in range(NB)]
    copies += [pltpu.make_async_copy(kc, ko_hbm, sem.at[NB]), pltpu.make_async_copy(vc, vo_hbm, sem.at[NB + 1])]
    for cp in copies:
        cp.start()
    for cp in copies:
        cp.wait()


def solution(mesh):
    def local_layer(hidden, rms_attn, rms_mlp, w_q, w_k, w_v, w_o, w_gate, w_up, w_down, k_cache, v_cache, past_len):
        new_len, width = hidden.shape
        tokens = k_cache.shape[0]
        k_flat = k_cache.transpose(1, 2, 0).reshape(-1, tokens)
        v_flat = v_cache.transpose(1, 2, 0).reshape(-1, tokens)
        any_spec = pl.BlockSpec(memory_space=pl.ANY)

        def v(*shape, dtype=BF16):
            return pltpu.VMEM(shape, dtype)
        tok = v(NB, HALF, width)
        scratch = [
            pltpu.SMEM((1,), jnp.int32), v(1, width, dtype=F32), v(1, width, dtype=F32),
            v(new_len, width), v(*w_q.shape), v(*w_k.shape), v(*w_v.shape), v(*w_o.shape), v(*w_gate.shape), v(*w_up.shape), v(*w_down.shape),
            v(NB, BLK, 384), v(NB, BLK, 256), v(NB, BLK, 384), v(NB, 8, BLK, dtype=F32), v(NB, 8, BLK, dtype=F32),
            v(new_len, 128, dtype=F32), v(new_len, 128, dtype=F32), v(64, PAST_MAX + new_len), v(PAST_MAX + new_len, 64),
            v(BLK, 256), v(NB, 128, BLK), v(NB, BLK, 128), v(NB, BLK, 128), v(BLK, PAST_MAX), v(NB, 2, BLK, 128), v(NB, 2, BLK, 128),
            tok, tok, tok, tok, tok, v(NB, 2, HALF, width), v(NB, 8, BLK, dtype=F32), v(NB, 8, BLK, dtype=F32), v(BLK, width), v(BLK, 128, dtype=F32),
            v(NB, CH, BLK, 2 * CW), v(2, CH, BLK, 2 * CW), v(NB, CH, BLK, 2 * CW), v(NB, CH, BLK, CW), v(NB, CH, BLK, CW),
            v(BLK, width, dtype=F32),
            tok, tok, tok, tok, tok,
            pltpu.SemaphoreType.DMA((16,)),
            pltpu.SemaphoreType.DMA((N_REMOTE,)), pltpu.SemaphoreType.DMA((N_REMOTE,)),
        ]
        vmem_spec = pl.BlockSpec(memory_space=pltpu.VMEM)
        done = pl.pallas_call(
            lambda *refs: kernel(2 * width, *refs),
            out_shape=tuple(v(*a) for a in (hidden.shape, k_flat.shape, v_flat.shape)),
            in_specs=[any_spec] * 13,
            out_specs=(vmem_spec,) * 3,
            scratch_shapes=scratch,
            compiler_params=pltpu.CompilerParams(collective_id=0, has_side_effects=True, vmem_limit_bytes=60 << 20),
            name="layer",
        )(past_len, hidden, rms_attn.reshape(1, width), rms_mlp.reshape(1, width), w_q, w_k, w_v, w_o, w_gate, w_up, w_down,
          k_flat, v_flat)
        out, k_full, v_full = pl.pallas_call(
            results_body,
            out_shape=tuple(jax.ShapeDtypeStruct(a, BF16) for a in (hidden.shape, k_flat.shape, v_flat.shape)),
            in_specs=[vmem_spec] * 3, out_specs=(any_spec,) * 3,
            scratch_shapes=[pltpu.SemaphoreType.DMA((NB + 2,))],
            compiler_params=pltpu.CompilerParams(vmem_limit_bytes=1 << 20),
            name="results",
        )(*done)
        heads, dim = k_cache.shape[1:]
        return (out, k_full.reshape(heads, dim, tokens).transpose(2, 0, 1), v_full.reshape(heads, dim, tokens).transpose(2, 0, 1))

    row_split = P('hid', 'tp')
    col_split = P('tp', 'hid')
    cache_spec = P('dp', 'tp', None)
    in_specs = (P('dp', 'hid'), P('hid'), P('hid'), row_split, row_split, row_split, col_split,
                row_split, row_split, col_split, cache_spec, cache_spec, P('dp'))
    out_specs = (P('dp', 'hid'), cache_spec, cache_spec)
    return jax.shard_map(local_layer, mesh=mesh, in_specs=in_specs, out_specs=out_specs, check_vma=False)
```

```python
import math
import jax
import jax.numpy as jnp
from jax import lax
from jax.experimental import pallas as pl
from jax.experimental.pallas import tpu as pltpu
from jax.sharding import PartitionSpec as P

ROPE_BASE = 10000.0
F32, BF16 = jnp.float32, jnp.bfloat16
NEG = -1e30
BLK = 256
HALF = BLK // 2
PAST_MAX = 1024
NB = 4
CH = 4
CW = 256
MESH = pl.DeviceIdType.MESH

UNITS = ((0, 0, 256), (1, 0, 256), (2, 0, 256), (3, 0, 128), (3, 2, 64), (3, 3, 64))
NU = len(UNITS)
Q, R, C, X, D, T, O = 0, 4, 8, 12, 16, 20, 24
E, Y, F, G = 32, 32 + NU, 32 + 2 * NU, 32 + 3 * NU
A = G + CH * NU
KV = A + CH * NU
N_REMOTE = KV + NB


def rope(t, cos_t, sin_t):
    width = t.shape[1]
    lane = lax.broadcasted_iota(jnp.int32, t.shape, 1)
    swapped = jnp.where((lane & 63) < 32, pltpu.roll(t, width - 32, 1), pltpu.roll(t, 32, 1))
    cos_w = jnp.concatenate([cos_t] * (width // 128), axis=1)
    sin_w = jnp.concatenate([sin_t] * (width // 128), axis=1)
    return (t * cos_w + swapped * sin_w).astype(BF16)


EPS = 1e-5


def square_sums(t):
    col = jnp.sum(t * t, axis=1, keepdims=True)
    return col, jnp.transpose(jnp.broadcast_to(col, (t.shape[0], 128)))[:8]


def as_column(row):
    return jnp.transpose(jnp.broadcast_to(row[:1], (128, row.shape[1])))[:, :1]


def half_factors(mine, theirs, d_model):
    r = lax.rsqrt((mine + theirs) / d_model + EPS)
    a = mine / (d_model // 2) + EPS
    b = theirs / (d_model // 2) + EPS
    return as_column(r * a * lax.rsqrt(a)), as_column(r * b * lax.rsqrt(b))


def kernel(d_model, p_hbm, x_hbm, g1_hbm, g2_hbm, wq_hbm, wk_hbm, wv_hbm, wo_hbm, wg_hbm, wu_hbm, wd_hbm, kc_hbm, vc_hbm,
           out, kc, vc,
           p_ref, g1_ref, g2_ref, x, wq, wk, wv, wo, wg, wu, wd, qsend, qkeep, qrecv, sq1, sq1r, cos_b, sin_b, kt, vv, qs, kvn, kvsend, kvrecv, picks, ob, orecv,
           csend, ckeep, crecv, part, xrecv, mid, sq2, sq2r, hg, sums, gsend, gkeep, grecv, ab, arecv, acc,
           esend, ekeep, erecv, part2, yrecv, lsem, ssem, rsem):
    h = lax.axis_index('hid')
    t = lax.axis_index('tp')
    c = lax.rem(t, 2)
    hid_dev = {'hid': 1 - h}
    core_dev = {'tp': t + 1 - 2 * c}
    x_dev = {'tp': lax.rem(t + 2, 4)}
    own = h == 0

    loads = []

    def load(src, dst):
        n = len(loads)
        cp = pltpu.make_async_copy(src, dst, lsem.at[n])
        cp.start()
        loads.append(cp)
        return cp

    ld_x = [load(x_hbm.at[pl.ds(0, BLK)], x.at[pl.ds(0, BLK)])]
    ld_q = [load(g1_hbm, g1_ref), load(wq_hbm, wq), load(wk_hbm, wk), load(wv_hbm, wv)]
    ld_x += [load(x_hbm.at[pl.ds(BLK, BLK)], x.at[pl.ds(BLK, BLK)])]
    ld_small = [load(p_hbm, p_ref), load(g2_hbm, g2_ref)]

    barrier = pltpu.get_barrier_semaphore()
    for dev in (hid_dev, core_dev, x_dev):
        pl.semaphore_signal(barrier, inc=1, device_id=dev, device_id_type=MESH)

    def remote(src, dst, n, dev):
        return pltpu.make_async_remote_copy(src_ref=src, dst_ref=dst, send_sem=ssem.at[n], recv_sem=rsem.at[n],
                                            device_id=dev, device_id_type=MESH)

    def q_copy(i): return remote(qsend.at[i], qrecv.at[i], Q + i, hid_dev)
    def r_copy(i): return remote(sq1.at[i], sq1r.at[i], R + i, hid_dev)
    def o_copy(i, n): return remote(ob.at[i, n], orecv.at[i, n], O + 2 * i + n, hid_dev)
    def kv_copy(i): return remote(kvsend.at[i], kvrecv.at[i], KV + i, hid_dev)
    def c_copy(i): return remote(csend.at[i], crecv.at[i], C + i, core_dev)
    def x_copy(i): return remote(part.at[i], xrecv.at[i], X + i, x_dev)
    def d_copy(i): return remote(mid.at[i, 0], mid.at[i, 1], D + i, core_dev)
    def t_copy(i): return remote(sq2.at[i], sq2r.at[i], T + i, hid_dev)

    def whole(u):
        return pl.ds(UNITS[u][1] * UNITS[u][2], UNITS[u][2])

    def half(u):
        return pl.ds(UNITS[u][1] * UNITS[u][2] // 2, UNITS[u][2] // 2)

    def own_rows(u):
        i, part_no, n = UNITS[u]
        return pl.ds(pl.multiple_of(i * BLK + c * HALF + part_no * (n // 2), 32), n // 2)

    def g_copy(u, j): return remote(gsend.at[UNITS[u][0], j, whole(u)], grecv.at[UNITS[u][0], j, whole(u)], G + CH * u + j, hid_dev)
    def a_copy(u, j): return remote(ab.at[UNITS[u][0], j, whole(u)], arecv.at[UNITS[u][0], j, whole(u)], A + CH * u + j, hid_dev)
    def e_copy(u): return remote(esend.at[UNITS[u][0], half(u)], erecv.at[UNITS[u][0], half(u)], E + u, core_dev)
    def y_copy(u): return remote(part2.at[UNITS[u][0], half(u)], yrecv.at[UNITS[u][0], half(u)], Y + u, x_dev)
    def f_copy(u):
        rows = own_rows(u)
        return remote(out.at[rows], out.at[rows], F + u, core_dev)

    def qkv(i, send):
        xf = x[pl.ds(i * BLK, BLK), :].astype(F32)
        sq, sq_row = square_sums(xf)
        xg = (xf * lax.rsqrt(sq / (d_model // 2) + EPS) * g1_ref[...]).astype(BF16)
        theirs = wq[:, pl.ds(pl.multiple_of((1 - h) * 256, 256), 256)]
        qsend[i, :, :256] = jnp.dot(xg, theirs, preferred_element_type=F32).astype(BF16)
        k = jnp.dot(xg, wk[...], preferred_element_type=F32).astype(BF16)
        v = jnp.dot(xg, wv[...], preferred_element_type=F32).astype(BF16)
        low = jnp.concatenate([k[:, :64], v[:, :64]], axis=1)
        high = jnp.concatenate([k[:, 64:], v[:, 64:]], axis=1)
        qsend[i, :, 256:] = jnp.where(own, high, low)
        if i == 0:
            pl.semaphore_wait(barrier, 3)
        if send:
            q_copy(i).start()
        kvsend[i] = jnp.where(own, low, high)
        mine = wq[:, pl.ds(pl.multiple_of(h * 256, 256), 256)]
        qkeep[i] = jnp.dot(xg, mine, preferred_element_type=F32).astype(BF16)
        sq1[i] = sq_row
        if send:
            r_copy(i).start()

    def tables(i):
        pos = (p_ref[0] + i * BLK + lax.broadcasted_iota(jnp.int32, (BLK, 128), 0)).astype(F32)
        lane = lax.broadcasted_iota(jnp.int32, (BLK, 128), 1)
        freq = jnp.exp((lane[:8] & 31).astype(F32) * (-2.0 * math.log(ROPE_BASE) / 64))[:1]
        ang = pos * freq
        cos_b[pl.ds(i * BLK, BLK), :] = jnp.cos(ang)
        sin = jnp.sin(ang)
        sin_b[pl.ds(i * BLK, BLK), :] = jnp.where((lane & 63) < 32, -sin, sin)

    def row_factors(i):
        return half_factors(sq1[i], sq1r[i], d_model)

    def keys_values(i, factors, mine, theirs):
        rows = slice(i * BLK, (i + 1) * BLK)
        mine, theirs = mine.astype(F32) * factors[0], theirs.astype(F32) * factors[1]
        kv = (jnp.where(own, mine, theirs) + jnp.where(own, theirs, mine)).astype(BF16)
        lane = lax.broadcasted_iota(jnp.int32, kv.shape, 1)
        return jnp.where(lane < 64, rope(kv.astype(F32), cos_b[rows, :], sin_b[rows, :]), kv)

    def att(i):
        rows = slice(i * BLK, (i + 1) * BLK)
        q_copy(i).wait_recv()
        r_copy(i).wait_recv()
        factors = row_factors(i)
        cos_t, sin_t = cos_b[rows, :], sin_b[rows, :]
        q = (qkeep[i].astype(F32) * factors[0] + qrecv[i, :, :256].astype(F32) * factors[1]).astype(BF16)
        kv = keys_values(i, factors, kvsend[i], qrecv[i, :, 256:])
        qs[...] = (rope(q.astype(F32), cos_t, sin_t).astype(F32) * 0.125).astype(BF16)
        kv_t = jnp.transpose(kv.astype(F32)).astype(BF16)
        kvn[i] = kv_t
        main = PAST_MAX + i * BLK
        kt[:, main:main + BLK] = kv_t[:64]
        vv[main:main + BLK, :] = kv[:, 64:]
        col = lax.broadcasted_iota(jnp.int32, (1, main), 1)
        bias = jnp.where((col >= p_ref[0]) & (col < PAST_MAX), NEG, 0.0)
        causal = lax.broadcasted_iota(jnp.int32, (BLK, BLK), 1) <= lax.broadcasted_iota(jnp.int32, (BLK, BLK), 0)

        def pair(n, carry):
            lanes = pl.ds(pl.multiple_of(n * 128, 128), 128)
            qp = qs[:, lanes]
            done = []
            for s in range(2):
                qn = qp[:, s * 64:(s + 1) * 64]
                s_main = jnp.dot(qn, kt[:, :main], preferred_element_type=F32) + bias
                s_diag = jnp.where(causal, jnp.dot(qn, kt[:, main:main + BLK], preferred_element_type=F32), NEG)
                top = jnp.maximum(jnp.max(s_main, axis=1, keepdims=True), jnp.max(s_diag, axis=1, keepdims=True))
                e_main = jnp.exp(s_main - top)
                e_diag = jnp.exp(s_diag - top)
                inv = 1.0 / (jnp.sum(e_main, axis=1, keepdims=True) + jnp.sum(e_diag, axis=1, keepdims=True))
                o = jnp.dot((e_main * inv).astype(BF16), vv[:main, :], preferred_element_type=F32)
                o += jnp.dot((e_diag * inv).astype(BF16), vv[main:main + BLK, :], preferred_element_type=F32)
                done.append(o.astype(BF16))
            ob[i, n] = jnp.concatenate(done, axis=1)
            o_copy(i, n).start()
            return carry
        lax.fori_loop(0, 2, pair, 0)

    def wo_step(i):
        o_copy(i, 0).wait_recv()
        o_copy(i, 1).wait_recv()
        mine = jnp.concatenate([ob[i, 0], ob[i, 1]], axis=1)
        theirs = jnp.concatenate([orecv[i, 0], orecv[i, 1]], axis=1)
        acc[...] = jnp.dot(mine, wo[pl.ds(pl.multiple_of(h * 256, 256), 256), :], preferred_element_type=F32)
        acc[...] += jnp.dot(theirs, wo[pl.ds(pl.multiple_of((1 - h) * 256, 256), 256), :], preferred_element_type=F32)
        ckeep[i] = acc[pl.ds(pl.multiple_of(c * HALF, HALF), HALF), :].astype(BF16)
        csend[i] = acc[pl.ds(pl.multiple_of((1 - c) * HALF, HALF), HALF), :].astype(BF16)
        c_copy(i).start()

    def add(a, b):
        return (a.astype(F32) + b.astype(F32)).astype(BF16)

    def c_step(i):
        c_copy(i).wait_recv()
        part[i] = add(ckeep[i], crecv[i])
        x_copy(i).start()

    def x_step(i):
        x_copy(i).wait_recv()
        res = x[pl.ds(pl.multiple_of(i * BLK + c * HALF, HALF), HALF), :]
        mid[i, 0] = add(res, add(part[i], xrecv[i]))
        d_copy(i).start()

    def d_step(i):
        d_copy(i).wait_recv()
        at = 0
        for u in range(NU):
            if UNITS[u][0] != i:
                continue
            for k in range(2):
                n = UNITS[u][2] // 2
                m = mid[i, k, half(u), :].astype(F32)
                sq = jnp.sum(m * m, axis=1, keepdims=True)
                sums[at:at + n, :] = jnp.broadcast_to(sq, (n, 128))
                hg[at:at + n, :] = (m * lax.rsqrt(sq / (d_model // 2) + EPS) * g2_ref[...]).astype(BF16)
                at += n
        sq2[i] = jnp.transpose(sums[...])[:8]

    def gate_up(u, side, j, dst):
        cols = pl.ds(pl.multiple_of(side * (CH * CW) + j * CW, CW), CW)
        rows = hg[whole(u), :]
        dst[:, :CW] = jnp.dot(rows, wg[:, cols], preferred_element_type=F32).astype(BF16)
        dst[:, CW:] = jnp.dot(rows, wu[:, cols], preferred_element_type=F32).astype(BF16)

    def u_step(u, j):
        i = UNITS[u][0]
        gate_up(u, 1 - h, j, gsend.at[i, j, whole(u)])
        g_copy(u, j).start()
        gate_up(u, h, j, gkeep.at[i % 2, j, whole(u)])

    def v_step(u, j):
        i = UNITS[u][0]
        g_copy(u, j).wait_recv()
        rows = slice(UNITS[u][1] * UNITS[u][2], (UNITS[u][1] + 1) * UNITS[u][2])
        mine, theirs = (f[rows] for f in half_factors(sq2[i], sq2r[i], d_model))
        both = gkeep[i % 2, j, whole(u), :].astype(F32) * mine + grecv[i, j, whole(u), :].astype(F32) * theirs
        both = both.astype(BF16).astype(F32)
        g, e = both[:, :CW], both[:, CW:]
        ab[i, j, whole(u), :] = (g * jax.nn.sigmoid(g) * e).astype(BF16)
        a_copy(u, j).start()

    def w_step(u, j):
        i = UNITS[u][0]
        a_copy(u, j).wait_recv()
        mine = wd[pl.ds(pl.multiple_of(h * (CH * CW) + j * CW, CW), CW), :]
        theirs = wd[pl.ds(pl.multiple_of((1 - h) * (CH * CW) + j * CW, CW), CW), :]
        y = jnp.dot(ab[i, j, whole(u), :], mine, preferred_element_type=F32)
        y += jnp.dot(arecv[i, j, whole(u), :], theirs, preferred_element_type=F32)
        acc[whole(u), :] = jnp.where(j == 0, 0.0, acc[whole(u), :]) + y

    def e_start(u):
        i, k, n = UNITS[u]
        ekeep[i, half(u), :] = acc[k * n:k * n + n // 2, :].astype(BF16)
        esend[i, half(u), :] = acc[k * n + n // 2:k * n + n, :].astype(BF16)
        e_copy(u).start()

    def e_step(u):
        i = UNITS[u][0]
        e_copy(u).wait_recv()
        part2[i, half(u), :] = add(ekeep[i, half(u), :], erecv[i, half(u), :])
        y_copy(u).start()

    def y_step(u):
        i = UNITS[u][0]
        y_copy(u).wait_recv()
        down = add(part2[i, half(u), :], yrecv[i, half(u), :])
        out[own_rows(u), :] = add(mid[i, 0, half(u), :], down)
        f_copy(u).start()

    def f_step(u):
        f_copy(u).wait_recv()

    def loop(*steps):
        def body(j, carry):
            for step, i in steps:
                step(i, j)
            return carry
        lax.fori_loop(0, CH, body, 0)

    span = PAST_MAX

    def make_picks():
        at = BLK - p_ref[0] + lax.broadcasted_iota(jnp.int32, (BLK, span), 1)
        picks[...] = jnp.where(at == lax.broadcasted_iota(jnp.int32, (BLK, span), 0), 1.0, 0.0).astype(BF16)

    def place(i, head, kv_t):
        lanes = pl.ds(pl.multiple_of(head * 64, 64), 64)
        cols = slice((i + 1) * BLK, (i + 1) * BLK + span)
        where = BLK - p_ref[0] + lax.broadcasted_iota(jnp.int32, (1, span), 1)
        fresh = (where >= 0) & (where < BLK)
        new = jnp.dot(kv_t, picks[...], preferred_element_type=F32)
        kc[lanes, cols] = jnp.where(fresh, new[:64], kc[lanes, cols].astype(F32)).astype(BF16)
        vc[lanes, cols] = jnp.where(fresh, new[64:], vc[lanes, cols].astype(F32)).astype(BF16)

    def kv_step(i):
        factors = row_factors(i)
        kv_copy(i).wait_recv()
        kv = keys_values(i, factors, qsend[i, :, 256:], kvrecv[i])
        place(i, 1 - h, jnp.transpose(kv.astype(F32)).astype(BF16))

    for cp in ld_q:
        cp.wait()
    ld_x[0].wait()
    qkv(0, True)
    ld_x += [load(x_hbm.at[pl.ds(i * BLK, BLK)], x.at[pl.ds(i * BLK, BLK)]) for i in range(2, NB)]
    ld_kc, ld_vc = load(kc_hbm, kc), load(vc_hbm, vc)
    ld_wo = load(wo_hbm, wo)
    ld_gu = [load(wg_hbm, wg), load(wu_hbm, wu)]
    ld_wd = load(wd_hbm, wd)
    for i in range(1, NB):
        ld_x[i].wait()
        qkv(i, i < 2)
    for cp in ld_small:
        cp.wait()
    for i in range(NB):
        tables(i)
    ld_kc.wait()
    ld_vc.wait()
    kt[:, :PAST_MAX] = kc[pl.ds(pl.multiple_of(h * 64, 64), 64), :PAST_MAX]
    v_old = jnp.transpose(vc[:, :PAST_MAX].astype(F32)).astype(BF16)
    vv[:PAST_MAX, :] = jnp.where(own, v_old[:, :64], v_old[:, 64:])
    att(0)
    q_copy(2).start()
    r_copy(2).start()
    att(1)
    q_copy(3).start()
    r_copy(3).start()
    ld_wo.wait()
    wo_step(0)
    c_step(0)
    att(2)
    x_step(0)
    wo_step(1)
    d_step(0)
    for cp in ld_gu:
        cp.wait()
    t_copy(0).start()
    loop((u_step, 0))
    c_step(1)
    att(3)
    x_step(1)
    wo_step(2)
    d_step(1)
    t_copy(1).start()
    t_copy(0).wait_recv()
    c_step(2)
    loop((u_step, 1), (v_step, 0))
    x_step(2)
    wo_step(3)
    c_step(3)
    d_step(2)
    t_copy(2).start()
    t_copy(1).wait_recv()
    ld_wd.wait()
    loop((u_step, 2), (v_step, 1), (w_step, 0))
    e_start(0)
    x_step(3)
    d_step(3)
    t_copy(3).start()
    e_step(0)
    t_copy(2).wait_recv()
    make_picks()
    for i in range(NB):
        place(i, h, kvn[i])
    loop((u_step, 3), (v_step, 2), (w_step, 1))
    loop((u_step, 4))
    loop((u_step, 5))
    e_start(1)
    y_step(0)
    e_step(1)
    f_step(0)
    t_copy(3).wait_recv()
    loop((v_step, 3), (w_step, 2))
    e_start(2)
    y_step(1)
    e_step(2)
    f_step(1)
    loop((v_step, 4))
    loop((v_step, 5))
    for i in range(NB):
        kv_copy(i).start()
    y_step(2)
    loop((w_step, 3))
    e_start(3)
    f_step(2)
    w_step(4, 0)
    e_step(3)
    for j in range(1, CH):
        w_step(4, j)
    e_start(4)
    w_step(5, 0)
    e_step(4)
    for j in range(1, CH):
        w_step(5, j)
    e_start(5)
    y_step(3)
    e_step(5)
    kv_step(0)
    y_step(4)
    f_step(3)
    kv_step(1)
    kv_step(2)
    y_step(5)
    f_step(4)
    for i in range(NB):
        for cp in (q_copy, r_copy, c_copy, x_copy, d_copy, t_copy):
            cp(i).wait_send()
        for n in range(2):
            o_copy(i, n).wait_send()
    for u in range(NU):
        def drain(j, carry, u=u):
            g_copy(u, j).wait_send()
            a_copy(u, j).wait_send()
            return carry
        lax.fori_loop(0, CH, drain, 0)
        for cp in (e_copy, y_copy, f_copy):
            cp(u).wait_send()
    f_step(5)
    kv_step(3)
    for i in range(NB):
        kv_copy(i).wait_send()


def results_body(out, kc, vc, out_hbm, ko_hbm, vo_hbm, sem):
    copies = [pltpu.make_async_copy(out.at[pl.ds(i * BLK, BLK)], out_hbm.at[pl.ds(i * BLK, BLK)], sem.at[i]) for i in range(NB)]
    copies += [pltpu.make_async_copy(kc, ko_hbm, sem.at[NB]), pltpu.make_async_copy(vc, vo_hbm, sem.at[NB + 1])]
    for cp in copies:
        cp.start()
    for cp in copies:
        cp.wait()


def solution(mesh):
    def local_layer(hidden, rms_attn, rms_mlp, w_q, w_k, w_v, w_o, w_gate, w_up, w_down, k_cache, v_cache, past_len):
        new_len, width = hidden.shape
        tokens = k_cache.shape[0]
        k_flat = k_cache.transpose(1, 2, 0).reshape(-1, tokens)
        v_flat = v_cache.transpose(1, 2, 0).reshape(-1, tokens)
        any_spec = pl.BlockSpec(memory_space=pl.ANY)

        def v(*shape, dtype=BF16):
            return pltpu.VMEM(shape, dtype)
        tok = v(NB, HALF, width)
        scratch = [
            pltpu.SMEM((1,), jnp.int32), v(1, width, dtype=F32), v(1, width, dtype=F32),
            v(new_len, width), v(*w_q.shape), v(*w_k.shape), v(*w_v.shape), v(*w_o.shape), v(*w_gate.shape), v(*w_up.shape), v(*w_down.shape),
            v(NB, BLK, 384), v(NB, BLK, 256), v(NB, BLK, 384), v(NB, 8, BLK, dtype=F32), v(NB, 8, BLK, dtype=F32),
            v(new_len, 128, dtype=F32), v(new_len, 128, dtype=F32), v(64, PAST_MAX + new_len), v(PAST_MAX + new_len, 64),
            v(BLK, 256), v(NB, 128, BLK), v(NB, BLK, 128), v(NB, BLK, 128), v(BLK, PAST_MAX), v(NB, 2, BLK, 128), v(NB, 2, BLK, 128),
            tok, tok, tok, tok, tok, v(NB, 2, HALF, width), v(NB, 8, BLK, dtype=F32), v(NB, 8, BLK, dtype=F32), v(BLK, width), v(BLK, 128, dtype=F32),
            v(NB, CH, BLK, 2 * CW), v(2, CH, BLK, 2 * CW), v(NB, CH, BLK, 2 * CW), v(NB, CH, BLK, CW), v(NB, CH, BLK, CW),
            v(BLK, width, dtype=F32),
            tok, tok, tok, tok, tok,
            pltpu.SemaphoreType.DMA((16,)),
            pltpu.SemaphoreType.DMA((N_REMOTE,)), pltpu.SemaphoreType.DMA((N_REMOTE,)),
        ]
        vmem_spec = pl.BlockSpec(memory_space=pltpu.VMEM)
        done = pl.pallas_call(
            lambda *refs: kernel(2 * width, *refs),
            out_shape=tuple(v(*a) for a in (hidden.shape, k_flat.shape, v_flat.shape)),
            in_specs=[any_spec] * 13,
            out_specs=(vmem_spec,) * 3,
            scratch_shapes=scratch,
            compiler_params=pltpu.CompilerParams(collective_id=0, has_side_effects=True, vmem_limit_bytes=60 << 20),
            name="layer",
        )(past_len, hidden, rms_attn.reshape(1, width), rms_mlp.reshape(1, width), w_q, w_k, w_v, w_o, w_gate, w_up, w_down,
          k_flat, v_flat)
        out, k_full, v_full = pl.pallas_call(
            results_body,
            out_shape=tuple(jax.ShapeDtypeStruct(a, BF16) for a in (hidden.shape, k_flat.shape, v_flat.shape)),
            in_specs=[vmem_spec] * 3, out_specs=(any_spec,) * 3,
            scratch_shapes=[pltpu.SemaphoreType.DMA((NB + 2,))],
            compiler_params=pltpu.CompilerParams(vmem_limit_bytes=1 << 20),
            name="results",
        )(*done)
        heads, dim = k_cache.shape[1:]
        return (out, k_full.reshape(heads, dim, tokens).transpose(2, 0, 1), v_full.reshape(heads, dim, tokens).transpose(2, 0, 1))

    row_split = P('hid', 'tp')
    col_split = P('tp', 'hid')
    cache_spec = P('dp', 'tp', None)
    in_specs = (P('dp', 'hid'), P('hid'), P('hid'), row_split, row_split, row_split, col_split,
                row_split, row_split, col_split, cache_spec, cache_spec, P('dp'))
    out_specs = (P('dp', 'hid'), cache_spec, cache_spec)
    return jax.shard_map(local_layer, mesh=mesh, in_specs=in_specs, out_specs=out_specs, check_vma=False)
```

```python
import math
import jax
import jax.numpy as jnp
from jax import lax
from jax.experimental import pallas as pl
from jax.experimental.pallas import tpu as pltpu
from jax.sharding import PartitionSpec as P

ROPE_BASE = 10000.0
F32, BF16 = jnp.float32, jnp.bfloat16
NEG = -1e30
BLK = 256
HALF = BLK // 2
PAST_MAX = 1024
NB = 4
CH = 4
CW = 256
MESH = pl.DeviceIdType.MESH

UNITS = ((0, 0, 256), (1, 0, 256), (2, 0, 256), (3, 0, 128), (3, 2, 64), (3, 3, 64))
NU = len(UNITS)
Q, R, C, X, D, T, O = 0, 4, 8, 12, 16, 20, 24
E, Y, F, G = 32, 32 + NU, 32 + 2 * NU, 32 + 3 * NU
A = G + CH * NU
KV = A + CH * NU
N_REMOTE = KV + NB


def rope(t, cos_t, sin_t):
    width = t.shape[1]
    lane = lax.broadcasted_iota(jnp.int32, t.shape, 1)
    swapped = jnp.where((lane & 63) < 32, pltpu.roll(t, width - 32, 1), pltpu.roll(t, 32, 1))
    cos_w = jnp.concatenate([cos_t] * (width // 128), axis=1)
    sin_w = jnp.concatenate([sin_t] * (width // 128), axis=1)
    return (t * cos_w + swapped * sin_w).astype(BF16)


EPS = 1e-5


def square_sums(t):
    col = jnp.sum(t * t, axis=1, keepdims=True)
    return col, jnp.transpose(jnp.broadcast_to(col, (t.shape[0], 128)))[:8]


def as_column(row):
    return jnp.transpose(jnp.broadcast_to(row[:1], (128, row.shape[1])))[:, :1]


def half_factors(mine, theirs, d_model):
    r = lax.rsqrt((mine + theirs) / d_model + EPS)
    a = mine / (d_model // 2) + EPS
    b = theirs / (d_model // 2) + EPS
    return as_column(r * a * lax.rsqrt(a)), as_column(r * b * lax.rsqrt(b))


def kernel(d_model, p_hbm, x_hbm, g1_hbm, g2_hbm, wq_hbm, wk_hbm, wv_hbm, wo_hbm, wg_hbm, wu_hbm, wd_hbm, kc_hbm, vc_hbm,
           out, kc, vc,
           p_ref, g1_ref, g2_ref, x, wq, wk, wv, wo, wg, wu, wd, qsend, qkeep, qrecv, sq1, sq1r, cos_b, sin_b, kt, vv, qs, kvn, kvsend, kvrecv, picks, ob, orecv,
           csend, ckeep, crecv, part, xrecv, mid, sq2, sq2r, hg, sums, gsend, gkeep, grecv, ab, arecv, acc,
           esend, ekeep, erecv, part2, yrecv, lsem, ssem, rsem):
    h = lax.axis_index('hid')
    t = lax.axis_index('tp')
    c = lax.rem(t, 2)
    hid_dev = {'hid': 1 - h}
    core_dev = {'tp': t + 1 - 2 * c}
    x_dev = {'tp': lax.rem(t + 2, 4)}
    own = h == 0

    loads = []

    def load(src, dst):
        n = len(loads)
        cp = pltpu.make_async_copy(src, dst, lsem.at[n])
        cp.start()
        loads.append(cp)
        return cp

    ld_x = [load(x_hbm.at[pl.ds(0, BLK)], x.at[pl.ds(0, BLK)])]
    ld_q = [load(g1_hbm, g1_ref), load(wq_hbm, wq), load(wk_hbm, wk), load(wv_hbm, wv)]
    ld_x += [load(x_hbm.at[pl.ds(BLK, BLK)], x.at[pl.ds(BLK, BLK)])]
    ld_small = [load(p_hbm, p_ref), load(g2_hbm, g2_ref)]

    barrier = pltpu.get_barrier_semaphore()
    for dev in (hid_dev, core_dev, x_dev):
        pl.semaphore_signal(barrier, inc=1, device_id=dev, device_id_type=MESH)

    def remote(src, dst, n, dev):
        return pltpu.make_async_remote_copy(src_ref=src, dst_ref=dst, send_sem=ssem.at[n], recv_sem=rsem.at[n],
                                            device_id=dev, device_id_type=MESH)

    def q_copy(i): return remote(qsend.at[i], qrecv.at[i], Q + i, hid_dev)
    def r_copy(i): return remote(sq1.at[i], sq1r.at[i], R + i, hid_dev)
    def o_copy(i, n): return remote(ob.at[i, n], orecv.at[i, n], O + 2 * i + n, hid_dev)
    def kv_copy(i): return remote(kvsend.at[i], kvrecv.at[i], KV + i, hid_dev)
    def c_copy(i): return remote(csend.at[i], crecv.at[i], C + i, core_dev)
    def x_copy(i): return remote(part.at[i], xrecv.at[i], X + i, x_dev)
    def d_copy(i): return remote(mid.at[i, 0], mid.at[i, 1], D + i, core_dev)
    def t_copy(i): return remote(sq2.at[i], sq2r.at[i], T + i, hid_dev)

    def whole(u):
        return pl.ds(UNITS[u][1] * UNITS[u][2], UNITS[u][2])

    def half(u):
        return pl.ds(UNITS[u][1] * UNITS[u][2] // 2, UNITS[u][2] // 2)

    def own_rows(u):
        i, part_no, n = UNITS[u]
        return pl.ds(pl.multiple_of(i * BLK + c * HALF + part_no * (n // 2), 32), n // 2)

    def g_copy(u, j): return remote(gsend.at[UNITS[u][0], j, whole(u)], grecv.at[UNITS[u][0], j, whole(u)], G + CH * u + j, hid_dev)
    def a_copy(u, j): return remote(ab.at[UNITS[u][0], j, whole(u)], arecv.at[UNITS[u][0], j, whole(u)], A + CH * u + j, hid_dev)
    def e_copy(u): return remote(esend.at[UNITS[u][0], half(u)], erecv.at[UNITS[u][0], half(u)], E + u, core_dev)
    def y_copy(u): return remote(part2.at[UNITS[u][0], half(u)], yrecv.at[UNITS[u][0], half(u)], Y + u, x_dev)
    def f_copy(u):
        rows = own_rows(u)
        return remote(out.at[rows], out.at[rows], F + u, core_dev)

    def qkv(i, send):
        xf = x[pl.ds(i * BLK, BLK), :].astype(F32)
        sq, sq_row = square_sums(xf)
        xg = (xf * lax.rsqrt(sq / (d_model // 2) + EPS) * g1_ref[...]).astype(BF16)
        theirs = wq[:, pl.ds(pl.multiple_of((1 - h) * 256, 256), 256)]
        qsend[i, :, :256] = jnp.dot(xg, theirs, preferred_element_type=F32).astype(BF16)
        k = jnp.dot(xg, wk[...], preferred_element_type=F32).astype(BF16)
        v = jnp.dot(xg, wv[...], preferred_element_type=F32).astype(BF16)
        low = jnp.concatenate([k[:, :64], v[:, :64]], axis=1)
        high = jnp.concatenate([k[:, 64:], v[:, 64:]], axis=1)
        qsend[i, :, 256:] = jnp.where(own, high, low)
        if i == 0:
            pl.semaphore_wait(barrier, 3)
        if send:
            q_copy(i).start()
        kvsend[i] = jnp.where(own, low, high)
        mine = wq[:, pl.ds(pl.multiple_of(h * 256, 256), 256)]
        qkeep[i] = jnp.dot(xg, mine, preferred_element_type=F32).astype(BF16)
        sq1[i] = sq_row
        if send:
            r_copy(i).start()

    def tables(i):
        pos = (p_ref[0] + i * BLK + lax.broadcasted_iota(jnp.int32, (BLK, 128), 0)).astype(F32)
        lane = lax.broadcasted_iota(jnp.int32, (BLK, 128), 1)
        freq = jnp.exp((lane[:8] & 31).astype(F32) * (-2.0 * math.log(ROPE_BASE) / 64))[:1]
        ang = pos * freq
        cos_b[pl.ds(i * BLK, BLK), :] = jnp.cos(ang)
        sin = jnp.sin(ang)
        sin_b[pl.ds(i * BLK, BLK), :] = jnp.where((lane & 63) < 32, -sin, sin)

    def row_factors(i):
        return half_factors(sq1[i], sq1r[i], d_model)

    def keys_values(i, factors, mine, theirs):
        rows = slice(i * BLK, (i + 1) * BLK)
        mine, theirs = mine.astype(F32) * factors[0], theirs.astype(F32) * factors[1]
        kv = (jnp.where(own, mine, theirs) + jnp.where(own, theirs, mine)).astype(BF16)
        lane = lax.broadcasted_iota(jnp.int32, kv.shape, 1)
        return jnp.where(lane < 64, rope(kv.astype(F32), cos_b[rows, :], sin_b[rows, :]), kv)

    def att(i):
        rows = slice(i * BLK, (i + 1) * BLK)
        q_copy(i).wait_recv()
        r_copy(i).wait_recv()
        factors = row_factors(i)
        cos_t, sin_t = cos_b[rows, :], sin_b[rows, :]
        q = (qkeep[i].astype(F32) * factors[0] + qrecv[i, :, :256].astype(F32) * factors[1]).astype(BF16)
        kv = keys_values(i, factors, kvsend[i], qrecv[i, :, 256:])
        qs[...] = (rope(q.astype(F32), cos_t, sin_t).astype(F32) * 0.125).astype(BF16)
        kv_t = jnp.transpose(kv.astype(F32)).astype(BF16)
        kvn[i] = kv_t
        main = PAST_MAX + i * BLK
        kt[:, main:main + BLK] = kv_t[:64]
        vv[main:main + BLK, :] = kv[:, 64:]
        col = lax.broadcasted_iota(jnp.int32, (1, main), 1)
        bias = jnp.where((col >= p_ref[0]) & (col < PAST_MAX), NEG, 0.0)
        causal = lax.broadcasted_iota(jnp.int32, (BLK, BLK), 1) <= lax.broadcasted_iota(jnp.int32, (BLK, BLK), 0)

        def pair(n, carry):
            lanes = pl.ds(pl.multiple_of(n * 128, 128), 128)
            qp = qs[:, lanes]
            done = []
            for s in range(2):
                qn = qp[:, s * 64:(s + 1) * 64]
                s_main = jnp.dot(qn, kt[:, :main], preferred_element_type=F32) + bias
                s_diag = jnp.where(causal, jnp.dot(qn, kt[:, main:main + BLK], preferred_element_type=F32), NEG)
                top = jnp.maximum(jnp.max(s_main, axis=1, keepdims=True), jnp.max(s_diag, axis=1, keepdims=True))
                e_main = jnp.exp(s_main - top)
                e_diag = jnp.exp(s_diag - top)
                inv = 1.0 / (jnp.sum(e_main, axis=1, keepdims=True) + jnp.sum(e_diag, axis=1, keepdims=True))
                o = jnp.dot((e_main * inv).astype(BF16), vv[:main, :], preferred_element_type=F32)
                o += jnp.dot((e_diag * inv).astype(BF16), vv[main:main + BLK, :], preferred_element_type=F32)
                done.append(o.astype(BF16))
            ob[i, n] = jnp.concatenate(done, axis=1)
            o_copy(i, n).start()
            return carry
        lax.fori_loop(0, 2, pair, 0)

    def wo_step(i):
        o_copy(i, 0).wait_recv()
        o_copy(i, 1).wait_recv()
        mine = jnp.concatenate([ob[i, 0], ob[i, 1]], axis=1)
        theirs = jnp.concatenate([orecv[i, 0], orecv[i, 1]], axis=1)
        acc[...] = jnp.dot(mine, wo[pl.ds(pl.multiple_of(h * 256, 256), 256), :], preferred_element_type=F32)
        acc[...] += jnp.dot(theirs, wo[pl.ds(pl.multiple_of((1 - h) * 256, 256), 256), :], preferred_element_type=F32)
        ckeep[i] = acc[pl.ds(pl.multiple_of(c * HALF, HALF), HALF), :].astype(BF16)
        csend[i] = acc[pl.ds(pl.multiple_of((1 - c) * HALF, HALF), HALF), :].astype(BF16)
        c_copy(i).start()

    def add(a, b):
        return (a.astype(F32) + b.astype(F32)).astype(BF16)

    def c_step(i):
        c_copy(i).wait_recv()
        part[i] = add(ckeep[i], crecv[i])
        x_copy(i).start()

    def x_step(i):
        x_copy(i).wait_recv()
        res = x[pl.ds(pl.multiple_of(i * BLK + c * HALF, HALF), HALF), :]
        mid[i, 0] = add(res, add(part[i], xrecv[i]))
        d_copy(i).start()

    def d_step(i):
        d_copy(i).wait_recv()
        at = 0
        for u in range(NU):
            if UNITS[u][0] != i:
                continue
            for k in range(2):
                n = UNITS[u][2] // 2
                m = mid[i, k, half(u), :].astype(F32)
                sq = jnp.sum(m * m, axis=1, keepdims=True)
                sums[at:at + n, :] = jnp.broadcast_to(sq, (n, 128))
                hg[at:at + n, :] = (m * lax.rsqrt(sq / (d_model // 2) + EPS) * g2_ref[...]).astype(BF16)
                at += n
        sq2[i] = jnp.transpose(sums[...])[:8]

    def gate_up(u, side, j, dst):
        cols = pl.ds(pl.multiple_of(side * (CH * CW) + j * CW, CW), CW)
        rows = hg[whole(u), :]
        dst[:, :CW] = jnp.dot(rows, wg[:, cols], preferred_element_type=F32).astype(BF16)
        dst[:, CW:] = jnp.dot(rows, wu[:, cols], preferred_element_type=F32).astype(BF16)

    def u_step(u, j):
        i = UNITS[u][0]
        gate_up(u, 1 - h, j, gsend.at[i, j, whole(u)])
        g_copy(u, j).start()
        gate_up(u, h, j, gkeep.at[i % 2, j, whole(u)])

    def v_step(u, j):
        i = UNITS[u][0]
        g_copy(u, j).wait_recv()
        rows = slice(UNITS[u][1] * UNITS[u][2], (UNITS[u][1] + 1) * UNITS[u][2])
        mine, theirs = (f[rows] for f in half_factors(sq2[i], sq2r[i], d_model))
        both = gkeep[i % 2, j, whole(u), :].astype(F32) * mine + grecv[i, j, whole(u), :].astype(F32) * theirs
        both = both.astype(BF16).astype(F32)
        g, e = both[:, :CW], both[:, CW:]
        ab[i, j, whole(u), :] = (g * jax.nn.sigmoid(g) * e).astype(BF16)
        a_copy(u, j).start()

    def w_step(u, j):
        i = UNITS[u][0]
        a_copy(u, j).wait_recv()
        mine = wd[pl.ds(pl.multiple_of(h * (CH * CW) + j * CW, CW), CW), :]
        theirs = wd[pl.ds(pl.multiple_of((1 - h) * (CH * CW) + j * CW, CW), CW), :]
        y = jnp.dot(ab[i, j, whole(u), :], mine, preferred_element_type=F32)
        y += jnp.dot(arecv[i, j, whole(u), :], theirs, preferred_element_type=F32)
        acc[whole(u), :] = jnp.where(j == 0, 0.0, acc[whole(u), :]) + y

    def e_start(u):
        i, k, n = UNITS[u]
        ekeep[i, half(u), :] = acc[k * n:k * n + n // 2, :].astype(BF16)
        esend[i, half(u), :] = acc[k * n + n // 2:k * n + n, :].astype(BF16)
        e_copy(u).start()

    def e_step(u):
        i = UNITS[u][0]
        e_copy(u).wait_recv()
        part2[i, half(u), :] = add(ekeep[i, half(u), :], erecv[i, half(u), :])
        y_copy(u).start()

    def y_step(u):
        i = UNITS[u][0]
        y_copy(u).wait_recv()
        down = add(part2[i, half(u), :], yrecv[i, half(u), :])
        out[own_rows(u), :] = add(mid[i, 0, half(u), :], down)
        f_copy(u).start()

    def f_step(u):
        f_copy(u).wait_recv()

    def loop(*steps):
        def body(j, carry):
            for step, i in steps:
                step(i, j)
            return carry
        lax.fori_loop(0, CH, body, 0)

    span = PAST_MAX

    def make_picks():
        at = BLK - p_ref[0] + lax.broadcasted_iota(jnp.int32, (BLK, span), 1)
        picks[...] = jnp.where(at == lax.broadcasted_iota(jnp.int32, (BLK, span), 0), 1.0, 0.0).astype(BF16)

    def place(i, head, kv_t):
        lanes = pl.ds(pl.multiple_of(head * 64, 64), 64)
        cols = slice((i + 1) * BLK, (i + 1) * BLK + span)
        where = BLK - p_ref[0] + lax.broadcasted_iota(jnp.int32, (1, span), 1)
        fresh = (where >= 0) & (where < BLK)
        new = jnp.dot(kv_t, picks[...], preferred_element_type=F32)
        kc[lanes, cols] = jnp.where(fresh, new[:64], kc[lanes, cols].astype(F32)).astype(BF16)
        vc[lanes, cols] = jnp.where(fresh, new[64:], vc[lanes, cols].astype(F32)).astype(BF16)

    def kv_step(i):
        factors = row_factors(i)
        kv_copy(i).wait_recv()
        kv = keys_values(i, factors, qsend[i, :, 256:], kvrecv[i])
        place(i, 1 - h, jnp.transpose(kv.astype(F32)).astype(BF16))

    for cp in ld_q:
        cp.wait()
    ld_x[0].wait()
    qkv(0, True)
    ld_x += [load(x_hbm.at[pl.ds(i * BLK, BLK)], x.at[pl.ds(i * BLK, BLK)]) for i in range(2, NB)]
    ld_kc, ld_vc = load(kc_hbm, kc), load(vc_hbm, vc)
    ld_wo = load(wo_hbm, wo)
    ld_gu = [load(wg_hbm, wg), load(wu_hbm, wu)]
    ld_wd = load(wd_hbm, wd)
    for i in range(1, NB):
        ld_x[i].wait()
        qkv(i, i < 2)
    for cp in ld_small:
        cp.wait()
    for i in range(NB):
        tables(i)
    ld_kc.wait()
    ld_vc.wait()
    kt[:, :PAST_MAX] = kc[pl.ds(pl.multiple_of(h * 64, 64), 64), :PAST_MAX]
    v_old = jnp.transpose(vc[:, :PAST_MAX].astype(F32)).astype(BF16)
    vv[:PAST_MAX, :] = jnp.where(own, v_old[:, :64], v_old[:, 64:])
    att(0)
    q_copy(2).start()
    r_copy(2).start()
    att(1)
    q_copy(3).start()
    r_copy(3).start()
    ld_wo.wait()
    wo_step(0)
    c_step(0)
    att(2)
    x_step(0)
    wo_step(1)
    d_step(0)
    for cp in ld_gu:
        cp.wait()
    t_copy(0).start()
    loop((u_step, 0))
    c_step(1)
    att(3)
    x_step(1)
    wo_step(2)
    d_step(1)
    t_copy(1).start()
    t_copy(0).wait_recv()
    c_step(2)
    loop((u_step, 1), (v_step, 0))
    x_step(2)
    wo_step(3)
    c_step(3)
    d_step(2)
    t_copy(2).start()
    t_copy(1).wait_recv()
    ld_wd.wait()
    loop((u_step, 2), (v_step, 1), (w_step, 0))
    e_start(0)
    x_step(3)
    d_step(3)
    t_copy(3).start()
    e_step(0)
    t_copy(2).wait_recv()
    make_picks()
    for i in range(NB):
        place(i, h, kvn[i])
    loop((u_step, 3), (v_step, 2), (w_step, 1))
    loop((u_step, 4))
    loop((u_step, 5))
    e_start(1)
    y_step(0)
    e_step(1)
    f_step(0)
    t_copy(3).wait_recv()
    loop((v_step, 3), (w_step, 2))
    e_start(2)
    y_step(1)
    e_step(2)
    f_step(1)
    loop((v_step, 4))
    loop((v_step, 5))
    for i in range(NB):
        kv_copy(i).start()
    y_step(2)
    loop((w_step, 3))
    e_start(3)
    f_step(2)
    w_step(4, 0)
    e_step(3)
    for j in range(1, CH):
        w_step(4, j)
    e_start(4)
    w_step(5, 0)
    e_step(4)
    for j in range(1, CH):
        w_step(5, j)
    e_start(5)
    e_step(5)
    y_step(3)
    y_step(4)
    kv_step(0)
    kv_step(1)
    y_step(5)
    f_step(3)
    f_step(4)
    kv_step(2)
    for i in range(NB):
        for cp in (q_copy, r_copy, c_copy, x_copy, d_copy, t_copy):
            cp(i).wait_send()
        for n in range(2):
            o_copy(i, n).wait_send()
    for u in range(NU):
        def drain(j, carry, u=u):
            g_copy(u, j).wait_send()
            a_copy(u, j).wait_send()
            return carry
        lax.fori_loop(0, CH, drain, 0)
        for cp in (e_copy, y_copy, f_copy):
            cp(u).wait_send()
    f_step(5)
    kv_step(3)
    for i in range(NB):
        kv_copy(i).wait_send()


def results_body(out, kc, vc, out_hbm, ko_hbm, vo_hbm, sem):
    copies = [pltpu.make_async_copy(out.at[pl.ds(i * BLK, BLK)], out_hbm.at[pl.ds(i * BLK, BLK)], sem.at[i]) for i in range(NB)]
    copies += [pltpu.make_async_copy(kc, ko_hbm, sem.at[NB]), pltpu.make_async_copy(vc, vo_hbm, sem.at[NB + 1])]
    for cp in copies:
        cp.start()
    for cp in copies:
        cp.wait()


def solution(mesh):
    def local_layer(hidden, rms_attn, rms_mlp, w_q, w_k, w_v, w_o, w_gate, w_up, w_down, k_cache, v_cache, past_len):
        new_len, width = hidden.shape
        tokens = k_cache.shape[0]
        k_flat = k_cache.transpose(1, 2, 0).reshape(-1, tokens)
        v_flat = v_cache.transpose(1, 2, 0).reshape(-1, tokens)
        any_spec = pl.BlockSpec(memory_space=pl.ANY)

        def v(*shape, dtype=BF16):
            return pltpu.VMEM(shape, dtype)
        tok = v(NB, HALF, width)
        scratch = [
            pltpu.SMEM((1,), jnp.int32), v(1, width, dtype=F32), v(1, width, dtype=F32),
            v(new_len, width), v(*w_q.shape), v(*w_k.shape), v(*w_v.shape), v(*w_o.shape), v(*w_gate.shape), v(*w_up.shape), v(*w_down.shape),
            v(NB, BLK, 384), v(NB, BLK, 256), v(NB, BLK, 384), v(NB, 8, BLK, dtype=F32), v(NB, 8, BLK, dtype=F32),
            v(new_len, 128, dtype=F32), v(new_len, 128, dtype=F32), v(64, PAST_MAX + new_len), v(PAST_MAX + new_len, 64),
            v(BLK, 256), v(NB, 128, BLK), v(NB, BLK, 128), v(NB, BLK, 128), v(BLK, PAST_MAX), v(NB, 2, BLK, 128), v(NB, 2, BLK, 128),
            tok, tok, tok, tok, tok, v(NB, 2, HALF, width), v(NB, 8, BLK, dtype=F32), v(NB, 8, BLK, dtype=F32), v(BLK, width), v(BLK, 128, dtype=F32),
            v(NB, CH, BLK, 2 * CW), v(2, CH, BLK, 2 * CW), v(NB, CH, BLK, 2 * CW), v(NB, CH, BLK, CW), v(NB, CH, BLK, CW),
            v(BLK, width, dtype=F32),
            tok, tok, tok, tok, tok,
            pltpu.SemaphoreType.DMA((16,)),
            pltpu.SemaphoreType.DMA((N_REMOTE,)), pltpu.SemaphoreType.DMA((N_REMOTE,)),
        ]
        vmem_spec = pl.BlockSpec(memory_space=pltpu.VMEM)
        done = pl.pallas_call(
            lambda *refs: kernel(2 * width, *refs),
            out_shape=tuple(v(*a) for a in (hidden.shape, k_flat.shape, v_flat.shape)),
            in_specs=[any_spec] * 13,
            out_specs=(vmem_spec,) * 3,
            scratch_shapes=scratch,
            compiler_params=pltpu.CompilerParams(collective_id=0, has_side_effects=True, vmem_limit_bytes=60 << 20),
            name="layer",
        )(past_len, hidden, rms_attn.reshape(1, width), rms_mlp.reshape(1, width), w_q, w_k, w_v, w_o, w_gate, w_up, w_down,
          k_flat, v_flat)
        out, k_full, v_full = pl.pallas_call(
            results_body,
            out_shape=tuple(jax.ShapeDtypeStruct(a, BF16) for a in (hidden.shape, k_flat.shape, v_flat.shape)),
            in_specs=[vmem_spec] * 3, out_specs=(any_spec,) * 3,
            scratch_shapes=[pltpu.SemaphoreType.DMA((NB + 2,))],
            compiler_params=pltpu.CompilerParams(vmem_limit_bytes=1 << 20),
            name="results",
        )(*done)
        heads, dim = k_cache.shape[1:]
        return (out, k_full.reshape(heads, dim, tokens).transpose(2, 0, 1), v_full.reshape(heads, dim, tokens).transpose(2, 0, 1))

    row_split = P('hid', 'tp')
    col_split = P('tp', 'hid')
    cache_spec = P('dp', 'tp', None)
    in_specs = (P('dp', 'hid'), P('hid'), P('hid'), row_split, row_split, row_split, col_split,
                row_split, row_split, col_split, cache_spec, cache_spec, P('dp'))
    out_specs = (P('dp', 'hid'), cache_spec, cache_spec)
    return jax.shard_map(local_layer, mesh=mesh, in_specs=in_specs, out_specs=out_specs, check_vma=False)
```

```python
import math
import jax
import jax.numpy as jnp
from jax import lax
from jax.experimental import pallas as pl
from jax.experimental.pallas import tpu as pltpu
from jax.sharding import PartitionSpec as P

ROPE_BASE = 10000.0
F32, BF16 = jnp.float32, jnp.bfloat16
NEG = -1e30
BLK = 256
HALF = BLK // 2
PAST_MAX = 1024
NB = 4
CH = 4
CW = 256
MESH = pl.DeviceIdType.MESH

UNITS = ((0, 0, 256), (1, 0, 256), (2, 0, 256), (3, 0, 128), (3, 2, 64), (3, 3, 64))
NU = len(UNITS)
Q, R, C, X, D, T, O = 0, 4, 8, 12, 16, 20, 24
E, Y, F, G = 32, 32 + NU, 32 + 2 * NU, 32 + 3 * NU
A = G + CH * NU
KV = A + CH * NU
N_REMOTE = KV + NB


def rope(t, cos_t, sin_t):
    width = t.shape[1]
    lane = lax.broadcasted_iota(jnp.int32, t.shape, 1)
    swapped = jnp.where((lane & 63) < 32, pltpu.roll(t, width - 32, 1), pltpu.roll(t, 32, 1))
    cos_w = jnp.concatenate([cos_t] * (width // 128), axis=1)
    sin_w = jnp.concatenate([sin_t] * (width // 128), axis=1)
    return (t * cos_w + swapped * sin_w).astype(BF16)


EPS = 1e-5


def square_sums(t):
    col = jnp.sum(t * t, axis=1, keepdims=True)
    return col, jnp.transpose(jnp.broadcast_to(col, (t.shape[0], 128)))[:8]


def as_column(row):
    return jnp.transpose(jnp.broadcast_to(row[:1], (128, row.shape[1])))[:, :1]


def half_factors(mine, theirs, d_model):
    r = lax.rsqrt((mine + theirs) / d_model + EPS)
    a = mine / (d_model // 2) + EPS
    b = theirs / (d_model // 2) + EPS
    return as_column(r * a * lax.rsqrt(a)), as_column(r * b * lax.rsqrt(b))


def kernel(d_model, p_hbm, x_hbm, g1_hbm, g2_hbm, wq_hbm, wk_hbm, wv_hbm, wo_hbm, wg_hbm, wu_hbm, wd_hbm, kc_hbm, vc_hbm,
           out, kc, vc,
           p_ref, g1_ref, g2_ref, x, wq, wk, wv, wo, wg, wu, wd, qsend, qkeep, qrecv, sq1, sq1r, cos_b, sin_b, kt, vv, qs, kvn, kvsend, kvrecv, picks, ob, orecv,
           csend, ckeep, crecv, part, xrecv, mid, sq2, sq2r, hg, sums, gsend, gkeep, grecv, ab, arecv, acc,
           esend, ekeep, erecv, part2, yrecv, lsem, ssem, rsem):
    h = lax.axis_index('hid')
    t = lax.axis_index('tp')
    c = lax.rem(t, 2)
    hid_dev = {'hid': 1 - h}
    core_dev = {'tp': t + 1 - 2 * c}
    x_dev = {'tp': lax.rem(t + 2, 4)}
    own = h == 0

    barrier = pltpu.get_barrier_semaphore()
    for dev in (hid_dev, core_dev, x_dev):
        pl.semaphore_signal(barrier, inc=1, device_id=dev, device_id_type=MESH)

    loads = []

    def load(src, dst):
        n = len(loads)
        cp = pltpu.make_async_copy(src, dst, lsem.at[n])
        cp.start()
        loads.append(cp)
        return cp

    ld_x = [load(x_hbm.at[pl.ds(0, BLK)], x.at[pl.ds(0, BLK)])]
    q_theirs = pl.ds(pl.multiple_of((1 - h) * 256, 256), 256)
    q_mine = pl.ds(pl.multiple_of(h * 256, 256), 256)
    ld_q = [load(g1_hbm, g1_ref), load(wq_hbm.at[:, q_theirs], wq.at[:, q_theirs]), load(wk_hbm, wk), load(wv_hbm, wv)]
    ld_mine = load(wq_hbm.at[:, q_mine], wq.at[:, q_mine])
    ld_x += [load(x_hbm.at[pl.ds(BLK, BLK)], x.at[pl.ds(BLK, BLK)])]
    ld_small = [load(p_hbm, p_ref), load(g2_hbm, g2_ref)]


    def remote(src, dst, n, dev):
        return pltpu.make_async_remote_copy(src_ref=src, dst_ref=dst, send_sem=ssem.at[n], recv_sem=rsem.at[n],
                                            device_id=dev, device_id_type=MESH)

    def q_copy(i): return remote(qsend.at[i], qrecv.at[i], Q + i, hid_dev)
    def r_copy(i): return remote(sq1.at[i], sq1r.at[i], R + i, hid_dev)
    def o_copy(i, n): return remote(ob.at[i, n], orecv.at[i, n], O + 2 * i + n, hid_dev)
    def kv_copy(i): return remote(kvsend.at[i], kvrecv.at[i], KV + i, hid_dev)
    def c_copy(i): return remote(csend.at[i], crecv.at[i], C + i, core_dev)
    def x_copy(i): return remote(part.at[i], xrecv.at[i], X + i, x_dev)
    def d_copy(i): return remote(mid.at[i, 0], mid.at[i, 1], D + i, core_dev)
    def t_copy(i): return remote(sq2.at[i], sq2r.at[i], T + i, hid_dev)

    def whole(u):
        return pl.ds(UNITS[u][1] * UNITS[u][2], UNITS[u][2])

    def half(u):
        return pl.ds(UNITS[u][1] * UNITS[u][2] // 2, UNITS[u][2] // 2)

    def own_rows(u):
        i, part_no, n = UNITS[u]
        return pl.ds(pl.multiple_of(i * BLK + c * HALF + part_no * (n // 2), 32), n // 2)

    def g_copy(u, j): return remote(gsend.at[UNITS[u][0], j, whole(u)], grecv.at[UNITS[u][0], j, whole(u)], G + CH * u + j, hid_dev)
    def a_copy(u, j): return remote(ab.at[UNITS[u][0], j, whole(u)], arecv.at[UNITS[u][0], j, whole(u)], A + CH * u + j, hid_dev)
    def e_copy(u): return remote(esend.at[UNITS[u][0], half(u)], erecv.at[UNITS[u][0], half(u)], E + u, core_dev)
    def y_copy(u): return remote(part2.at[UNITS[u][0], half(u)], yrecv.at[UNITS[u][0], half(u)], Y + u, x_dev)
    def f_copy(u):
        rows = own_rows(u)
        return remote(out.at[rows], out.at[rows], F + u, core_dev)

    def qkv(i, send):
        xf = x[pl.ds(i * BLK, BLK), :].astype(F32)
        sq, sq_row = square_sums(xf)
        xg = (xf * lax.rsqrt(sq / (d_model // 2) + EPS) * g1_ref[...]).astype(BF16)
        theirs = wq[:, q_theirs]
        qsend[i, :, :256] = jnp.dot(xg, theirs, preferred_element_type=F32).astype(BF16)
        k = jnp.dot(xg, wk[...], preferred_element_type=F32).astype(BF16)
        v = jnp.dot(xg, wv[...], preferred_element_type=F32).astype(BF16)
        low = jnp.concatenate([k[:, :64], v[:, :64]], axis=1)
        high = jnp.concatenate([k[:, 64:], v[:, 64:]], axis=1)
        qsend[i, :, 256:] = jnp.where(own, high, low)
        if i == 0:
            pl.semaphore_wait(barrier, 3)
        if send:
            q_copy(i).start()
        kvsend[i] = jnp.where(own, low, high)
        if i == 0:
            ld_mine.wait()
        mine = wq[:, q_mine]
        qkeep[i] = jnp.dot(xg, mine, preferred_element_type=F32).astype(BF16)
        sq1[i] = sq_row
        if send:
            r_copy(i).start()

    def tables(i):
        pos = (p_ref[0] + i * BLK + lax.broadcasted_iota(jnp.int32, (BLK, 128), 0)).astype(F32)
        lane = lax.broadcasted_iota(jnp.int32, (BLK, 128), 1)
        freq = jnp.exp((lane[:8] & 31).astype(F32) * (-2.0 * math.log(ROPE_BASE) / 64))[:1]
        ang = pos * freq
        cos_b[pl.ds(i * BLK, BLK), :] = jnp.cos(ang)
        sin = jnp.sin(ang)
        sin_b[pl.ds(i * BLK, BLK), :] = jnp.where((lane & 63) < 32, -sin, sin)

    def row_factors(i):
        return half_factors(sq1[i], sq1r[i], d_model)

    def keys_values(i, factors, mine, theirs):
        rows = slice(i * BLK, (i + 1) * BLK)
        mine, theirs = mine.astype(F32) * factors[0], theirs.astype(F32) * factors[1]
        kv = (jnp.where(own, mine, theirs) + jnp.where(own, theirs, mine)).astype(BF16)
        lane = lax.broadcasted_iota(jnp.int32, kv.shape, 1)
        return jnp.where(lane < 64, rope(kv.astype(F32), cos_b[rows, :], sin_b[rows, :]), kv)

    def att(i):
        rows = slice(i * BLK, (i + 1) * BLK)
        q_copy(i).wait_recv()
        r_copy(i).wait_recv()
        factors = row_factors(i)
        cos_t, sin_t = cos_b[rows, :], sin_b[rows, :]
        q = (qkeep[i].astype(F32) * factors[0] + qrecv[i, :, :256].astype(F32) * factors[1]).astype(BF16)
        kv = keys_values(i, factors, kvsend[i], qrecv[i, :, 256:])
        qs[...] = (rope(q.astype(F32), cos_t, sin_t).astype(F32) * 0.125).astype(BF16)
        kv_t = jnp.transpose(kv.astype(F32)).astype(BF16)
        kvn[i] = kv_t
        main = PAST_MAX + i * BLK
        kt[:, main:main + BLK] = kv_t[:64]
        vv[main:main + BLK, :] = kv[:, 64:]
        col = lax.broadcasted_iota(jnp.int32, (1, main), 1)
        bias = jnp.where((col >= p_ref[0]) & (col < PAST_MAX), NEG, 0.0)
        causal = lax.broadcasted_iota(jnp.int32, (BLK, BLK), 1) <= lax.broadcasted_iota(jnp.int32, (BLK, BLK), 0)

        def pair(n, carry):
            lanes = pl.ds(pl.multiple_of(n * 128, 128), 128)
            qp = qs[:, lanes]
            done = []
            for s in range(2):
                qn = qp[:, s * 64:(s + 1) * 64]
                s_main = jnp.dot(qn, kt[:, :main], preferred_element_type=F32) + bias
                s_diag = jnp.where(causal, jnp.dot(qn, kt[:, main:main + BLK], preferred_element_type=F32), NEG)
                top = jnp.maximum(jnp.max(s_main, axis=1, keepdims=True), jnp.max(s_diag, axis=1, keepdims=True))
                e_main = jnp.exp(s_main - top)
                e_diag = jnp.exp(s_diag - top)
                inv = 1.0 / (jnp.sum(e_main, axis=1, keepdims=True) + jnp.sum(e_diag, axis=1, keepdims=True))
                o = jnp.dot((e_main * inv).astype(BF16), vv[:main, :], preferred_element_type=F32)
                o += jnp.dot((e_diag * inv).astype(BF16), vv[main:main + BLK, :], preferred_element_type=F32)
                done.append(o.astype(BF16))
            ob[i, n] = jnp.concatenate(done, axis=1)
            o_copy(i, n).start()
            return carry
        lax.fori_loop(0, 2, pair, 0)

    def wo_step(i):
        o_copy(i, 0).wait_recv()
        o_copy(i, 1).wait_recv()
        mine = jnp.concatenate([ob[i, 0], ob[i, 1]], axis=1)
        theirs = jnp.concatenate([orecv[i, 0], orecv[i, 1]], axis=1)
        acc[...] = jnp.dot(mine, wo[pl.ds(pl.multiple_of(h * 256, 256), 256), :], preferred_element_type=F32)
        acc[...] += jnp.dot(theirs, wo[pl.ds(pl.multiple_of((1 - h) * 256, 256), 256), :], preferred_element_type=F32)
        ckeep[i] = acc[pl.ds(pl.multiple_of(c * HALF, HALF), HALF), :].astype(BF16)
        csend[i] = acc[pl.ds(pl.multiple_of((1 - c) * HALF, HALF), HALF), :].astype(BF16)
        c_copy(i).start()

    def add(a, b):
        return (a.astype(F32) + b.astype(F32)).astype(BF16)

    def c_step(i):
        c_copy(i).wait_recv()
        part[i] = add(ckeep[i], crecv[i])
        x_copy(i).start()

    def x_step(i):
        x_copy(i).wait_recv()
        res = x[pl.ds(pl.multiple_of(i * BLK + c * HALF, HALF), HALF), :]
        mid[i, 0] = add(res, add(part[i], xrecv[i]))
        d_copy(i).start()

    def d_step(i):
        d_copy(i).wait_recv()
        at = 0
        for u in range(NU):
            if UNITS[u][0] != i:
                continue
            for k in range(2):
                n = UNITS[u][2] // 2
                m = mid[i, k, half(u), :].astype(F32)
                sq = jnp.sum(m * m, axis=1, keepdims=True)
                sums[at:at + n, :] = jnp.broadcast_to(sq, (n, 128))
                hg[at:at + n, :] = (m * lax.rsqrt(sq / (d_model // 2) + EPS) * g2_ref[...]).astype(BF16)
                at += n
        sq2[i] = jnp.transpose(sums[...])[:8]

    def gate_up(u, side, j, dst):
        cols = pl.ds(pl.multiple_of(side * (CH * CW) + j * CW, CW), CW)
        rows = hg[whole(u), :]
        dst[:, :CW] = jnp.dot(rows, wg[:, cols], preferred_element_type=F32).astype(BF16)
        dst[:, CW:] = jnp.dot(rows, wu[:, cols], preferred_element_type=F32).astype(BF16)

    def u_step(u, j):
        i = UNITS[u][0]
        gate_up(u, 1 - h, j, gsend.at[i, j, whole(u)])
        g_copy(u, j).start()
        gate_up(u, h, j, gkeep.at[i % 2, j, whole(u)])

    def v_step(u, j):
        i = UNITS[u][0]
        g_copy(u, j).wait_recv()
        rows = slice(UNITS[u][1] * UNITS[u][2], (UNITS[u][1] + 1) * UNITS[u][2])
        mine, theirs = (f[rows] for f in half_factors(sq2[i], sq2r[i], d_model))
        both = gkeep[i % 2, j, whole(u), :].astype(F32) * mine + grecv[i, j, whole(u), :].astype(F32) * theirs
        both = both.astype(BF16).astype(F32)
        g, e = both[:, :CW], both[:, CW:]
        ab[i, j, whole(u), :] = (g * jax.nn.sigmoid(g) * e).astype(BF16)
        a_copy(u, j).start()

    def w_step(u, j):
        i = UNITS[u][0]
        a_copy(u, j).wait_recv()
        mine = wd[pl.ds(pl.multiple_of(h * (CH * CW) + j * CW, CW), CW), :]
        theirs = wd[pl.ds(pl.multiple_of((1 - h) * (CH * CW) + j * CW, CW), CW), :]
        y = jnp.dot(ab[i, j, whole(u), :], mine, preferred_element_type=F32)
        y += jnp.dot(arecv[i, j, whole(u), :], theirs, preferred_element_type=F32)
        acc[whole(u), :] = jnp.where(j == 0, 0.0, acc[whole(u), :]) + y

    def e_start(u):
        i, k, n = UNITS[u]
        ekeep[i, half(u), :] = acc[k * n:k * n + n // 2, :].astype(BF16)
        esend[i, half(u), :] = acc[k * n + n // 2:k * n + n, :].astype(BF16)
        e_copy(u).start()

    def e_step(u):
        i = UNITS[u][0]
        e_copy(u).wait_recv()
        part2[i, half(u), :] = add(ekeep[i, half(u), :], erecv[i, half(u), :])
        y_copy(u).start()

    def y_step(u):
        i = UNITS[u][0]
        y_copy(u).wait_recv()
        down = add(part2[i, half(u), :], yrecv[i, half(u), :])
        out[own_rows(u), :] = add(mid[i, 0, half(u), :], down)
        f_copy(u).start()

    def f_step(u):
        f_copy(u).wait_recv()

    def loop(*steps):
        def body(j, carry):
            for step, i in steps:
                step(i, j)
            return carry
        lax.fori_loop(0, CH, body, 0)

    span = PAST_MAX

    def make_picks():
        at = BLK - p_ref[0] + lax.broadcasted_iota(jnp.int32, (BLK, span), 1)
        picks[...] = jnp.where(at == lax.broadcasted_iota(jnp.int32, (BLK, span), 0), 1.0, 0.0).astype(BF16)

    def place(i, head, kv_t):
        lanes = pl.ds(pl.multiple_of(head * 64, 64), 64)
        cols = slice((i + 1) * BLK, (i + 1) * BLK + span)
        where = BLK - p_ref[0] + lax.broadcasted_iota(jnp.int32, (1, span), 1)
        fresh = (where >= 0) & (where < BLK)
        new = jnp.dot(kv_t, picks[...], preferred_element_type=F32)
        kc[lanes, cols] = jnp.where(fresh, new[:64], kc[lanes, cols].astype(F32)).astype(BF16)
        vc[lanes, cols] = jnp.where(fresh, new[64:], vc[lanes, cols].astype(F32)).astype(BF16)

    def kv_step(i):
        factors = row_factors(i)
        kv_copy(i).wait_recv()
        kv = keys_values(i, factors, qsend[i, :, 256:], kvrecv[i])
        place(i, 1 - h, jnp.transpose(kv.astype(F32)).astype(BF16))

    for cp in ld_q:
        cp.wait()
    ld_x[0].wait()
    qkv(0, True)
    ld_x += [load(x_hbm.at[pl.ds(i * BLK, BLK)], x.at[pl.ds(i * BLK, BLK)]) for i in range(2, NB)]
    ld_kc, ld_vc = load(kc_hbm, kc), load(vc_hbm, vc)
    ld_wo = load(wo_hbm, wo)
    ld_gu = [load(wg_hbm, wg), load(wu_hbm, wu)]
    ld_wd = load(wd_hbm, wd)
    for i in range(1, NB):
        ld_x[i].wait()
        qkv(i, i < 2)
    for cp in ld_small:
        cp.wait()
    for i in range(NB):
        tables(i)
    ld_kc.wait()
    ld_vc.wait()
    kt[:, :PAST_MAX] = kc[pl.ds(pl.multiple_of(h * 64, 64), 64), :PAST_MAX]
    v_old = jnp.transpose(vc[:, :PAST_MAX].astype(F32)).astype(BF16)
    vv[:PAST_MAX, :] = jnp.where(own, v_old[:, :64], v_old[:, 64:])
    att(0)
    q_copy(2).start()
    r_copy(2).start()
    att(1)
    q_copy(3).start()
    r_copy(3).start()
    ld_wo.wait()
    wo_step(0)
    c_step(0)
    att(2)
    x_step(0)
    wo_step(1)
    d_step(0)
    for cp in ld_gu:
        cp.wait()
    t_copy(0).start()
    loop((u_step, 0))
    c_step(1)
    att(3)
    x_step(1)
    wo_step(2)
    d_step(1)
    t_copy(1).start()
    t_copy(0).wait_recv()
    c_step(2)
    loop((u_step, 1), (v_step, 0))
    x_step(2)
    wo_step(3)
    c_step(3)
    d_step(2)
    t_copy(2).start()
    t_copy(1).wait_recv()
    ld_wd.wait()
    loop((u_step, 2), (v_step, 1), (w_step, 0))
    e_start(0)
    x_step(3)
    d_step(3)
    t_copy(3).start()
    e_step(0)
    t_copy(2).wait_recv()
    make_picks()
    for i in range(NB):
        place(i, h, kvn[i])
    loop((u_step, 3), (v_step, 2), (w_step, 1))
    loop((u_step, 4))
    loop((u_step, 5))
    e_start(1)
    y_step(0)
    e_step(1)
    f_step(0)
    t_copy(3).wait_recv()
    loop((v_step, 3), (w_step, 2))
    e_start(2)
    y_step(1)
    e_step(2)
    f_step(1)
    loop((v_step, 4))
    loop((v_step, 5))
    for i in range(NB):
        kv_copy(i).start()
    y_step(2)
    loop((w_step, 3))
    e_start(3)
    f_step(2)
    w_step(4, 0)
    e_step(3)
    for j in range(1, CH):
        w_step(4, j)
    e_start(4)
    w_step(5, 0)
    e_step(4)
    for j in range(1, CH):
        w_step(5, j)
    e_start(5)
    e_step(5)
    y_step(3)
    y_step(4)
    kv_step(0)
    kv_step(1)
    y_step(5)
    f_step(3)
    f_step(4)
    kv_step(2)
    for i in range(NB):
        for cp in (q_copy, r_copy, c_copy, x_copy, d_copy, t_copy):
            cp(i).wait_send()
        for n in range(2):
            o_copy(i, n).wait_send()
    for u in range(NU):
        def drain(j, carry, u=u):
            g_copy(u, j).wait_send()
            a_copy(u, j).wait_send()
            return carry
        lax.fori_loop(0, CH, drain, 0)
        for cp in (e_copy, y_copy, f_copy):
            cp(u).wait_send()
    f_step(5)
    kv_step(3)
    for i in range(NB):
        kv_copy(i).wait_send()


def results_body(out, kc, vc, out_hbm, ko_hbm, vo_hbm, sem):
    copies = [pltpu.make_async_copy(out.at[pl.ds(i * BLK, BLK)], out_hbm.at[pl.ds(i * BLK, BLK)], sem.at[i]) for i in range(NB)]
    copies += [pltpu.make_async_copy(kc, ko_hbm, sem.at[NB]), pltpu.make_async_copy(vc, vo_hbm, sem.at[NB + 1])]
    for cp in copies:
        cp.start()
    for cp in copies:
        cp.wait()


def solution(mesh):
    def local_layer(hidden, rms_attn, rms_mlp, w_q, w_k, w_v, w_o, w_gate, w_up, w_down, k_cache, v_cache, past_len):
        new_len, width = hidden.shape
        tokens = k_cache.shape[0]
        k_flat = k_cache.transpose(1, 2, 0).reshape(-1, tokens)
        v_flat = v_cache.transpose(1, 2, 0).reshape(-1, tokens)
        any_spec = pl.BlockSpec(memory_space=pl.ANY)

        def v(*shape, dtype=BF16):
            return pltpu.VMEM(shape, dtype)
        tok = v(NB, HALF, width)
        scratch = [
            pltpu.SMEM((1,), jnp.int32), v(1, width, dtype=F32), v(1, width, dtype=F32),
            v(new_len, width), v(*w_q.shape), v(*w_k.shape), v(*w_v.shape), v(*w_o.shape), v(*w_gate.shape), v(*w_up.shape), v(*w_down.shape),
            v(NB, BLK, 384), v(NB, BLK, 256), v(NB, BLK, 384), v(NB, 8, BLK, dtype=F32), v(NB, 8, BLK, dtype=F32),
            v(new_len, 128, dtype=F32), v(new_len, 128, dtype=F32), v(64, PAST_MAX + new_len), v(PAST_MAX + new_len, 64),
            v(BLK, 256), v(NB, 128, BLK), v(NB, BLK, 128), v(NB, BLK, 128), v(BLK, PAST_MAX), v(NB, 2, BLK, 128), v(NB, 2, BLK, 128),
            tok, tok, tok, tok, tok, v(NB, 2, HALF, width), v(NB, 8, BLK, dtype=F32), v(NB, 8, BLK, dtype=F32), v(BLK, width), v(BLK, 128, dtype=F32),
            v(NB, CH, BLK, 2 * CW), v(2, CH, BLK, 2 * CW), v(NB, CH, BLK, 2 * CW), v(NB, CH, BLK, CW), v(NB, CH, BLK, CW),
            v(BLK, width, dtype=F32),
            tok, tok, tok, tok, tok,
            pltpu.SemaphoreType.DMA((17,)),
            pltpu.SemaphoreType.DMA((N_REMOTE,)), pltpu.SemaphoreType.DMA((N_REMOTE,)),
        ]
        vmem_spec = pl.BlockSpec(memory_space=pltpu.VMEM)
        done = pl.pallas_call(
            lambda *refs: kernel(2 * width, *refs),
            out_shape=tuple(v(*a) for a in (hidden.shape, k_flat.shape, v_flat.shape)),
            in_specs=[any_spec] * 13,
            out_specs=(vmem_spec,) * 3,
            scratch_shapes=scratch,
            compiler_params=pltpu.CompilerParams(collective_id=0, has_side_effects=True, vmem_limit_bytes=60 << 20),
            name="layer",
        )(past_len, hidden, rms_attn.reshape(1, width), rms_mlp.reshape(1, width), w_q, w_k, w_v, w_o, w_gate, w_up, w_down,
          k_flat, v_flat)
        out, k_full, v_full = pl.pallas_call(
            results_body,
            out_shape=tuple(jax.ShapeDtypeStruct(a, BF16) for a in (hidden.shape, k_flat.shape, v_flat.shape)),
            in_specs=[vmem_spec] * 3, out_specs=(any_spec,) * 3,
            scratch_shapes=[pltpu.SemaphoreType.DMA((NB + 2,))],
            compiler_params=pltpu.CompilerParams(vmem_limit_bytes=1 << 20),
            name="results",
        )(*done)
        heads, dim = k_cache.shape[1:]
        return (out, k_full.reshape(heads, dim, tokens).transpose(2, 0, 1), v_full.reshape(heads, dim, tokens).transpose(2, 0, 1))

    row_split = P('hid', 'tp')
    col_split = P('tp', 'hid')
    cache_spec = P('dp', 'tp', None)
    in_specs = (P('dp', 'hid'), P('hid'), P('hid'), row_split, row_split, row_split, col_split,
                row_split, row_split, col_split, cache_spec, cache_spec, P('dp'))
    out_specs = (P('dp', 'hid'), cache_spec, cache_spec)
    return jax.shard_map(local_layer, mesh=mesh, in_specs=in_specs, out_specs=out_specs, check_vma=False)
```
